256 devices in a mesh: cls: 64 (over x, z, y_lo), dp: 4 (over y_hi, core).
Axes of the slice: x: 4, y: 4 (y_hi: 2, y_lo: 2; y = y_hi * 2 + y_lo), z: 8, core: 2. Of those that a mesh axis runs over, the one named last changes fastest.
Arguments:
- embeddings: bfloat16 [2048, 512], P(('dp', 'cls')), parts along dimension 0, may hold values from -4.4194174 to 4.4194174
- labels: int32 [2048], P(('dp', 'cls')), parts along dimension 0, may hold values from 0 to 262143
- centers: bfloat16 [1048576, 512], P(('dp', 'cls')), parts along dimension 0, may hold values from -3.0935922 to 3.0935922
Outputs:
- losses: float32 [2048], P(('dp', 'cls')), parts along dimension 0
- emb_grad: float32 [2048, 512], P(('dp', 'cls')), parts along dimension 0
- center_grad: float32 [1048576, 512], P(('dp', 'cls')), parts along dimension 0
The draws below stay inside these ranges and needn't reach their ends.
There are 4 independent parts, one for each index of `dp`. The reference program is written for one: setup_inputs(seed, part) draws one part's arguments, and reference() takes and returns one part's arrays. A program takes and returns all parts, laid end to end along the dimension named above; each array names one. Nothing has to cross between parts.
All inputs are finite; a program needn't handle non-finite values.
Results may differ from the reference program's by a relative error of at most 0.0042.
Values may be sent and summed in bfloat16 or wider, within the bound.
No kernel may reach another device: no remote copies, remote signals or barrier semaphores. Data moves between devices by JAX's collectives and lax.ppermute only.
A program may use at most 64 MiB of HBM per device.

```python
import math
import jax
import jax.numpy as jnp
from jax import lax

D = 512
C_DEV = 4096
CLASSES = 262144
BATCH = 512
N_CLS = 64


def shared_direction(key):
    return jnp.clip(jax.random.normal(jax.random.fold_in(key, 101), (D,), jnp.float32), -3.0, 3.0)


def noisy_rows(key, row_count):
    noise_key = jax.random.fold_in(key, 11)
    scale_key = jax.random.fold_in(key, 12)
    noise_part = jnp.clip(jax.random.normal(noise_key, (row_count, D), jnp.float32), -5.0, 5.0)
    scales = jnp.exp(jax.random.uniform(scale_key, (row_count, 1), jnp.float32, 0.0, math.log(10.0)))
    return (noise_part, scales)


def draw_embeddings(key, part):
    direction = shared_direction(key)
    noise_part, scales = noisy_rows(jax.random.fold_in(key, 21), BATCH)
    lean_share = 0.3
    values = scales * (noise_part + lean_share * direction[None, :]) / math.sqrt(D)
    return values.astype(jnp.bfloat16)


def draw_centers(key, part):
    direction = shared_direction(key)
    noise_part, scales = noisy_rows(jax.random.fold_in(key, 31), CLASSES)
    ramp_share = 0.06
    ramp = jnp.arange(CLASSES, dtype=jnp.float32) / max(CLASSES - 1, 1) * ramp_share
    values = scales * (noise_part + ramp[:, None] * direction[None, :]) / math.sqrt(D)
    return values.astype(jnp.bfloat16)


def place_ends(entries, key, least, high):
    longest = entries.shape.index(max(entries.shape))
    spots = []
    for shift in (0, 1):
        where = [jax.random.randint(jax.random.fold_in(key, axis), (), 0, length) for axis, length in enumerate(entries.shape)]
        where[longest] = (where[longest] + shift) % entries.shape[longest]
        spots.append(tuple(where))
    return entries.at[spots[0]].set(least).at[spots[1]].set(high)


def setup_inputs(seed: int = 0, part: int = 0) -> dict:
    streams_of = jax.random.split(jax.random.key(seed), 4)
    part_splits = jax.random.split(jax.random.fold_in(streams_of[3], part), 4)
    embeddings = draw_embeddings(jax.random.fold_in(jax.random.fold_in(streams_of[3], part), 71), part)
    labels = place_ends(jax.random.randint(part_splits[1], (BATCH,), 0, CLASSES), jax.random.fold_in(part_splits[1], 1), 0, CLASSES - 1).astype(jnp.int32)
    centers = draw_centers(jax.random.fold_in(jax.random.fold_in(streams_of[3], part), 71), part)
    return dict(embeddings=embeddings, labels=labels, centers=centers)


logit_scale = 64.0
margin_cosine = math.cos(0.5)
margin_sine = math.sin(0.5)
sine_soften = 0.04
norm_eps = 1e-06

def unit_rows(values):
    widened = values.astype(jnp.float32)
    inverse = lax.rsqrt(lax.optimization_barrier(jnp.sum(widened * widened, axis=1, keepdims=True)) + norm_eps)
    normed = widened * inverse
    return (inverse, normed, normed.astype(jnp.bfloat16))

def score_block(rows_hat, rows_label, center_block, class_base):
    cosine = jnp.dot(rows_hat, center_block.T, preferred_element_type=jnp.float32)
    local_col = rows_label - class_base
    is_owned = (local_col >= 0) & (local_col < center_block.shape[0])
    column = lax.broadcasted_iota(jnp.int32, cosine.shape, 1)
    target_mask = column == local_col[:, None]
    target_cos = lax.optimization_barrier(jnp.sum(jnp.where(target_mask, cosine, 0.0), axis=1))
    target_sine = jnp.sqrt(1.0 + sine_soften - target_cos * target_cos)
    shifted = target_cos * margin_cosine - target_sine * margin_sine
    slopes = margin_cosine + margin_sine * target_cos / target_sine
    logits = jnp.where(target_mask, logit_scale * shifted[:, None], logit_scale * cosine)
    exp_terms = jnp.exp(logits - logit_scale)
    row_total = lax.optimization_barrier(jnp.sum(exp_terms, axis=1))
    weighted = (logit_scale * exp_terms * jnp.where(target_mask, slopes[:, None], 1.0)).astype(jnp.bfloat16)
    target = jnp.where(is_owned, logit_scale * shifted, 0.0)
    columns = jnp.where(is_owned, local_col, -1).astype(jnp.int32)
    return (weighted, row_total, target, columns, jnp.where(is_owned, slopes, 0.0))

def row_term(weighted, center_block, totals, columns, slopes):
    product = jnp.dot(weighted, center_block, preferred_element_type=jnp.float32)
    picked = jnp.take(center_block, jnp.clip(columns, 0, center_block.shape[0] - 1), axis=0).astype(jnp.float32)
    return product / totals[:, None] - (logit_scale * slopes)[:, None] * picked

def class_term(weighted, scaled, rows_hat, columns, slopes, class_count):
    product = lax.dot_general(weighted, scaled, (((0,), (0,)), ((), ())), preferred_element_type=jnp.float32)
    drop_index = jnp.where(columns >= 0, columns, class_count).astype(jnp.int32)
    updates = -(logit_scale * slopes)[:, None] * rows_hat.astype(jnp.float32)
    return product.at[drop_index].add(updates, mode='drop')

def reference(embeddings, labels, centers):
    inv_x, units_x, emb_hat = unit_rows(embeddings)
    inv_w, units_w, center_hat = unit_rows(centers)
    hat_blocks = center_hat.reshape(N_CLS, C_DEV, D)
    starts = jnp.arange(N_CLS, dtype=jnp.int32) * C_DEV
    zero_rows = jnp.zeros((BATCH,), jnp.float32)

    def forward(carry, block_item):
        center_block, class_base = block_item
        weighted, row_total, target, columns, slopes = score_block(emb_hat, labels, center_block, class_base)
        return ((carry[0] + row_total, carry[1] + target), None)
    (totals, targets), _ = lax.scan(forward, (zero_rows, zero_rows), (hat_blocks, starts))
    losses = jnp.log(totals) + logit_scale - targets
    scaled = (emb_hat.astype(jnp.float32) / totals[:, None]).astype(jnp.bfloat16)

    def backward(row_sums, block_item):
        center_block, class_base = block_item
        weighted, row_total, target, columns, slopes = score_block(emb_hat, labels, center_block, class_base)
        row_sums = row_sums + row_term(weighted, center_block, totals, columns, slopes)
        return (row_sums, class_term(weighted, scaled, emb_hat, columns, slopes, C_DEV))
    grad_hat_x, grad_blocks = lax.scan(backward, jnp.zeros((BATCH, D), jnp.float32), (hat_blocks, starts))
    grad_hat_w = grad_blocks.reshape(CLASSES, D)
    emb_grad = inv_x * (grad_hat_x - units_x * lax.optimization_barrier(jnp.sum(units_x * grad_hat_x, axis=1, keepdims=True)))
    center_grad = inv_w * (grad_hat_w - units_w * lax.optimization_barrier(jnp.sum(units_w * grad_hat_w, axis=1, keepdims=True)))
    return (losses, emb_grad, center_grad)
```

```python
import math

import jax
import jax.numpy as jnp
from jax import lax
from jax.experimental import pallas as pl
from jax.experimental.pallas import tpu as pltpu
from jax.sharding import PartitionSpec as P

logit_scale = 64.0
margin_cosine = math.cos(0.5)
margin_sine = math.sin(0.5)
sine_soften = 0.04
norm_eps = 1e-06

slope2 = logit_scale * math.log2(math.e)
shift2 = slope2 - math.log2(logit_scale)

LANES = 128
MIB = 1024 * 1024
f32, bf16, i32 = jnp.float32, jnp.bfloat16, jnp.int32
VMEM = pl.BlockSpec(memory_space=pltpu.VMEM)
SMEM = pl.BlockSpec(memory_space=pltpu.SMEM)


def params(mib):
    return pltpu.CompilerParams(vmem_limit_bytes=mib * MIB)


def cost(flops, nbytes):
    return pl.CostEstimate(flops=int(flops), bytes_accessed=int(nbytes), transcendentals=0)


def dot(a, b, ca, cb):
    return lax.dot_general(a, b, (((ca,), (cb,)), ((), ())), preferred_element_type=f32)


def norm_kernel(c_ref, o_ref):
    w = c_ref[...].astype(f32)
    inv = lax.rsqrt(jnp.sum(w * w, axis=1, keepdims=True) + norm_eps)
    o_ref[...] = (w * inv).astype(bf16)


def unit_centers(centers, tile=1024):
    n, d = centers.shape
    return pl.pallas_call(
        norm_kernel,
        grid=(n // tile,),
        in_specs=[pl.BlockSpec((tile, d), lambda i: (i, 0))],
        out_specs=pl.BlockSpec((tile, d), lambda i: (i, 0)),
        out_shape=jax.ShapeDtypeStruct((n, d), bf16),
        compiler_params=params(16),
        cost_estimate=cost(3e9, 8 * MIB),
        name="unit_centers",
    )(centers)


def digit_weights(shape, dim):
    lane = lax.broadcasted_iota(i32, shape, dim)
    return jnp.where(lane == 0, 4096.0, jnp.where(lane == 1, 64.0, jnp.where(lane == 2, 1.0, 0.0)))


def score_kernel(base_ref, g_ref, c_ref, w_ref, e_ref, st_ref, pay_ref, *, tile, peers):
    n, d = c_ref.shape
    m = g_ref.shape[0]
    x = g_ref[:, :d].astype(f32)
    inv = lax.rsqrt(jnp.sum(x * x, axis=1, keepdims=True) + norm_eps)
    e_ref[...] = (x * inv).astype(bf16)
    weights = digit_weights((8, LANES), 1).astype(bf16)
    lab = dot(weights, g_ref[:, d:], 1, 1).astype(i32) - base_ref[0]
    lab1 = lab[0:1, :]
    ehat = e_ref[...]

    def step(k, carry):
        tot, tcs = carry
        row0 = pl.multiple_of(k * tile, tile)
        cos = dot(c_ref[pl.ds(row0, tile), :], ehat, 1, 1)
        row = lax.broadcasted_iota(i32, (tile, m), 0) + row0
        hit = row == lab1
        e = jnp.where(hit, 0.0, jnp.exp2(cos * slope2 - shift2))
        w_ref[pl.ds(row0, tile), :] = e.astype(bf16)
        tot = tot + e.reshape(tile // 8, 8, m).sum(axis=0)
        tcs = tcs + jnp.where(hit, cos, 0.0).reshape(tile // 8, 8, m).sum(axis=0)
        return tot, tcs

    zero = jnp.zeros((8, m), f32)
    tot, tcs = lax.fori_loop(0, n // tile, step, (zero, zero))
    tot = tot.sum(axis=0, keepdims=True)
    tc = tcs.sum(axis=0, keepdims=True)
    owned = (lab1 >= 0) & (lab1 < n)
    sine = jnp.sqrt(1.0 + sine_soften - tc * tc)
    shifted = tc * margin_cosine - sine * margin_sine
    slopes = jnp.where(owned, margin_cosine + margin_sine * tc / sine, 0.0)
    texp = jnp.where(owned, jnp.exp2(slope2 * shifted - shift2), 0.0)
    total = (tot + texp) * (1.0 / logit_scale)
    target = jnp.where(owned, logit_scale * shifted, 0.0)
    row8 = lax.broadcasted_iota(i32, (8, m), 0)
    st_ref[...] = jnp.where(row8 == 0, slopes, jnp.where(row8 == 1, texp, lab.astype(f32)))
    per = LANES // (m // peers)
    for p in range(peers):
        q = p // per
        pay_ref[p] = jnp.concatenate([total, target[:, q * LANES : (q + 1) * LANES]], axis=1)


def scores(base, gathered, chat, peers):
    n, d = chat.shape
    m = gathered.shape[0]
    return pl.pallas_call(
        lambda *refs: score_kernel(*refs, tile=256, peers=peers),
        in_specs=[SMEM, VMEM, VMEM],
        out_specs=[VMEM, VMEM, VMEM, VMEM],
        out_shape=[
            jax.ShapeDtypeStruct((n, m), bf16),
            jax.ShapeDtypeStruct((m, d), bf16),
            jax.ShapeDtypeStruct((8, m), f32),
            jax.ShapeDtypeStruct((peers, 1, m + LANES), f32),
        ],
        compiler_params=params(24),
        cost_estimate=cost(4e9, 8 * MIB),
        name="scores",
    )(base, gathered, chat)


def rows_kernel(st_ref, w_ref, c_ref, p_ref, t_ref, *, tile):
    n, d = c_ref.shape
    m = p_ref.shape[0]
    lab1 = st_ref[2:3, :].astype(i32)

    def step(k, _):
        row0 = pl.multiple_of(k * tile, tile)
        c = c_ref[pl.ds(row0, tile), :]
        row = lax.broadcasted_iota(i32, (tile, m), 0) + row0
        hot = jnp.where(row == lab1, 1.0, 0.0).astype(bf16)
        prod = dot(w_ref[pl.ds(row0, tile), :], c, 0, 0)
        pick = dot(hot, c, 0, 0)

        @pl.when(k == 0)
        def _():
            p_ref[...] = prod
            t_ref[...] = pick

        @pl.when(k > 0)
        def _():
            p_ref[...] += prod
            t_ref[...] += pick

        return 0

    lax.fori_loop(0, n // tile, step, 0)


def row_sums(stats, weighted, chat):
    n, d = chat.shape
    m = weighted.shape[1]
    return pl.pallas_call(
        lambda *refs: rows_kernel(*refs, tile=1024),
        in_specs=[VMEM, VMEM, VMEM],
        out_specs=[VMEM, VMEM],
        out_shape=[jax.ShapeDtypeStruct((m, d), f32), jax.ShapeDtypeStruct((m, d), f32)],
        compiler_params=params(24),
        cost_estimate=cost(6e9, 10 * MIB),
        name="row_sums",
    )(stats, weighted, chat)


def close_kernel(tr_ref, st_ref, p_ref, t_ref, q_ref, col_ref, tot_ref):
    m = p_ref.shape[0]
    sums = tr_ref[...].sum(axis=0)
    tot_ref[...] = sums
    total = sums[:, :m]
    coef = st_ref[0:1, :] * (st_ref[1:2, :] / total - logit_scale)
    row = lax.broadcasted_iota(i32, (LANES, m), 0)
    cols = jnp.where(row == 0, 1.0 / total, coef).T
    col_ref[...] = cols
    q_ref[...] = (p_ref[...] * cols[:, 0:1] + t_ref[...] * cols[:, 1:2]).astype(bf16)


def close_rows(received, stats, prod, pick):
    m, d = prod.shape
    return pl.pallas_call(
        close_kernel,
        in_specs=[VMEM, VMEM, VMEM, VMEM],
        out_specs=[VMEM, VMEM, VMEM],
        out_shape=[
            jax.ShapeDtypeStruct((m, d), bf16),
            jax.ShapeDtypeStruct((m, LANES), f32),
            jax.ShapeDtypeStruct((1, m + LANES), f32),
        ],
        compiler_params=params(16),
        cost_estimate=cost(1e9, 3 * MIB),
        name="close_rows",
    )(received, stats, prod, pick)


def class_kernel(st_ref, e_ref, col_ref, w_ref, c_ref, o_ref, s_ref, hi_ref, lo_ref, *, tile):
    m = e_ref.shape[0]

    @pl.when(pl.program_id(0) == 0)
    def _():
        e = e_ref[...].astype(f32)
        s_ref[...] = (e * col_ref[:, 0:1]).astype(bf16)
        own = e * col_ref[:, 1:2]
        hi = own.astype(bf16)
        hi_ref[...] = hi
        lo_ref[...] = (own - hi.astype(f32)).astype(bf16)

    row0 = pl.program_id(0) * tile
    lab1 = st_ref[2:3, :].astype(i32)
    row = lax.broadcasted_iota(i32, (tile, m), 0) + row0
    hot = jnp.where(row == lab1, 1.0, 0.0).astype(bf16)
    grad = dot(w_ref[...], s_ref[...], 1, 0)
    grad = grad + dot(hot, hi_ref[...], 1, 0)
    grad = grad + dot(hot, lo_ref[...], 1, 0)
    w = c_ref[...].astype(f32)
    inv = lax.rsqrt(jnp.sum(w * w, axis=1, keepdims=True) + norm_eps)
    units = w * inv
    along = jnp.sum(units * grad, axis=1, keepdims=True)
    o_ref[...] = inv * (grad - units * along)


def class_grads(stats, ehat, cols, weighted, centers, tile=512):
    n, d = centers.shape
    m = ehat.shape[0]
    whole = lambda a: pl.BlockSpec(a.shape, lambda i: (0, 0))
    return pl.pallas_call(
        lambda *refs: class_kernel(*refs, tile=tile),
        grid=(n // tile,),
        in_specs=[
            whole(stats),
            whole(ehat),
            whole(cols),
            pl.BlockSpec((tile, m), lambda i: (i, 0)),
            pl.BlockSpec((tile, d), lambda i: (i, 0)),
        ],
        out_specs=pl.BlockSpec((tile, d), lambda i: (i, 0)),
        out_shape=jax.ShapeDtypeStruct((n, d), f32),
        scratch_shapes=[pltpu.VMEM((m, d), bf16)] * 3,
        compiler_params=params(24),
        cost_estimate=cost(8e9, 16 * MIB),
        name="class_grads",
    )(stats, ehat, cols, weighted, centers)


def final_kernel(x_ref, r_ref, o_ref):
    x = x_ref[...].astype(f32)
    inv = lax.rsqrt(jnp.sum(x * x, axis=1, keepdims=True) + norm_eps)
    units = x * inv
    grad = r_ref[...].astype(f32).sum(axis=0)
    o_ref[...] = inv * (grad - units * jnp.sum(units * grad, axis=1, keepdims=True))


def example_grads(embeddings, received):
    return pl.pallas_call(
        final_kernel,
        in_specs=[VMEM, VMEM],
        out_specs=VMEM,
        out_shape=jax.ShapeDtypeStruct(embeddings.shape, f32),
        compiler_params=params(8),
        cost_estimate=cost(1e7, MIB),
        name="example_grads",
    )(embeddings, received)


def exchange(blocks):
    return lax.all_to_all(blocks, "cls", 0, 0, tiled=True)


def per_device(embeddings, labels, centers):
    own, d = embeddings.shape
    n = centers.shape[0]
    peers = lax.axis_size("cls")
    m = own * peers
    index = lax.axis_index("cls")
    lane = lax.broadcasted_iota(i32, (own, LANES), 1)
    lab = labels[:, None]
    digits = jnp.where(
        lane == 0, lab >> 12, jnp.where(lane == 1, (lab >> 6) & 63, jnp.where(lane == 2, lab & 63, 0))
    )
    packed = jnp.concatenate([embeddings, digits.astype(bf16)], axis=1)
    gathered = exchange(jnp.broadcast_to(packed[None], (peers, own, d + LANES)))
    chat = unit_centers(centers)
    base = (index * n).astype(i32)[None]
    weighted, ehat, stats, pay = scores(base, gathered.reshape(m, d + LANES), chat, peers)
    received = exchange(pay)
    prod, pick = row_sums(stats, weighted, chat)
    rows, cols, sums = close_rows(received, stats, prod, pick)
    rows = exchange(rows.reshape(peers, own, d))
    center_grad = class_grads(stats, ehat, cols, weighted, centers)
    per = LANES // own
    own_total = lax.dynamic_slice(sums[0], (index * own,), (own,))
    own_target = lax.dynamic_slice(sums[0], (m + (index % per) * own,), (own,))
    losses = jnp.log(own_total) + logit_scale - own_target
    emb_grad = example_grads(embeddings, rows)
    return (losses, emb_grad, center_grad)


def solution(mesh):
    in_specs = (P(("dp", "cls"), None), P(("dp", "cls")), P(("dp", "cls"), None))
    out_specs = (P(("dp", "cls")), P(("dp", "cls"), None), P(("dp", "cls"), None))
    return jax.shard_map(
        per_device, mesh=mesh, in_specs=in_specs, out_specs=out_specs, check_vma=False
    )
```

```python
import functools
import math

import jax
import jax.numpy as jnp
from jax import lax
from jax.experimental import pallas as pl
from jax.experimental.pallas import tpu as pltpu
from jax.sharding import Mesh
from jax.sharding import PartitionSpec as P

logit_scale = 64.0
margin_cosine = math.cos(0.5)
margin_sine = math.sin(0.5)
sine_soften = 0.04
norm_eps = 1e-06

slope2 = logit_scale * math.log2(math.e)
shift2 = slope2 - math.log2(logit_scale)

LANES = 128
MIB = 1024 * 1024
NEAR = ("x", "y")
FAR = "z"
f32, bf16, i32 = jnp.float32, jnp.bfloat16, jnp.int32
VMEM = pl.BlockSpec(memory_space=pltpu.VMEM)
SMEM = pl.BlockSpec(memory_space=pltpu.SMEM)
HBM = pl.BlockSpec(memory_space=pltpu.HBM)


def params(mib):
    return pltpu.CompilerParams(vmem_limit_bytes=mib * MIB)


def dot(a, b, ca, cb):
    return lax.dot_general(a, b, (((ca,), (cb,)), ((), ())), preferred_element_type=f32)


def inverse_norm(x):
    return lax.rsqrt(jnp.sum(x * x, axis=1, keepdims=True) + norm_eps)


def margin(cosine):
    sine = jnp.sqrt(1.0 + sine_soften - cosine * cosine)
    shifted = cosine * margin_cosine - sine * margin_sine
    slope = margin_cosine + margin_sine * cosine / sine
    return jnp.exp2(slope2 * shifted - shift2), logit_scale * shifted, slope


def total_rows(total):
    row8 = lax.broadcasted_iota(i32, (8, total.shape[1]), 0)
    out = jnp.zeros(row8.shape, f32)
    rest = total
    for r in range(3):
        part = rest.astype(bf16).astype(f32)
        out = jnp.where(row8 == r, part, out)
        rest = rest - part
    return out.astype(bf16)


def pack_kernel(x_ref, lab_ref, o_ref):
    rows, d = x_ref.shape
    row = lax.broadcasted_iota(i32, (rows, LANES), 0)
    lane = lax.broadcasted_iota(i32, (rows, LANES), 1)
    lab = jnp.zeros((rows, LANES), i32)
    for j in range(rows):
        lab = jnp.where(row == j, lab_ref[j], lab)
    digit = jnp.where(lane == 0, lab >> 12, jnp.where(lane == 1, (lab >> 6) & 63, lab & 63))
    digit = jnp.where(lane < 3, digit, 0).astype(f32).astype(bf16)
    for p in range(o_ref.shape[0]):
        o_ref[p, :, :d] = x_ref[...]
        o_ref[p, :, d:] = digit


def pack(embeddings, labels, peers):
    rows, d = embeddings.shape
    return pl.pallas_call(
        pack_kernel,
        in_specs=[VMEM, SMEM],
        out_specs=VMEM,
        out_shape=jax.ShapeDtypeStruct((peers, rows, d + LANES), bf16),
        compiler_params=params(4),
        name="pack",
    )(embeddings, labels)


def digit_weights(shape):
    lane = lax.broadcasted_iota(i32, shape, 1)
    return jnp.where(lane == 0, 4096.0, jnp.where(lane == 1, 64.0, jnp.where(lane == 2, 1.0, 0.0)))


def score_kernel(
    base_ref, g_ref, c_hbm, w_hbm, e_ref, st_ref, pay_ref, raw, chat, wv, isem, osem, *, tile, chunk, iblk
):
    n, d = c_hbm.shape
    m = g_ref.shape[0]
    groups = pay_ref.shape[0]
    chunks = n // chunk

    def load(k):
        rows = pl.ds(pl.multiple_of(k * chunk, chunk), chunk)
        return pltpu.make_async_copy(c_hbm.at[rows], raw.at[rows], isem.at[k])

    def save(k):
        rows = pl.ds(pl.multiple_of(k * chunk, chunk), chunk)
        return pltpu.make_async_copy(wv.at[rows], w_hbm.at[rows], osem.at[k])

    for k in range(chunks):
        load(k).start()
    x = g_ref[:, :d].astype(f32)
    e_ref[...] = (x * inverse_norm(x)).astype(bf16)
    tail = g_ref[:, d:]
    lab = dot(digit_weights((8, LANES)).astype(bf16), tail, 1, 1).astype(i32) - base_ref[0]
    lab1 = lab[0:1, :]
    col = jnp.sum(tail.astype(f32) * digit_weights((1, LANES)), axis=1, keepdims=True)
    col = col.astype(i32) - base_ref[0]

    def unit(k):
        rows = pl.ds(pl.multiple_of(k * tile, tile), tile)
        w = raw[rows, :].astype(f32)
        chat[rows, :] = (w * inverse_norm(w)).astype(bf16)

    per = chunk // tile
    load(0).wait()
    unit(0)

    def step(k, carry):
        tot, tcs = carry
        nxt = jnp.minimum(k + 1, n // tile - 1)

        @pl.when((lax.rem(nxt, per) == 0) & (k + 1 < n // tile))
        def _():
            load(nxt // per).wait()

        row0 = pl.multiple_of(k * tile, tile)
        cos = dot(chat[pl.ds(row0, tile), :], e_ref[...], 1, 1)
        unit(nxt)
        row = lax.broadcasted_iota(i32, (tile, m), 0) + row0
        hit = row == lab1
        e = jnp.where(hit, 0.0, jnp.exp2(cos * slope2 - shift2))
        wv[pl.ds(row0, tile), :] = e.astype(bf16)
        tot = tot + e.reshape(tile // 8, 8, m).sum(axis=0)
        tcs = tcs + jnp.where(hit, cos, 0.0).reshape(tile // 8, 8, m).sum(axis=0)

        @pl.when(lax.rem(k, per) == per - 1)
        def _():
            save(k // per).start()

        return tot, tcs

    zero = jnp.zeros((8, m), f32)
    tot, tcs = lax.fori_loop(0, n // tile, step, (zero, zero))
    owned = (lab1 >= 0) & (lab1 < n)
    texp, _, slope = margin(tcs.sum(axis=0, keepdims=True))
    texp = jnp.where(owned, texp, 0.0)
    slope = jnp.where(owned, slope, 0.0)
    total = (tot.sum(axis=0, keepdims=True) + texp) * (1.0 / logit_scale)
    row8 = lax.broadcasted_iota(i32, (8, m), 0)
    st_ref[...] = jnp.where(row8 == 0, slope, jnp.where(row8 == 1, texp, lab.astype(f32)))
    sums = total_rows(total)
    span = m // groups
    for p in range(groups):
        pay_ref[p, 2 * span :, :] = sums
    lane = lax.broadcasted_iota(i32, (iblk, n), 1)
    for b in range(m // iblk):
        rows = slice(b * iblk, (b + 1) * iblk)
        hot = jnp.where(lane == col[rows], 1.0, 0.0).astype(bf16)
        prod = dot(wv[:, rows], chat[...], 0, 0).astype(bf16)
        pick = dot(hot, chat[...], 1, 0).astype(bf16)
        for q in range(iblk // span):
            p = b * (iblk // span) + q
            pay_ref[p, 0:span, :] = prod[q * span : (q + 1) * span]
            pay_ref[p, span : 2 * span, :] = pick[q * span : (q + 1) * span]
    for k in range(chunks):
        save(k).wait()


def scores(base, gathered, centers, groups, tile=512, chunk=512, iblk=128):
    n, d = centers.shape
    m = gathered.shape[0]
    return pl.pallas_call(
        functools.partial(score_kernel, tile=tile, chunk=chunk, iblk=iblk),
        in_specs=[SMEM, VMEM, HBM],
        out_specs=[HBM, VMEM, VMEM, VMEM],
        out_shape=[
            jax.ShapeDtypeStruct((n, m), bf16),
            jax.ShapeDtypeStruct((m, d), bf16),
            jax.ShapeDtypeStruct((8, m), f32),
            jax.ShapeDtypeStruct((groups, 2 * (m // groups) + 8, d), bf16),
        ],
        scratch_shapes=[
            pltpu.VMEM((n, d), bf16),
            pltpu.VMEM((n, d), bf16),
            pltpu.VMEM((n, m), bf16),
            pltpu.SemaphoreType.DMA((n // chunk,)),
            pltpu.SemaphoreType.DMA((n // chunk,)),
        ],
        compiler_params=params(32),
        name="scores",
    )(base, gathered, centers)


def middle_kernel(r_ref, o_ref):
    far, rows, d = o_ref.shape
    own = rows // 3
    half = far * own
    sums = r_ref[...].astype(f32).sum(axis=0)
    low = sums[: 2 * half].astype(bf16)
    totals = total_rows(sums[2 * half :].sum(axis=0, keepdims=True))
    for q in range(far):
        o_ref[q, :own, :] = low[q * own : (q + 1) * own]
        o_ref[q, own : 2 * own, :] = low[half + q * own : half + (q + 1) * own]
        o_ref[q, 2 * own :, :] = totals


def middle(received, far, own):
    d = received.shape[2]
    return pl.pallas_call(
        middle_kernel,
        in_specs=[VMEM],
        out_specs=VMEM,
        out_shape=jax.ShapeDtypeStruct((far, 3 * own, d), bf16),
        compiler_params=params(8),
        name="middle",
    )(received)


def grad_kernel(
    own_ref, r_ref, x_ref, st_ref, e_ref, w_hbm, c_hbm, l_ref, xg_ref, o_hbm, wv, raw, out, wsem, csem, osem, *, chunk
):
    n, d = c_hbm.shape
    m = e_ref.shape[0]
    own = x_ref.shape[0]
    chunks = n // chunk

    def load(k):
        rows = pl.ds(pl.multiple_of(k * chunk, chunk), chunk)
        return (
            pltpu.make_async_copy(w_hbm.at[rows], wv.at[rows], wsem.at[k]),
            pltpu.make_async_copy(c_hbm.at[rows], raw.at[rows], csem.at[k]),
        )

    def save(k):
        rows = pl.ds(pl.multiple_of(k * chunk, chunk), chunk)
        return pltpu.make_async_copy(out.at[rows], o_hbm.at[rows], osem.at[k])

    for k in range(chunks):
        for copy in load(k):
            copy.start()
    sums = r_ref[...].astype(f32).sum(axis=0)
    total = sums[2 * own :].sum(axis=0, keepdims=True)
    scale = 1.0 / total
    coef = st_ref[0:1, :] * (st_ref[1:2, :] * scale - logit_scale)
    lab1 = st_ref[2:3, :].astype(i32)

    def step(k, _):
        for copy in load(k):
            copy.wait()
        rows = pl.ds(pl.multiple_of(k * chunk, chunk), chunk)
        hit = lax.broadcasted_iota(i32, (chunk, m), 0) == lab1 - k * chunk
        share = jnp.where(hit, coef, wv[rows, :].astype(f32) * scale).astype(bf16)
        grad = dot(share, e_ref[...], 1, 0)
        w = raw[rows, :].astype(f32)
        inv = inverse_norm(w)
        along = jnp.sum(w * grad, axis=1, keepdims=True) * (inv * inv)
        out[rows, :] = inv * (grad - w * along)
        save(k).start()
        return 0

    lax.fori_loop(0, chunks, step, 0)

    x = x_ref[...].astype(f32)
    inv = inverse_norm(x)
    units = x * inv
    unit16 = units.astype(bf16).astype(f32)
    pick = sums[own : 2 * own]
    texp, logit, slope = margin(jnp.sum(unit16 * pick, axis=1, keepdims=True))
    lane = lax.broadcasted_iota(i32, (own, m), 1)
    row = lax.broadcasted_iota(i32, (own, m), 0)
    own_total = jnp.sum(jnp.where(lane == row + own_ref[0], total, 0.0), axis=1, keepdims=True)
    grad = sums[:own] / own_total + (slope * (texp / own_total - logit_scale)) * pick
    xg_ref[...] = inv * (grad - units * jnp.sum(units * grad, axis=1, keepdims=True))
    loss = jnp.log(own_total) + logit_scale - logit
    spread = jnp.where(lane[:, :LANES] == row[:, :LANES], loss, 0.0).sum(axis=0, keepdims=True)
    l_ref[...] = spread[:, :own]
    for k in range(chunks):
        save(k).wait()


def grads(own_first, received, embeddings, stats, ehat, weighted, centers, chunk=512):
    n, d = centers.shape
    m = ehat.shape[0]
    own = embeddings.shape[0]
    return pl.pallas_call(
        functools.partial(grad_kernel, chunk=chunk),
        in_specs=[SMEM, VMEM, VMEM, VMEM, VMEM, HBM, HBM],
        out_specs=[VMEM, VMEM, HBM],
        out_shape=[
            jax.ShapeDtypeStruct((1, own), f32),
            jax.ShapeDtypeStruct((own, d), f32),
            jax.ShapeDtypeStruct((n, d), f32),
        ],
        scratch_shapes=[
            pltpu.VMEM((n, m), bf16),
            pltpu.VMEM((n, d), bf16),
            pltpu.VMEM((n, d), f32),
            pltpu.SemaphoreType.DMA((n // chunk,)),
            pltpu.SemaphoreType.DMA((n // chunk,)),
            pltpu.SemaphoreType.DMA((n // chunk,)),
        ],
        compiler_params=params(32),
        name="grads",
    )(own_first, received, embeddings, stats, ehat, weighted, centers)


def exchange(blocks, axis):
    return lax.all_to_all(blocks, axis, 0, 0, tiled=True)


def per_device(embeddings, labels, centers):
    own, d = embeddings.shape
    n = centers.shape[0]
    far = lax.axis_size(FAR)
    near = lax.axis_size(NEAR)
    m = own * far * near
    at_near = lax.axis_index(NEAR)
    at_far = lax.axis_index(FAR)
    place = lax.axis_index(("x", FAR, "y"))
    base = (place * n).astype(i32)[None]
    own_first = ((at_near * far + at_far) * own).astype(i32)[None]
    embeddings, base, own_first = lax.optimization_barrier((embeddings, base, own_first))
    line = exchange(pack(embeddings, labels, far), FAR).reshape(1, far * own, d + LANES)
    gathered = exchange(jnp.broadcast_to(line, (near, *line.shape[1:])), NEAR)
    weighted, ehat, stats, pay = scores(base, gathered.reshape(m, d + LANES), centers, near)
    half = middle(exchange(pay, NEAR), far, own)
    losses, emb_grad, center_grad = grads(
        own_first, exchange(half, FAR), embeddings, stats, ehat, weighted, centers
    )
    return (losses.reshape(own), emb_grad, center_grad)


def solution(mesh):
    dp = mesh.shape["dp"]
    fine = Mesh(mesh.devices.reshape(4, mesh.shape["cls"] // 8, 2, dp), ("x", FAR, "y", "dp"))
    rows = ("dp", "x", FAR, "y")
    in_specs = (P(rows, None), P(rows), P(rows, None))
    out_specs = (P(rows), P(rows, None), P(rows, None))
    return jax.shard_map(
        per_device, mesh=fine, in_specs=in_specs, out_specs=out_specs, check_vma=False
    )
```

```python
import functools
import math

import jax
import jax.numpy as jnp
from jax import lax
from jax.experimental import pallas as pl
from jax.experimental.pallas import tpu as pltpu
from jax.sharding import Mesh
from jax.sharding import PartitionSpec as P

logit_scale = 64.0
margin_cosine = math.cos(0.5)
margin_sine = math.sin(0.5)
sine_soften = 0.04
norm_eps = 1e-06

slope2 = logit_scale * math.log2(math.e)
shift2 = slope2 - math.log2(logit_scale)

LANES = 128
MIB = 1024 * 1024
NEAR = ("x", "y")
FAR = "z"
f32, bf16, i32 = jnp.float32, jnp.bfloat16, jnp.int32
VMEM = pl.BlockSpec(memory_space=pltpu.VMEM)
SMEM = pl.BlockSpec(memory_space=pltpu.SMEM)
HBM = pl.BlockSpec(memory_space=pltpu.HBM)


def params(mib):
    return pltpu.CompilerParams(vmem_limit_bytes=mib * MIB)


def in_hbm(x):
    return pltpu.with_memory_space_constraint(x, pltpu.HBM)


def dot(a, b, ca, cb):
    return lax.dot_general(a, b, (((ca,), (cb,)), ((), ())), preferred_element_type=f32)


def inverse_norm(x):
    return lax.rsqrt(jnp.sum(x * x, axis=1, keepdims=True) + norm_eps)


def margin(cosine):
    sine = jnp.sqrt(1.0 + sine_soften - cosine * cosine)
    shifted = cosine * margin_cosine - sine * margin_sine
    slope = margin_cosine + margin_sine * cosine / sine
    return jnp.exp2(slope2 * shifted - shift2), logit_scale * shifted, slope


def total_rows(total):
    row8 = lax.broadcasted_iota(i32, (8, total.shape[1]), 0)
    out = jnp.zeros(row8.shape, f32)
    rest = total
    for r in range(3):
        part = rest.astype(bf16).astype(f32)
        out = jnp.where(row8 == r, part, out)
        rest = rest - part
    return out.astype(bf16)


def pack_kernel(x_hbm, lab_hbm, o_ref, x_ref, lab_ref, sem):
    rows, d = x_ref.shape
    copies = (
        pltpu.make_async_copy(lab_hbm, lab_ref, sem.at[0]),
        pltpu.make_async_copy(x_hbm, x_ref, sem.at[1]),
    )
    for copy in copies:
        copy.start()
    for copy in copies:
        copy.wait()
    row = lax.broadcasted_iota(i32, (rows, LANES), 0)
    lane = lax.broadcasted_iota(i32, (rows, LANES), 1)
    lab = jnp.zeros((rows, LANES), i32)
    for j in range(rows):
        lab = jnp.where(row == j, lab_ref[j], lab)
    digit = jnp.where(lane == 0, lab >> 12, jnp.where(lane == 1, (lab >> 6) & 63, lab & 63))
    digit = jnp.where(lane < 3, digit, 0).astype(f32).astype(bf16)
    for p in range(o_ref.shape[0]):
        o_ref[p, :, :d] = x_ref[...]
        o_ref[p, :, d:] = digit


def pack(embeddings, labels, peers):
    rows, d = embeddings.shape
    return pl.pallas_call(
        pack_kernel,
        in_specs=[HBM, HBM],
        out_specs=VMEM,
        out_shape=jax.ShapeDtypeStruct((peers, rows, d + LANES), bf16),
        scratch_shapes=[
            pltpu.VMEM((rows, d), bf16),
            pltpu.SMEM((rows,), i32),
            pltpu.SemaphoreType.DMA((2,)),
        ],
        compiler_params=params(4),
        name="pack",
    )(in_hbm(embeddings), in_hbm(labels))


def digit_weights(shape):
    lane = lax.broadcasted_iota(i32, shape, 1)
    return jnp.where(lane == 0, 4096.0, jnp.where(lane == 1, 64.0, jnp.where(lane == 2, 1.0, 0.0)))


def score_kernel(
    base_ref, g_ref, c_hbm, wv, raw, e_ref, st_ref, pay_ref, chat, isem, *, tile, chunk, iblk
):
    n, d = c_hbm.shape
    m = g_ref.shape[0]
    groups = pay_ref.shape[0]
    chunks = n // chunk

    def load(k):
        rows = pl.ds(pl.multiple_of(k * chunk, chunk), chunk)
        return pltpu.make_async_copy(c_hbm.at[rows], raw.at[rows], isem.at[k])

    for k in range(chunks):
        load(k).start()
    x = g_ref[:, :d].astype(f32)
    e_ref[...] = (x * inverse_norm(x)).astype(bf16)
    tail = g_ref[:, d:]
    lab = dot(digit_weights((8, LANES)).astype(bf16), tail, 1, 1).astype(i32) - base_ref[0]
    lab1 = lab[0:1, :]
    col = jnp.sum(tail.astype(f32) * digit_weights((1, LANES)), axis=1, keepdims=True)
    col = col.astype(i32) - base_ref[0]

    def unit(k):
        rows = pl.ds(pl.multiple_of(k * tile, tile), tile)
        w = raw[rows, :].astype(f32)
        chat[rows, :] = (w * inverse_norm(w)).astype(bf16)

    per = chunk // tile
    load(0).wait()
    unit(0)

    def step(k, carry):
        tot, tcs = carry
        nxt = jnp.minimum(k + 1, n // tile - 1)

        @pl.when((lax.rem(nxt, per) == 0) & (k + 1 < n // tile))
        def _():
            load(nxt // per).wait()

        row0 = pl.multiple_of(k * tile, tile)
        cos = dot(chat[pl.ds(row0, tile), :], e_ref[...], 1, 1)
        unit(nxt)
        row = lax.broadcasted_iota(i32, (tile, m), 0) + row0
        hit = row == lab1
        e = jnp.where(hit, 0.0, jnp.exp2(cos * slope2 - shift2))
        wv[pl.ds(row0, tile), :] = e.astype(bf16)
        tot = tot + e.reshape(tile // 8, 8, m).sum(axis=0)
        tcs = tcs + jnp.where(hit, cos, 0.0).reshape(tile // 8, 8, m).sum(axis=0)
        return tot, tcs

    zero = jnp.zeros((8, m), f32)
    tot, tcs = lax.fori_loop(0, n // tile, step, (zero, zero))
    owned = (lab1 >= 0) & (lab1 < n)
    texp, _, slope = margin(tcs.sum(axis=0, keepdims=True))
    texp = jnp.where(owned, texp, 0.0)
    slope = jnp.where(owned, slope, 0.0)
    total = (tot.sum(axis=0, keepdims=True) + texp) * (1.0 / logit_scale)
    row8 = lax.broadcasted_iota(i32, (8, m), 0)
    st_ref[...] = jnp.where(row8 == 0, slope, jnp.where(row8 == 1, texp, lab.astype(f32)))
    sums = total_rows(total)
    span = m // groups
    for p in range(groups):
        pay_ref[p, 2 * span :, :] = sums
    lane = lax.broadcasted_iota(i32, (iblk, n), 1)
    for b in range(m // iblk):
        rows = slice(b * iblk, (b + 1) * iblk)
        hot = jnp.where(lane == col[rows], 1.0, 0.0).astype(bf16)
        prod = dot(wv[:, rows], chat[...], 0, 0).astype(bf16)
        pick = dot(hot, chat[...], 1, 0).astype(bf16)
        for q in range(iblk // span):
            p = b * (iblk // span) + q
            pay_ref[p, 0:span, :] = prod[q * span : (q + 1) * span]
            pay_ref[p, span : 2 * span, :] = pick[q * span : (q + 1) * span]


def scores(base, gathered, centers, groups, tile=512, chunk=512, iblk=128):
    n, d = centers.shape
    m = gathered.shape[0]
    return pl.pallas_call(
        functools.partial(score_kernel, tile=tile, chunk=chunk, iblk=iblk),
        in_specs=[SMEM, VMEM, HBM],
        out_specs=[VMEM] * 5,
        out_shape=[
            pltpu.VMEM((n, m), bf16),
            pltpu.VMEM((n, d), bf16),
            jax.ShapeDtypeStruct((m, d), bf16),
            jax.ShapeDtypeStruct((8, m), f32),
            jax.ShapeDtypeStruct((groups, 2 * (m // groups) + 8, d), bf16),
        ],
        scratch_shapes=[
            pltpu.VMEM((n, d), bf16),
            pltpu.SemaphoreType.DMA((n // chunk,)),
        ],
        compiler_params=params(24),
        name="scores",
    )(base, gathered, in_hbm(centers))


def middle_kernel(r_ref, o_ref):
    far, rows, d = o_ref.shape
    own = rows // 3
    half = far * own
    sums = r_ref[...].astype(f32).sum(axis=0)
    low = sums[: 2 * half].astype(bf16)
    totals = total_rows(sums[2 * half :].sum(axis=0, keepdims=True))
    for q in range(far):
        o_ref[q, :own, :] = low[q * own : (q + 1) * own]
        o_ref[q, own : 2 * own, :] = low[half + q * own : half + (q + 1) * own]
        o_ref[q, 2 * own :, :] = totals


def middle(received, far, own):
    d = received.shape[2]
    return pl.pallas_call(
        middle_kernel,
        in_specs=[VMEM],
        out_specs=VMEM,
        out_shape=jax.ShapeDtypeStruct((far, 3 * own, d), bf16),
        compiler_params=params(8),
        name="middle",
    )(received)


def grad_kernel(
    own_ref, r_ref, x_ref, st_ref, e_ref, wv, raw, l_ref, xg_ref, o_hbm, out, osem, *, chunk
):
    n, d = raw.shape
    m = e_ref.shape[0]
    own = x_ref.shape[0]
    chunks = n // chunk

    def save(k):
        rows = pl.ds(pl.multiple_of(k * chunk, chunk), chunk)
        return pltpu.make_async_copy(out.at[rows], o_hbm.at[rows], osem.at[k])

    sums = r_ref[...].astype(f32).sum(axis=0)
    total = sums[2 * own :].sum(axis=0, keepdims=True)
    scale = 1.0 / total
    coef = st_ref[0:1, :] * (st_ref[1:2, :] * scale - logit_scale)
    lab1 = st_ref[2:3, :].astype(i32)

    def step(k, _):
        rows = pl.ds(pl.multiple_of(k * chunk, chunk), chunk)
        hit = lax.broadcasted_iota(i32, (chunk, m), 0) == lab1 - k * chunk
        share = jnp.where(hit, coef, wv[rows, :].astype(f32) * scale).astype(bf16)
        grad = dot(share, e_ref[...], 1, 0)
        w = raw[rows, :].astype(f32)
        inv = inverse_norm(w)
        along = jnp.sum(w * grad, axis=1, keepdims=True) * (inv * inv)
        out[rows, :] = inv * (grad - w * along)
        save(k).start()
        return 0

    lax.fori_loop(0, chunks, step, 0)

    x = x_ref[...].astype(f32)
    inv = inverse_norm(x)
    units = x * inv
    unit16 = units.astype(bf16).astype(f32)
    pick = sums[own : 2 * own]
    texp, logit, slope = margin(jnp.sum(unit16 * pick, axis=1, keepdims=True))
    lane = lax.broadcasted_iota(i32, (own, m), 1)
    row = lax.broadcasted_iota(i32, (own, m), 0)
    own_total = jnp.sum(jnp.where(lane == row + own_ref[0], total, 0.0), axis=1, keepdims=True)
    grad = sums[:own] / own_total + (slope * (texp / own_total - logit_scale)) * pick
    xg_ref[...] = inv * (grad - units * jnp.sum(units * grad, axis=1, keepdims=True))
    loss = jnp.log(own_total) + logit_scale - logit
    spread = jnp.where(lane[:, :LANES] == row[:, :LANES], loss, 0.0).sum(axis=0, keepdims=True)
    l_ref[...] = spread[:, :own]
    for k in range(chunks):
        save(k).wait()


def grads(own_first, received, embeddings, stats, ehat, weighted, centers, chunk=512):
    n, d = centers.shape
    m = ehat.shape[0]
    own = embeddings.shape[0]
    return pl.pallas_call(
        functools.partial(grad_kernel, chunk=chunk),
        in_specs=[SMEM] + [VMEM] * 6,
        out_specs=[VMEM, VMEM, HBM],
        out_shape=[
            jax.ShapeDtypeStruct((1, own), f32),
            jax.ShapeDtypeStruct((own, d), f32),
            jax.ShapeDtypeStruct((n, d), f32),
        ],
        scratch_shapes=[
            pltpu.VMEM((n, d), f32),
            pltpu.SemaphoreType.DMA((n // chunk,)),
        ],
        compiler_params=params(24),
        name="grads",
    )(own_first, received, embeddings, stats, ehat, weighted, centers)


def exchange(blocks, axis):
    return lax.all_to_all(blocks, axis, 0, 0, tiled=True)


def per_device(embeddings, labels, centers):
    own, d = embeddings.shape
    n = centers.shape[0]
    far = lax.axis_size(FAR)
    near = lax.axis_size(NEAR)
    m = own * far * near
    at_near = lax.axis_index(NEAR)
    at_far = lax.axis_index(FAR)
    place = lax.axis_index(("x", FAR, "y"))
    base = (place * n).astype(i32)[None]
    own_first = ((at_near * far + at_far) * own).astype(i32)[None]
    embeddings, base, own_first = lax.optimization_barrier((embeddings, base, own_first))
    line = exchange(pack(embeddings, labels, far), FAR).reshape(1, far * own, d + LANES)
    gathered = exchange(jnp.broadcast_to(line, (near, *line.shape[1:])), NEAR)
    weighted, raw, ehat, stats, pay = scores(base, gathered.reshape(m, d + LANES), centers, near)
    half = middle(exchange(pay, NEAR), far, own)
    losses, emb_grad, center_grad = grads(
        own_first, exchange(half, FAR), embeddings, stats, ehat, weighted, raw
    )
    return (losses.reshape(own), emb_grad, center_grad)


def solution(mesh):
    dp = mesh.shape["dp"]
    fine = Mesh(mesh.devices.reshape(4, mesh.shape["cls"] // 8, 2, dp), ("x", FAR, "y", "dp"))
    rows = ("dp", "x", FAR, "y")
    in_specs = (P(rows, None), P(rows), P(rows, None))
    out_specs = (P(rows), P(rows, None), P(rows, None))
    return jax.shard_map(
        per_device, mesh=fine, in_specs=in_specs, out_specs=out_specs, check_vma=False
    )
```

```python
import functools
import math

import jax
import jax.numpy as jnp
from jax import lax
from jax.experimental import pallas as pl
from jax.experimental.pallas import tpu as pltpu
from jax.sharding import Mesh
from jax.sharding import PartitionSpec as P

logit_scale = 64.0
margin_cosine = math.cos(0.5)
margin_sine = math.sin(0.5)
sine_soften = 0.04
norm_eps = 1e-06

slope2 = logit_scale * math.log2(math.e)
shift2 = slope2 - math.log2(logit_scale)

LANES = 128
MIB = 1024 * 1024
NEAR = ("x", "y")
FAR = "z"
f32, bf16, i32 = jnp.float32, jnp.bfloat16, jnp.int32
VMEM = pl.BlockSpec(memory_space=pltpu.VMEM)
SMEM = pl.BlockSpec(memory_space=pltpu.SMEM)
HBM = pl.BlockSpec(memory_space=pltpu.HBM)


def params(mib):
    return pltpu.CompilerParams(vmem_limit_bytes=mib * MIB)


def in_hbm(x):
    return pltpu.with_memory_space_constraint(x, pltpu.HBM)


def dot(a, b, ca, cb):
    return lax.dot_general(a, b, (((ca,), (cb,)), ((), ())), preferred_element_type=f32)


def inverse_norm(x):
    return lax.rsqrt(jnp.sum(x * x, axis=1, keepdims=True) + norm_eps)


def margin(cosine):
    sine = jnp.sqrt(1.0 + sine_soften - cosine * cosine)
    shifted = cosine * margin_cosine - sine * margin_sine
    slope = margin_cosine + margin_sine * cosine / sine
    return jnp.exp2(slope2 * shifted - shift2), logit_scale * shifted, slope


def total_rows(total):
    row8 = lax.broadcasted_iota(i32, (8, total.shape[1]), 0)
    out = jnp.zeros(row8.shape, f32)
    rest = total
    for r in range(3):
        part = rest.astype(bf16).astype(f32)
        out = jnp.where(row8 == r, part, out)
        rest = rest - part
    return out.astype(bf16)


def pack_kernel(x_hbm, lab_hbm, o_ref, x_ref, lab_ref, sem):
    rows, d = x_ref.shape
    copies = (
        pltpu.make_async_copy(lab_hbm, lab_ref, sem.at[0]),
        pltpu.make_async_copy(x_hbm, x_ref, sem.at[1]),
    )
    for copy in copies:
        copy.start()
    for copy in copies:
        copy.wait()
    row = lax.broadcasted_iota(i32, (rows, LANES), 0)
    lane = lax.broadcasted_iota(i32, (rows, LANES), 1)
    lab = jnp.zeros((rows, LANES), i32)
    for j in range(rows):
        lab = jnp.where(row == j, lab_ref[j], lab)
    digit = jnp.where(lane == 0, lab >> 12, jnp.where(lane == 1, (lab >> 6) & 63, lab & 63))
    digit = jnp.where(lane < 3, digit, 0).astype(f32).astype(bf16)
    for p in range(o_ref.shape[0]):
        o_ref[p, :, :d] = x_ref[...]
        o_ref[p, :, d:] = digit


def pack(embeddings, labels, peers):
    rows, d = embeddings.shape
    return pl.pallas_call(
        pack_kernel,
        in_specs=[HBM, HBM],
        out_specs=VMEM,
        out_shape=jax.ShapeDtypeStruct((peers, rows, d + LANES), bf16),
        scratch_shapes=[
            pltpu.VMEM((rows, d), bf16),
            pltpu.SMEM((rows,), i32),
            pltpu.SemaphoreType.DMA((2,)),
        ],
        compiler_params=params(4),
        name="pack",
    )(in_hbm(embeddings), in_hbm(labels))


def digit_weights(shape):
    lane = lax.broadcasted_iota(i32, shape, 1)
    return jnp.where(lane == 0, 4096.0, jnp.where(lane == 1, 64.0, jnp.where(lane == 2, 1.0, 0.0)))


def score_half(base_ref, g_ref, chat, raw, fetch, w_ref, e_ref, st_ref, acc, pck, *, tile):
    n, d = chat.shape
    m = g_ref.shape[0]
    steps = n // tile
    x = g_ref[:, :d].astype(f32)
    e_ref[...] = (x * inverse_norm(x)).astype(bf16)
    tail = g_ref[:, d:]
    lab = dot(digit_weights((8, LANES)).astype(bf16), tail, 1, 1).astype(i32) - base_ref[0]
    lab1 = lab[0:1, :]
    col = jnp.sum(tail.astype(f32) * digit_weights((1, LANES)), axis=1, keepdims=True)
    col = col.astype(i32) - base_ref[0]

    def span(k):
        return pl.ds(pl.multiple_of(k * tile, tile), tile)

    def unit(k):
        w = raw[span(k), :].astype(f32)
        chat[span(k), :] = (w * inverse_norm(w)).astype(bf16)

    def score(k, tot, tcs):
        cos = dot(chat[span(k), :], e_ref[...], 1, 1)
        hit = lax.broadcasted_iota(i32, (tile, m), 0) == lab1 - k * tile
        e = jnp.where(hit, 0.0, jnp.exp2(cos * slope2 - shift2))
        w_ref[span(k), :] = e.astype(bf16)
        tot = tot + e.reshape(tile // 8, 8, m).sum(axis=0)
        tcs = tcs + jnp.where(hit, cos, 0.0).reshape(tile // 8, 8, m).sum(axis=0)
        return tot, tcs

    def gather(k):
        hot = lax.broadcasted_iota(i32, (m, tile), 1) == col - k * tile
        c = chat[span(k), :]
        prod = dot(w_ref[span(k), :], c, 0, 0)
        pick = dot(jnp.where(hot, 1.0, 0.0).astype(bf16), c, 1, 0)
        return prod, pick

    zero = jnp.zeros((8, m), f32)
    if raw is not None:
        fetch(0).wait()
        unit(0)
        fetch(1).wait()
        unit(1)
    tot, tcs = score(0, zero, zero)
    acc[...] = jnp.zeros(acc.shape, f32)
    pck[...] = jnp.zeros(pck.shape, f32)

    def step(k, carry):
        tot, tcs = carry
        if raw is not None:
            ahead = jnp.minimum(k + 1, steps - 1)

            @pl.when(k + 1 < steps)
            def _():
                fetch(ahead).wait()

        prod, pick = gather(k - 1)
        tot, tcs = score(k, tot, tcs)
        if raw is not None:
            unit(ahead)
        acc[...] += prod
        pck[...] += pick
        return tot, tcs

    tot, tcs = lax.fori_loop(1, steps, step, (tot, tcs))
    prod, pick = gather(steps - 1)
    acc[...] += prod
    pck[...] += pick
    owned = (lab1 >= 0) & (lab1 < n)
    texp, _, slope = margin(tcs.sum(axis=0, keepdims=True))
    texp = jnp.where(owned, texp, 0.0)
    slope = jnp.where(owned, slope, 0.0)
    total = (tot.sum(axis=0, keepdims=True) + texp) * (1.0 / logit_scale)
    row8 = lax.broadcasted_iota(i32, (8, m), 0)
    tail = jnp.where(row8 == 3, total, lab.astype(f32))
    st_ref[...] = jnp.where(row8 == 0, slope, jnp.where(row8 == 1, texp, tail))
    return total


def first_kernel(base_ref, g_ref, c_hbm, w_ref, raw, chat, e_ref, st_ref, pay_ref, acc, pck, sem, *, tile):
    n = c_hbm.shape[0]

    def fetch(k):
        rows = pl.ds(pl.multiple_of(k * tile, tile), tile)
        return pltpu.make_async_copy(c_hbm.at[rows], raw.at[rows], sem.at[k])

    for k in range(n // tile):
        fetch(k).start()
    score_half(base_ref, g_ref, chat, raw, fetch, w_ref, e_ref, st_ref, acc, pck, tile=tile)
    blocks, rows = pay_ref.shape[0], pay_ref.shape[1] // 2
    for p in range(blocks):
        pay_ref[p, :rows, :] = acc[p * rows : (p + 1) * rows].astype(bf16)
        pay_ref[p, rows:, :] = pck[p * rows : (p + 1) * rows].astype(bf16)


def second_kernel(
    base_ref, side_ref, g_ref, chat, first_ref, firstst_ref, w_ref, e_ref, st_ref, pay_ref, acc, pck, *, tile
):
    m = g_ref.shape[0]
    total = score_half(base_ref, g_ref, chat, None, None, w_ref, e_ref, st_ref, acc, pck, tile=tile)
    blocks, rows = first_ref.shape[0], first_ref.shape[1] // 2
    side = side_ref[0]
    mine = firstst_ref[3:4, :]
    left = jnp.where(side == 0, mine, total)
    right = jnp.where(side == 0, total, mine)
    sums = total_rows(jnp.concatenate([left, right], axis=1))
    for p in range(2 * blocks):
        pay_ref[p, 2 * rows :, :] = sums
    for p in range(blocks):
        pay_ref[2 * p + side, : 2 * rows, :] = first_ref[p]
        other = 2 * p + 1 - side
        pay_ref[other, :rows, :] = acc[p * rows : (p + 1) * rows].astype(bf16)
        pay_ref[other, rows : 2 * rows, :] = pck[p * rows : (p + 1) * rows].astype(bf16)


def half_shapes(n, m, d):
    return [
        pltpu.VMEM((n, m), bf16),
        jax.ShapeDtypeStruct((m, d), bf16),
        jax.ShapeDtypeStruct((8, m), f32),
    ]


def cost(gflops):
    return pl.CostEstimate(flops=int(gflops * 1e9), bytes_accessed=8 * MIB, transcendentals=0)


def first_scores(base, gathered, centers, blocks, tile=512):
    n, d = centers.shape
    m = gathered.shape[0]
    w, e, st = half_shapes(n, m, d)
    c = pltpu.VMEM((n, d), bf16)
    return pl.pallas_call(
        functools.partial(first_kernel, tile=tile),
        in_specs=[SMEM, VMEM, HBM],
        out_specs=[VMEM] * 6,
        out_shape=[w, c, c, e, st, jax.ShapeDtypeStruct((blocks, 2 * (m // blocks), d), bf16)],
        scratch_shapes=[pltpu.VMEM((m, d), f32)] * 2 + [pltpu.SemaphoreType.DMA((n // tile,))],
        compiler_params=params(24),
        cost_estimate=cost(6),
        name="first_scores",
    )(base, gathered, in_hbm(centers))


def second_scores(base, side, gathered, chat, first, stats, tile=512):
    n, d = chat.shape
    m = gathered.shape[0]
    blocks, rows = first.shape[0], first.shape[1]
    w, e, st = half_shapes(n, m, d)
    return pl.pallas_call(
        functools.partial(second_kernel, tile=tile),
        in_specs=[SMEM, SMEM] + [VMEM] * 4,
        out_specs=[VMEM] * 4,
        out_shape=[w, e, st, jax.ShapeDtypeStruct((2 * blocks, rows + 8, d), bf16)],
        scratch_shapes=[pltpu.VMEM((m, d), f32)] * 2,
        compiler_params=params(24),
        cost_estimate=cost(6),
        name="second_scores",
    )(base, side, gathered, chat, first, stats)


def middle_kernel(r_ref, o_ref):
    far, rows, d = o_ref.shape
    own = rows // 3
    half = far * own
    sums = r_ref[...].astype(f32).sum(axis=0)
    low = sums[: 2 * half].astype(bf16)
    totals = total_rows(sums[2 * half :].sum(axis=0, keepdims=True))
    for q in range(far):
        o_ref[q, :own, :] = low[q * own : (q + 1) * own]
        o_ref[q, own : 2 * own, :] = low[half + q * own : half + (q + 1) * own]
        o_ref[q, 2 * own :, :] = totals


def middle(received, far, own):
    d = received.shape[2]
    return pl.pallas_call(
        middle_kernel,
        in_specs=[VMEM],
        out_specs=VMEM,
        out_shape=jax.ShapeDtypeStruct((far, 3 * own, d), bf16),
        compiler_params=params(8),
        name="middle",
    )(received)


def grad_kernel(
    own_ref, side_ref, r_ref, x_ref, sta_ref, stb_ref, ea_ref, eb_ref, wa_ref, wb_ref, raw, l_ref, xg_ref, o_hbm,
    out, osem, *, chunk
):
    n, d = raw.shape
    half = ea_ref.shape[0]
    m = 2 * half
    own = x_ref.shape[0]
    chunks = n // chunk

    def save(k):
        rows = pl.ds(pl.multiple_of(k * chunk, chunk), chunk)
        return pltpu.make_async_copy(out.at[rows], o_hbm.at[rows], osem.at[k])

    sums = r_ref[...].astype(f32).sum(axis=0)
    total = sums[2 * own :].sum(axis=0, keepdims=True)
    left, right = 1.0 / total[:, :half], 1.0 / total[:, half:]
    side = side_ref[0]

    def factors(st_ref, scale):
        return st_ref[2:3, :].astype(i32), scale, st_ref[0:1, :] * (st_ref[1:2, :] * scale - logit_scale)

    halves = (
        (ea_ref, wa_ref, *factors(sta_ref, jnp.where(side == 0, left, right))),
        (eb_ref, wb_ref, *factors(stb_ref, jnp.where(side == 0, right, left))),
    )

    def step(k, _):
        rows = pl.ds(pl.multiple_of(k * chunk, chunk), chunk)
        row = lax.broadcasted_iota(i32, (chunk, half), 0)
        grad = 0.0
        for e_ref, w_ref, lab, scale, coef in halves:
            share = jnp.where(row == lab - k * chunk, coef, w_ref[rows, :].astype(f32) * scale)
            grad = grad + dot(share.astype(bf16), e_ref[...], 1, 0)
        w = raw[rows, :].astype(f32)
        inv = inverse_norm(w)
        along = jnp.sum(w * grad, axis=1, keepdims=True) * (inv * inv)
        out[rows, :] = inv * (grad - w * along)
        save(k).start()
        return 0

    lax.fori_loop(0, chunks, step, 0)

    x = x_ref[...].astype(f32)
    inv = inverse_norm(x)
    units = x * inv
    unit16 = units.astype(bf16).astype(f32)
    pick = sums[own : 2 * own]
    texp, logit, slope = margin(jnp.sum(unit16 * pick, axis=1, keepdims=True))
    lane = lax.broadcasted_iota(i32, (own, m), 1)
    row = lax.broadcasted_iota(i32, (own, m), 0)
    own_total = jnp.sum(jnp.where(lane == row + own_ref[0], total, 0.0), axis=1, keepdims=True)
    grad = sums[:own] / own_total + (slope * (texp / own_total - logit_scale)) * pick
    xg_ref[...] = inv * (grad - units * jnp.sum(units * grad, axis=1, keepdims=True))
    loss = jnp.log(own_total) + logit_scale - logit
    spread = jnp.where(lane[:, :LANES] == row[:, :LANES], loss, 0.0).sum(axis=0, keepdims=True)
    l_ref[...] = spread[:, :own]
    for k in range(chunks):
        save(k).wait()


def grads(own_first, side, received, embeddings, stats, ehats, weights, raw, chunk=512):
    n, d = raw.shape
    own = embeddings.shape[0]
    return pl.pallas_call(
        functools.partial(grad_kernel, chunk=chunk),
        in_specs=[SMEM, SMEM] + [VMEM] * 9,
        out_specs=[VMEM, VMEM, HBM],
        out_shape=[
            jax.ShapeDtypeStruct((1, own), f32),
            jax.ShapeDtypeStruct((own, d), f32),
            jax.ShapeDtypeStruct((n, d), f32),
        ],
        scratch_shapes=[pltpu.VMEM((n, d), f32), pltpu.SemaphoreType.DMA((n // chunk,))],
        compiler_params=params(24),
        name="grads",
    )(own_first, side, received, embeddings, *stats, *ehats, *weights, raw)


def exchange(blocks, axis):
    return lax.all_to_all(blocks, axis, 0, 0, tiled=True)


def per_device(embeddings, labels, centers):
    own, d = embeddings.shape
    n = centers.shape[0]
    far, wide = lax.axis_size(FAR), lax.axis_size("x")
    at_y = lax.axis_index("y")
    at = (lax.axis_index("x") * far + lax.axis_index(FAR)) * own
    half = far * wide * own
    base = (lax.axis_index(("x", FAR, "y")) * n).astype(i32)[None]
    own_first = (at_y * half + at).astype(i32)[None]
    side = at_y.astype(i32)[None]
    embeddings, base, own_first, side = lax.optimization_barrier((embeddings, base, own_first, side))
    line = exchange(pack(embeddings, labels, far), FAR).reshape(1, far * own, d + LANES)
    first = exchange(jnp.broadcast_to(line, (wide, *line.shape[1:])), "x").reshape(half, d + LANES)
    second = lax.ppermute(first, "y", [(0, 1), (1, 0)])
    wa, raw, chat, ea, sta, pay = first_scores(base, first, centers, wide)
    wb, eb, stb, pay = second_scores(base, side, second, chat, pay, sta)
    received = exchange(middle(exchange(pay, NEAR), far, own), FAR)
    losses, emb_grad, center_grad = grads(
        own_first, side, received, embeddings, (sta, stb), (ea, eb), (wa, wb), raw
    )
    return (losses.reshape(own), emb_grad, center_grad)


def solution(mesh):
    dp = mesh.shape["dp"]
    fine = Mesh(mesh.devices.reshape(4, mesh.shape["cls"] // 8, 2, dp), ("x", FAR, "y", "dp"))
    rows = ("dp", "x", FAR, "y")
    in_specs = (P(rows, None), P(rows), P(rows, None))
    out_specs = (P(rows), P(rows, None), P(rows, None))
    return jax.shard_map(
        per_device, mesh=fine, in_specs=in_specs, out_specs=out_specs, check_vma=False
    )
```

```python
import functools
import math

import jax
import jax.numpy as jnp
from jax import lax
from jax.experimental import pallas as pl
from jax.experimental.pallas import tpu as pltpu
from jax.sharding import Mesh
from jax.sharding import PartitionSpec as P

logit_scale = 64.0
margin_cosine = math.cos(0.5)
margin_sine = math.sin(0.5)
sine_soften = 0.04
norm_eps = 1e-06

slope2 = logit_scale * math.log2(math.e)
shift2 = slope2 - math.log2(logit_scale)


LANES = 128
MIB = 1024 * 1024
NEAR = ("x", "y")
FAR = "z"
f32, bf16, i32 = jnp.float32, jnp.bfloat16, jnp.int32
VMEM = pl.BlockSpec(memory_space=pltpu.VMEM)
SMEM = pl.BlockSpec(memory_space=pltpu.SMEM)
HBM = pl.BlockSpec(memory_space=pltpu.HBM)


def params(mib):
    return pltpu.CompilerParams(vmem_limit_bytes=mib * MIB)


def cost(gflops):
    return pl.CostEstimate(flops=int(gflops * 1e9), bytes_accessed=8 * MIB, transcendentals=0)


def in_hbm(x):
    return pltpu.with_memory_space_constraint(x, pltpu.HBM)


def dot(a, b, ca, cb):
    return lax.dot_general(a, b, (((ca,), (cb,)), ((), ())), preferred_element_type=f32)


def inverse_norm(x):
    return lax.rsqrt(jnp.sum(x * x, axis=1, keepdims=True) + norm_eps)


def margin(cosine):
    sine = jnp.sqrt(1.0 + sine_soften - cosine * cosine)
    shifted = cosine * margin_cosine - sine * margin_sine
    slope = margin_cosine + margin_sine * cosine / sine
    return jnp.exp2(slope2 * shifted - shift2), logit_scale * shifted, slope


def total_rows(total):
    row8 = lax.broadcasted_iota(i32, (8, total.shape[1]), 0)
    out = jnp.zeros(row8.shape, f32)
    rest = total
    for r in range(3):
        part = rest.astype(bf16).astype(f32)
        out = jnp.where(row8 == r, part, out)
        rest = rest - part
    return out.astype(bf16)


def pack_kernel(x_hbm, lab_hbm, o_ref, x_ref, lab_ref, sem):
    rows, d = x_ref.shape
    copies = (
        pltpu.make_async_copy(lab_hbm, lab_ref, sem.at[0]),
        pltpu.make_async_copy(x_hbm, x_ref, sem.at[1]),
    )
    for copy in copies:
        copy.start()
    for copy in copies:
        copy.wait()
    row = lax.broadcasted_iota(i32, (rows, LANES), 0)
    lane = lax.broadcasted_iota(i32, (rows, LANES), 1)
    lab = jnp.zeros((rows, LANES), i32)
    for j in range(rows):
        lab = jnp.where(row == j, lab_ref[j], lab)
    digit = jnp.where(lane == 0, lab >> 12, jnp.where(lane == 1, (lab >> 6) & 63, lab & 63))
    digit = jnp.where(lane < 3, digit, 0).astype(f32).astype(bf16)
    for p in range(o_ref.shape[0]):
        o_ref[p, :, :d] = x_ref[...]
        o_ref[p, :, d:] = digit


def pack(embeddings, labels, peers):
    rows, d = embeddings.shape
    return pl.pallas_call(
        pack_kernel,
        in_specs=[HBM, HBM],
        out_specs=VMEM,
        out_shape=jax.ShapeDtypeStruct((peers, rows, d + LANES), bf16),
        scratch_shapes=[
            pltpu.VMEM((rows, d), bf16),
            pltpu.SMEM((rows,), i32),
            pltpu.SemaphoreType.DMA((2,)),
        ],
        compiler_params=params(4),
        name="pack",
    )(in_hbm(embeddings), in_hbm(labels))


def digit_weights(shape):
    lane = lax.broadcasted_iota(i32, shape, 1)
    return jnp.where(lane == 0, 4096.0, jnp.where(lane == 1, 64.0, jnp.where(lane == 2, 1.0, 0.0)))


def unit_kernel(c_hbm, raw, chat, sem, *, tile):
    steps = c_hbm.shape[0] // tile

    def span(k):
        return pl.ds(pl.multiple_of(k * tile, tile), tile)

    def fetch(k):
        return pltpu.make_async_copy(c_hbm.at[span(k)], raw.at[span(k)], sem.at[k])

    for k in range(steps):
        fetch(k).start()

    def step(k, _):
        fetch(k).wait()
        w = raw[span(k), :].astype(f32)
        chat[span(k), :] = (w * inverse_norm(w)).astype(bf16)
        return 0

    lax.fori_loop(0, steps, step, 0)


def unit_centers(centers, tile=512):
    return pl.pallas_call(
        functools.partial(unit_kernel, tile=tile),
        in_specs=[HBM],
        out_specs=[VMEM] * 2,
        out_shape=[pltpu.VMEM(centers.shape, bf16)] * 2,
        scratch_shapes=[pltpu.SemaphoreType.DMA((centers.shape[0] // tile,))],
        compiler_params=params(12),
        cost_estimate=cost(3),
        name="unit_centers",
    )(in_hbm(centers))


def score_half(base_ref, g_ref, chat, w_ref, e_ref, st_ref, acc, pck, *, tile):
    n, d = chat.shape
    m = g_ref.shape[0]
    steps = n // tile
    x = g_ref[:, :d].astype(f32)
    e_ref[...] = (x * inverse_norm(x)).astype(bf16)
    tail = g_ref[:, d:]
    lab = dot(digit_weights((8, LANES)).astype(bf16), tail, 1, 1).astype(i32) - base_ref[0]
    lab1 = lab[0:1, :]
    col = jnp.sum(tail.astype(f32) * digit_weights((1, LANES)), axis=1, keepdims=True)
    col = col.astype(i32) - base_ref[0]

    def span(k):
        return pl.ds(pl.multiple_of(k * tile, tile), tile)

    def score(k, tot, tcs):
        cos = dot(chat[span(k), :], e_ref[...], 1, 1)
        hit = lax.broadcasted_iota(i32, (tile, m), 0) == lab1 - k * tile
        e = jnp.where(hit, 0.0, jnp.exp2(cos * slope2 - shift2))
        w_ref[span(k), :] = e.astype(bf16)
        tot = tot + e.reshape(tile // 8, 8, m).sum(axis=0)
        tcs = tcs + jnp.where(hit, cos, 0.0).reshape(tile // 8, 8, m).sum(axis=0)
        return tot, tcs

    def gather(k):
        hot = lax.broadcasted_iota(i32, (m, tile), 1) == col - k * tile
        c = chat[span(k), :]
        prod = dot(w_ref[span(k), :], c, 0, 0)
        pick = dot(jnp.where(hot, 1.0, 0.0).astype(bf16), c, 1, 0)
        return prod, pick

    zero = jnp.zeros((8, m), f32)
    tot, tcs = score(0, zero, zero)
    acc[...] = jnp.zeros(acc.shape, f32)
    pck[...] = jnp.zeros(pck.shape, f32)

    def step(k, carry):
        tot, tcs = carry
        prod, pick = gather(k - 1)
        tot, tcs = score(k, tot, tcs)
        acc[...] += prod
        pck[...] += pick
        return tot, tcs

    tot, tcs = lax.fori_loop(1, steps, step, (tot, tcs))
    prod, pick = gather(steps - 1)
    acc[...] += prod
    pck[...] += pick
    owned = (lab1 >= 0) & (lab1 < n)
    texp, _, slope = margin(tcs.sum(axis=0, keepdims=True))
    texp = jnp.where(owned, texp, 0.0)
    slope = jnp.where(owned, slope, 0.0)
    total = (tot.sum(axis=0, keepdims=True) + texp) * (1.0 / logit_scale)
    row8 = lax.broadcasted_iota(i32, (8, m), 0)
    tail = jnp.where(row8 == 3, total, lab.astype(f32))
    st_ref[...] = jnp.where(row8 == 0, slope, jnp.where(row8 == 1, texp, tail))


def first_kernel(base_ref, g_ref, chat, w_ref, e_ref, st_ref, pay_ref, acc, pck, *, tile):
    score_half(base_ref, g_ref, chat, w_ref, e_ref, st_ref, acc, pck, tile=tile)
    blocks, rows = pay_ref.shape[0], pay_ref.shape[1] // 2
    for p in range(blocks):
        pay_ref[p, :rows, :] = acc[p * rows : (p + 1) * rows].astype(bf16)
        pay_ref[p, rows:, :] = pck[p * rows : (p + 1) * rows].astype(bf16)


def second_kernel(base_ref, side_ref, x_ref, g_ref, chat, first_ref, firstst_ref, w_ref, e_ref, st_ref, pay_ref, acc, pck, *, tile):
    m = g_ref.shape[0]
    score_half(base_ref, g_ref, chat, w_ref, e_ref, st_ref, acc, pck, tile=tile)
    blocks, rows = first_ref.shape[0], first_ref.shape[1] // 2
    side, at_x = side_ref[0], x_ref[0]
    mine = pltpu.roll(firstst_ref[...], at_x * rows, 1)[3:4, :]
    theirs = pltpu.roll(st_ref[...], at_x * rows, 1)[3:4, :]
    left = jnp.where(side == 0, mine, theirs)
    right = jnp.where(side == 0, theirs, mine)
    sums = total_rows(jnp.concatenate([left, right], axis=1))
    for p in range(2 * blocks):
        pay_ref[p, 2 * rows :, :] = sums
    for p in range(blocks):
        to = lax.rem(at_x + p, blocks)
        pay_ref[2 * to + side, : 2 * rows, :] = first_ref[p]
        other = 2 * to + 1 - side
        pay_ref[other, :rows, :] = acc[p * rows : (p + 1) * rows].astype(bf16)
        pay_ref[other, rows : 2 * rows, :] = pck[p * rows : (p + 1) * rows].astype(bf16)


def half_shapes(n, m, d):
    return [
        pltpu.VMEM((n, m), bf16),
        jax.ShapeDtypeStruct((m, d), bf16),
        jax.ShapeDtypeStruct((8, m), f32),
    ]


def first_scores(base, gathered, chat, blocks, tile=1024):
    n, d = chat.shape
    m = gathered.shape[0]
    w, e, st = half_shapes(n, m, d)
    return pl.pallas_call(
        functools.partial(first_kernel, tile=tile),
        in_specs=[SMEM, VMEM, VMEM],
        out_specs=[VMEM] * 4,
        out_shape=[w, e, st, jax.ShapeDtypeStruct((blocks, 2 * (m // blocks), d), bf16)],
        scratch_shapes=[pltpu.VMEM((m, d), f32)] * 2,
        compiler_params=params(24),
        cost_estimate=cost(6),
        name="first_scores",
    )(base, gathered, chat)


def second_scores(where, gathered, chat, first, stats, tile=1024):
    n, d = chat.shape
    m = gathered.shape[0]
    blocks, rows = first.shape[0], first.shape[1]
    w, e, st = half_shapes(n, m, d)
    return pl.pallas_call(
        functools.partial(second_kernel, tile=tile),
        in_specs=[SMEM] * 3 + [VMEM] * 4,
        out_specs=[VMEM] * 4,
        out_shape=[w, e, st, jax.ShapeDtypeStruct((2 * blocks, rows + 8, d), bf16)],
        scratch_shapes=[pltpu.VMEM((m, d), f32)] * 2,
        compiler_params=params(24),
        cost_estimate=cost(6),
        name="second_scores",
    )(*where, gathered, chat, first, stats)


def middle_kernel(r_ref, o_ref):
    far, rows, d = o_ref.shape
    own = rows // 3
    half = far * own
    sums = r_ref[...].astype(f32).sum(axis=0)
    low = sums[: 2 * half].astype(bf16)
    totals = total_rows(sums[2 * half :].sum(axis=0, keepdims=True))
    for q in range(far):
        o_ref[q, :own, :] = low[q * own : (q + 1) * own]
        o_ref[q, own : 2 * own, :] = low[half + q * own : half + (q + 1) * own]
        o_ref[q, 2 * own :, :] = totals


def middle(received, far, own):
    d = received.shape[2]
    return pl.pallas_call(
        middle_kernel,
        in_specs=[VMEM],
        out_specs=VMEM,
        out_shape=jax.ShapeDtypeStruct((far, 3 * own, d), bf16),
        compiler_params=params(8),
        name="middle",
    )(received)


def grad_kernel(
    side_ref, at_ref, own_ref, r_ref, x_ref, sta_ref, stb_ref, ea_ref, eb_ref, wa_ref, wb_ref, raw, l_hbm, xg_hbm, o_hbm,
    out, xg_ref, l_ref, osem, sem, *, chunk, blocks
):
    n, d = raw.shape
    half = ea_ref.shape[0]
    m = 2 * half
    own = x_ref.shape[0]
    chunks = n // chunk

    def save(k):
        rows = pl.ds(pl.multiple_of(k * chunk, chunk), chunk)
        return pltpu.make_async_copy(out.at[rows], o_hbm.at[rows], osem.at[k])

    side, at_x, own_first = side_ref[0], at_ref[0], own_ref[0]
    sums = r_ref[...].astype(f32).sum(axis=0)
    total = sums[2 * own :].sum(axis=0, keepdims=True)
    back = lax.rem(blocks - at_x, blocks) * (half // blocks)
    both = jnp.broadcast_to(total, (8, m))
    left = 1.0 / pltpu.roll(both[:, :half], back, 1)[0:1, :]
    right = 1.0 / pltpu.roll(both[:, half:], back, 1)[0:1, :]

    def factors(st_ref, scale):
        return st_ref[2:3, :].astype(i32), scale, st_ref[0:1, :] * (st_ref[1:2, :] * scale - logit_scale)

    halves = (
        (ea_ref, wa_ref, *factors(sta_ref, jnp.where(side == 0, left, right))),
        (eb_ref, wb_ref, *factors(stb_ref, jnp.where(side == 0, right, left))),
    )

    x = x_ref[...].astype(f32)
    inv = inverse_norm(x)
    units = x * inv
    unit16 = units.astype(bf16).astype(f32)
    pick = sums[own : 2 * own]
    texp, logit, slope = margin(jnp.sum(unit16 * pick, axis=1, keepdims=True))
    lane = lax.broadcasted_iota(i32, (own, m), 1)
    row = lax.broadcasted_iota(i32, (own, m), 0)
    own_total = jnp.sum(jnp.where(lane == row + own_first, total, 0.0), axis=1, keepdims=True)
    grad = sums[:own] / own_total + (slope * (texp / own_total - logit_scale)) * pick
    xg_ref[...] = inv * (grad - units * jnp.sum(units * grad, axis=1, keepdims=True))
    loss = jnp.log(own_total) + logit_scale - logit
    spread = jnp.where(lane[:, :LANES] == row[:, :LANES], loss, 0.0).sum(axis=0, keepdims=True)
    l_ref[...] = spread

    def step(k, _):
        rows = pl.ds(pl.multiple_of(k * chunk, chunk), chunk)
        row = lax.broadcasted_iota(i32, (chunk, half), 0)
        grad = 0.0
        for e_ref, w_ref, lab, scale, coef in halves:
            share = jnp.where(row == lab - k * chunk, coef, w_ref[rows, :].astype(f32) * scale)
            grad = grad + dot(share.astype(bf16), e_ref[...], 1, 0)
        w = raw[rows, :].astype(f32)
        inv = inverse_norm(w)
        along = jnp.sum(w * grad, axis=1, keepdims=True) * (inv * inv)
        out[rows, :] = inv * (grad - w * along)
        save(k).start()
        return 0

    step(0, 0)
    small = (
        pltpu.make_async_copy(xg_ref, xg_hbm, sem.at[0]),
        pltpu.make_async_copy(l_ref, l_hbm, sem.at[1]),
    )
    for copy in small:
        copy.start()
    lax.fori_loop(1, chunks, step, 0)
    for copy in small:
        copy.wait()
    for k in range(chunks):
        save(k).wait()


def grads(where, received, embeddings, stats, ehats, weights, raw, blocks, chunk=512):
    n, d = raw.shape
    own = embeddings.shape[0]
    return pl.pallas_call(
        functools.partial(grad_kernel, chunk=chunk, blocks=blocks),
        in_specs=[SMEM] * 3 + [VMEM] * 9,
        out_specs=[HBM] * 3,
        out_shape=[
            jax.ShapeDtypeStruct((1, LANES), f32),
            jax.ShapeDtypeStruct((own, d), f32),
            jax.ShapeDtypeStruct((n, d), f32),
        ],
        scratch_shapes=[
            pltpu.VMEM((n, d), f32),
            pltpu.VMEM((own, d), f32),
            pltpu.VMEM((1, LANES), f32),
            pltpu.SemaphoreType.DMA((n // chunk,)),
            pltpu.SemaphoreType.DMA((2,)),
        ],
        compiler_params=params(24),
        name="grads",
    )(*where, received, embeddings, *stats, *ehats, *weights, raw)


def exchange(blocks, axis):
    return lax.all_to_all(blocks, axis, 0, 0, tiled=True)


def per_device(embeddings, labels, centers):
    own, d = embeddings.shape
    n = centers.shape[0]
    far, wide = lax.axis_size(FAR), lax.axis_size("x")
    at_x, at_y = lax.axis_index("x"), lax.axis_index("y")
    half = far * wide * own
    base = lax.axis_index(("x", FAR, "y")) * n
    own_first = at_y * half + (at_x * far + lax.axis_index(FAR)) * own
    where = tuple(a.astype(i32)[None] for a in (base, at_y, at_x, own_first))
    embeddings, where = lax.optimization_barrier((embeddings, where))
    base, side, at_x, own_first = where
    line = exchange(pack(embeddings, labels, far), FAR).reshape(far * own, d + LANES)
    lines = [line] + [
        lax.ppermute(line, "x", [(i, (i - k) % wide) for i in range(wide)]) for k in range(1, wide)
    ]
    raw, chat = unit_centers(centers)
    first = jnp.concatenate(lines, axis=0)
    second = lax.ppermute(first, "y", [(0, 1), (1, 0)])
    wa, ea, sta, pay = first_scores(base, first, chat, wide)
    wb, eb, stb, pay = second_scores((base, side, at_x), second, chat, pay, sta)
    received = exchange(middle(exchange(pay, NEAR), far, own), FAR)
    losses, emb_grad, center_grad = grads(
        (side, at_x, own_first), received, embeddings, (sta, stb), (ea, eb), (wa, wb), raw, wide
    )
    return (losses[0, :own], emb_grad, center_grad)


def solution(mesh):
    dp = mesh.shape["dp"]
    fine = Mesh(mesh.devices.reshape(4, mesh.shape["cls"] // 8, 2, dp), ("x", FAR, "y", "dp"))
    rows = ("dp", "x", FAR, "y")
    in_specs = (P(rows, None), P(rows), P(rows, None))
    out_specs = (P(rows), P(rows, None), P(rows, None))
    return jax.shard_map(
        per_device, mesh=fine, in_specs=in_specs, out_specs=out_specs, check_vma=False
    )
```

```python
import functools
import math

import jax
import jax.numpy as jnp
from jax import lax
from jax.experimental import pallas as pl
from jax.experimental.pallas import tpu as pltpu
from jax.sharding import Mesh
from jax.sharding import PartitionSpec as P

logit_scale = 64.0
margin_cosine = math.cos(0.5)
margin_sine = math.sin(0.5)
sine_soften = 0.04
norm_eps = 1e-06

slope2 = logit_scale * math.log2(math.e)
shift2 = slope2 - math.log2(logit_scale)


LANES = 128
SLOTS = 64
MIB = 1024 * 1024
NEAR = ("x", "y")
FAR = "z"
f32, bf16, i32 = jnp.float32, jnp.bfloat16, jnp.int32
VMEM = pl.BlockSpec(memory_space=pltpu.VMEM)
SMEM = pl.BlockSpec(memory_space=pltpu.SMEM)
HBM = pl.BlockSpec(memory_space=pltpu.HBM)


def params(mib):
    return pltpu.CompilerParams(vmem_limit_bytes=mib * MIB)


def cost(gflops):
    return pl.CostEstimate(flops=int(gflops * 1e9), bytes_accessed=8 * MIB, transcendentals=0)


def in_hbm(x):
    return pltpu.with_memory_space_constraint(x, pltpu.HBM)


def dot(a, b, ca, cb):
    return lax.dot_general(a, b, (((ca,), (cb,)), ((), ())), preferred_element_type=f32)


def inverse_norm(x):
    return lax.rsqrt(jnp.sum(x * x, axis=1, keepdims=True) + norm_eps)


def margin(cosine):
    sine = jnp.sqrt(1.0 + sine_soften - cosine * cosine)
    shifted = cosine * margin_cosine - sine * margin_sine
    slope = margin_cosine + margin_sine * cosine / sine
    return jnp.exp2(slope2 * shifted - shift2), logit_scale * shifted, slope


def total_rows(total):
    row8 = lax.broadcasted_iota(i32, (8, total.shape[1]), 0)
    out = jnp.zeros(row8.shape, f32)
    rest = total
    for r in range(3):
        part = rest.astype(bf16).astype(f32)
        out = jnp.where(row8 == r, part, out)
        rest = rest - part
    return out.astype(bf16)


def pack_kernel(x_hbm, lab_hbm, o_ref, x_ref, lab_ref, sem):
    rows, d = x_ref.shape
    copies = (
        pltpu.make_async_copy(lab_hbm, lab_ref, sem.at[0]),
        pltpu.make_async_copy(x_hbm, x_ref, sem.at[1]),
    )
    for copy in copies:
        copy.start()
    for copy in copies:
        copy.wait()
    row = lax.broadcasted_iota(i32, (rows, LANES), 0)
    lane = lax.broadcasted_iota(i32, (rows, LANES), 1)
    lab = jnp.zeros((rows, LANES), i32)
    for j in range(rows):
        lab = jnp.where(row == j, lab_ref[j], lab)
    digit = jnp.where(lane == 0, lab >> 12, jnp.where(lane == 1, (lab >> 6) & 63, lab & 63))
    digit = jnp.where(lane < 3, digit, 0).astype(f32).astype(bf16)
    for p in range(o_ref.shape[0]):
        o_ref[p, :, :d] = x_ref[...]
        o_ref[p, :, d:] = digit


def pack(embeddings, labels, peers):
    rows, d = embeddings.shape
    return pl.pallas_call(
        pack_kernel,
        in_specs=[HBM, HBM],
        out_specs=VMEM,
        out_shape=jax.ShapeDtypeStruct((peers, rows, d + LANES), bf16),
        scratch_shapes=[
            pltpu.VMEM((rows, d), bf16),
            pltpu.SMEM((rows,), i32),
            pltpu.SemaphoreType.DMA((2,)),
        ],
        compiler_params=params(4),
        name="pack",
    )(in_hbm(embeddings), in_hbm(labels))


def merge_kernel(*refs):
    *line_refs, o_ref = refs
    rows, d = line_refs[0].shape[0], o_ref.shape[1]
    half = rows * len(line_refs)
    for p, line_ref in enumerate(line_refs):
        x = line_ref[:, :d].astype(f32)
        o_ref[p * rows : (p + 1) * rows, :] = (x * inverse_norm(x)).astype(bf16)
    tail = jnp.concatenate([line_ref[:, d:] for line_ref in line_refs], axis=0)
    same = lax.broadcasted_iota(i32, (8, LANES), 0) == lax.broadcasted_iota(i32, (8, LANES), 1)
    digits = dot(jnp.where(same, 1.0, 0.0).astype(bf16), tail, 1, 1).astype(bf16)
    o_ref[half:, :] = jnp.concatenate([digits] * (d // half), axis=1)


def merge(lines, d):
    rows = lines[0].shape[0] * len(lines)
    return pl.pallas_call(
        merge_kernel,
        in_specs=[VMEM] * len(lines),
        out_specs=VMEM,
        out_shape=jax.ShapeDtypeStruct((rows + 8, d), bf16),
        compiler_params=params(8),
        cost_estimate=cost(0.01),
        name="merge",
    )(*lines)


def unit_kernel(c_hbm, raw, chat, sem, *, tile):
    steps = c_hbm.shape[0] // tile

    def span(k):
        return pl.ds(pl.multiple_of(k * tile, tile), tile)

    def fetch(k):
        return pltpu.make_async_copy(c_hbm.at[span(k)], raw.at[span(k)], sem.at[k])

    for k in range(steps):
        fetch(k).start()

    def step(k, _):
        fetch(k).wait()
        w = raw[span(k), :].astype(f32)
        chat[span(k), :] = (w * inverse_norm(w)).astype(bf16)
        return 0

    lax.fori_loop(0, steps, step, 0)


def unit_centers(centers, tile=512):
    return pl.pallas_call(
        functools.partial(unit_kernel, tile=tile),
        in_specs=[HBM],
        out_specs=[VMEM] * 2,
        out_shape=[pltpu.VMEM(centers.shape, bf16)] * 2,
        scratch_shapes=[pltpu.SemaphoreType.DMA((centers.shape[0] // tile,))],
        compiler_params=params(12),
        cost_estimate=cost(3),
        name="unit_centers",
    )(in_hbm(centers))


def score_half(base_ref, g_ref, chat, w_ref, st_ref, acc, pck, *, tile):
    n, d = chat.shape
    m = w_ref.shape[1]
    steps = n // tile
    digits = g_ref[m:, :m].astype(f32)
    lab1 = (digits[0:1] * 4096.0 + digits[1:2] * 64.0 + digits[2:3]).astype(i32) - base_ref[0]
    owned = (lab1 >= 0) & (lab1 < n)
    ahead = lax.broadcasted_iota(i32, (m, m), 0) < lax.broadcasted_iota(i32, (m, m), 1)
    mine = jnp.where(owned, 1.0, 0.0)
    rank = dot(jnp.broadcast_to(mine, (8, m)).astype(bf16), jnp.where(ahead, 1.0, 0.0).astype(bf16), 1, 0)
    slot = lax.broadcasted_iota(i32, (SLOTS, m), 0).astype(f32)
    chosen = (slot == rank[0:1, :]) & owned
    held = jnp.sum(jnp.where(chosen, lab1.astype(f32) + 1.0, 0.0), axis=1, keepdims=True).astype(i32) - 1
    count = jnp.sum(mine)

    def span(k):
        return pl.ds(pl.multiple_of(k * tile, tile), tile)

    def score(k, tot, tcs):
        cos = dot(chat[span(k), :], g_ref[:m, :], 1, 1)
        hit = lax.broadcasted_iota(i32, (tile, m), 0) == lab1 - k * tile
        e = jnp.where(hit, 0.0, jnp.exp2(cos * slope2 - shift2))
        w_ref[span(k), :] = e.astype(bf16)
        tot = tot + e.reshape(tile // 8, 8, m).sum(axis=0)
        tcs = tcs + jnp.where(hit, cos, 0.0).reshape(tile // 8, 8, m).sum(axis=0)
        return tot, tcs

    def gather(k):
        hot = lax.broadcasted_iota(i32, (SLOTS, tile), 1) == held - k * tile
        c = chat[span(k), :]
        prod = dot(w_ref[span(k), :], c, 0, 0)
        pick = dot(jnp.where(hot, 1.0, 0.0).astype(bf16), c, 1, 0)
        return prod, pick

    zero = jnp.zeros((8, m), f32)
    tot, tcs = score(0, zero, zero)
    acc[...] = jnp.zeros(acc.shape, f32)

    def step(k, carry):
        tot, tcs, held_sum = carry
        prod, pick = gather(k - 1)
        tot, tcs = score(k, tot, tcs)
        acc[...] += prod
        return tot, tcs, held_sum + pick

    tot, tcs, held_sum = lax.fori_loop(1, steps, step, (tot, tcs, jnp.zeros((SLOTS, d), f32)))
    prod, pick = gather(steps - 1)
    acc[...] += prod
    pck[...] = dot(jnp.where(chosen, 1.0, 0.0).astype(bf16), (held_sum + pick).astype(bf16), 0, 0)

    @pl.when(count > SLOTS)
    def _():
        label = jnp.broadcast_to(lab1, (LANES, m)).T[:, 0:1]
        pck[...] = jnp.zeros(pck.shape, f32)

        def pick_all(k, _):
            hot = lax.broadcasted_iota(i32, (m, LANES), 1) == label - k * LANES
            c = chat[pl.ds(pl.multiple_of(k * LANES, LANES), LANES), :]
            pck[...] += dot(jnp.where(hot, 1.0, 0.0).astype(bf16), c, 1, 0)
            return 0

        lax.fori_loop(0, n // LANES, pick_all, 0)

    texp, _, slope = margin(tcs.sum(axis=0, keepdims=True))
    texp = jnp.where(owned, texp, 0.0)
    slope = jnp.where(owned, slope, 0.0)
    total = (tot.sum(axis=0, keepdims=True) + texp) * (1.0 / logit_scale)
    row8 = lax.broadcasted_iota(i32, (8, m), 0)
    rest = jnp.where(row8 == 3, total, lab1.astype(f32))
    st_ref[...] = jnp.where(row8 == 0, slope, jnp.where(row8 == 1, texp, rest))


def first_kernel(base_ref, g_ref, chat, w_ref, st_ref, pay_ref, acc, pck, *, tile):
    score_half(base_ref, g_ref, chat, w_ref, st_ref, acc, pck, tile=tile)
    blocks, rows = pay_ref.shape[0], pay_ref.shape[1] // 2
    for p in range(blocks):
        pay_ref[p, :rows, :] = acc[p * rows : (p + 1) * rows].astype(bf16)
        pay_ref[p, rows:, :] = pck[p * rows : (p + 1) * rows].astype(bf16)


def second_kernel(
    base_ref, side_ref, x_ref, g_ref, chat, first_ref, firstst_ref, w_ref, st_ref, pay_ref, acc, pck, *, tile
):
    score_half(base_ref, g_ref, chat, w_ref, st_ref, acc, pck, tile=tile)
    blocks, rows = first_ref.shape[0], first_ref.shape[1] // 2
    side, at_x = side_ref[0], x_ref[0]
    mine = pltpu.roll(firstst_ref[...], at_x * rows, 1)[3:4, :]
    theirs = pltpu.roll(st_ref[...], at_x * rows, 1)[3:4, :]
    left = jnp.where(side == 0, mine, theirs)
    right = jnp.where(side == 0, theirs, mine)
    sums = total_rows(jnp.concatenate([left, right], axis=1))
    for p in range(2 * blocks):
        pay_ref[p, 2 * rows :, :] = sums
    for p in range(blocks):
        to = lax.rem(at_x + p, blocks)
        pay_ref[2 * to + side, : 2 * rows, :] = first_ref[p]
        other = 2 * to + 1 - side
        pay_ref[other, :rows, :] = acc[p * rows : (p + 1) * rows].astype(bf16)
        pay_ref[other, rows : 2 * rows, :] = pck[p * rows : (p + 1) * rows].astype(bf16)


def half_shapes(n, m):
    return [pltpu.VMEM((n, m), bf16), jax.ShapeDtypeStruct((8, m), f32)]


def first_scores(base, gathered, chat, blocks, tile=1024):
    n, d = chat.shape
    m = gathered.shape[0] - 8
    w, st = half_shapes(n, m)
    return pl.pallas_call(
        functools.partial(first_kernel, tile=tile),
        in_specs=[SMEM, VMEM, VMEM],
        out_specs=[VMEM] * 3,
        out_shape=[w, st, jax.ShapeDtypeStruct((blocks, 2 * (m // blocks), d), bf16)],
        scratch_shapes=[pltpu.VMEM((m, d), f32)] * 2,
        compiler_params=params(24),
        cost_estimate=cost(6),
        name="first_scores",
    )(base, gathered, chat)


def second_scores(where, gathered, chat, first, stats, tile=1024):
    n, d = chat.shape
    m = gathered.shape[0] - 8
    blocks, rows = first.shape[0], first.shape[1]
    w, st = half_shapes(n, m)
    return pl.pallas_call(
        functools.partial(second_kernel, tile=tile),
        in_specs=[SMEM] * 3 + [VMEM] * 4,
        out_specs=[VMEM] * 3,
        out_shape=[w, st, jax.ShapeDtypeStruct((2 * blocks, rows + 8, d), bf16)],
        scratch_shapes=[pltpu.VMEM((m, d), f32)] * 2,
        compiler_params=params(24),
        cost_estimate=cost(6),
        name="second_scores",
    )(*where, gathered, chat, first, stats)


def middle_kernel(r_ref, o_ref):
    far, rows, d = o_ref.shape
    own = rows // 3
    half = far * own
    sums = r_ref[...].astype(f32).sum(axis=0)
    low = sums[: 2 * half].astype(bf16)
    totals = total_rows(sums[2 * half :].sum(axis=0, keepdims=True))
    for q in range(far):
        o_ref[q, :own, :] = low[q * own : (q + 1) * own]
        o_ref[q, own : 2 * own, :] = low[half + q * own : half + (q + 1) * own]
        o_ref[q, 2 * own :, :] = totals


def middle(received, far, own):
    d = received.shape[2]
    return pl.pallas_call(
        middle_kernel,
        in_specs=[VMEM],
        out_specs=VMEM,
        out_shape=jax.ShapeDtypeStruct((far, 3 * own, d), bf16),
        compiler_params=params(8),
        name="middle",
    )(received)


def grad_kernel(
    side_ref, at_ref, own_ref, r_ref, x_ref, sta_ref, stb_ref, ea_ref, eb_ref, wa_ref, wb_ref, raw, l_hbm, xg_hbm, o_hbm,
    out, xg_ref, l_ref, osem, sem, *, chunk, blocks
):
    n, d = raw.shape
    half = wa_ref.shape[1]
    m = 2 * half
    own = x_ref.shape[0]
    chunks = n // chunk

    def save(k):
        rows = pl.ds(pl.multiple_of(k * chunk, chunk), chunk)
        return pltpu.make_async_copy(out.at[rows], o_hbm.at[rows], osem.at[k])

    side, at_x, own_first = side_ref[0], at_ref[0], own_ref[0]
    sums = r_ref[...].astype(f32).sum(axis=0)
    total = sums[2 * own :].sum(axis=0, keepdims=True)
    back = lax.rem(blocks - at_x, blocks) * (half // blocks)
    both = jnp.broadcast_to(total, (8, m))
    left = 1.0 / pltpu.roll(both[:, :half], back, 1)[0:1, :]
    right = 1.0 / pltpu.roll(both[:, half:], back, 1)[0:1, :]

    def factors(st_ref, scale):
        return st_ref[2:3, :].astype(i32), scale, st_ref[0:1, :] * (st_ref[1:2, :] * scale - logit_scale)

    halves = (
        (ea_ref, wa_ref, *factors(sta_ref, jnp.where(side == 0, left, right))),
        (eb_ref, wb_ref, *factors(stb_ref, jnp.where(side == 0, right, left))),
    )

    x = x_ref[...].astype(f32)
    inv = inverse_norm(x)
    units = x * inv
    unit16 = units.astype(bf16).astype(f32)
    pick = sums[own : 2 * own]
    texp, logit, slope = margin(jnp.sum(unit16 * pick, axis=1, keepdims=True))
    lane = lax.broadcasted_iota(i32, (own, m), 1)
    row = lax.broadcasted_iota(i32, (own, m), 0)
    own_total = jnp.sum(jnp.where(lane == row + own_first, total, 0.0), axis=1, keepdims=True)
    grad = sums[:own] / own_total + (slope * (texp / own_total - logit_scale)) * pick
    xg_ref[...] = inv * (grad - units * jnp.sum(units * grad, axis=1, keepdims=True))
    loss = jnp.log(own_total) + logit_scale - logit
    spread = jnp.where(lane[:, :LANES] == row[:, :LANES], loss, 0.0).sum(axis=0, keepdims=True)
    l_ref[...] = spread[:, :own]

    def step(k, _):
        rows = pl.ds(pl.multiple_of(k * chunk, chunk), chunk)
        row = lax.broadcasted_iota(i32, (chunk, half), 0)
        grad = 0.0
        for e_ref, w_ref, lab, scale, coef in halves:
            share = jnp.where(row == lab - k * chunk, coef, w_ref[rows, :].astype(f32) * scale)
            grad = grad + dot(share.astype(bf16), e_ref[:half, :], 1, 0)
        w = raw[rows, :].astype(f32)
        inv = inverse_norm(w)
        along = jnp.sum(w * grad, axis=1, keepdims=True) * (inv * inv)
        out[rows, :] = inv * (grad - w * along)
        save(k).start()
        return 0

    step(0, 0)
    small = (
        pltpu.make_async_copy(xg_ref, xg_hbm, sem.at[0]),
        pltpu.make_async_copy(l_ref, l_hbm, sem.at[1]),
    )
    for copy in small:
        copy.start()
    lax.fori_loop(1, chunks, step, 0)
    for copy in small:
        copy.wait()
    for k in range(chunks):
        save(k).wait()


def grads(where, received, embeddings, stats, ehats, weights, raw, blocks, chunk=512):
    n, d = raw.shape
    own = embeddings.shape[0]
    return pl.pallas_call(
        functools.partial(grad_kernel, chunk=chunk, blocks=blocks),
        in_specs=[SMEM] * 3 + [VMEM] * 9,
        out_specs=[HBM] * 3,
        out_shape=[
            jax.ShapeDtypeStruct((1, own), f32),
            jax.ShapeDtypeStruct((own, d), f32),
            jax.ShapeDtypeStruct((n, d), f32),
        ],
        scratch_shapes=[
            pltpu.VMEM((n, d), f32),
            pltpu.VMEM((own, d), f32),
            pltpu.VMEM((1, own), f32),
            pltpu.SemaphoreType.DMA((n // chunk,)),
            pltpu.SemaphoreType.DMA((2,)),
        ],
        compiler_params=params(24),
        name="grads",
    )(*where, received, embeddings, *stats, *ehats, *weights, raw)


def exchange(blocks, axis):
    return lax.all_to_all(blocks, axis, 0, 0, tiled=True)


def per_device(embeddings, labels, centers):
    own, d = embeddings.shape
    n = centers.shape[0]
    far, wide = lax.axis_size(FAR), lax.axis_size("x")
    at_x, at_y = lax.axis_index("x"), lax.axis_index("y")
    half = far * wide * own
    base = lax.axis_index(("x", FAR, "y")) * n
    own_first = at_y * half + (at_x * far + lax.axis_index(FAR)) * own
    where = tuple(a.astype(i32)[None] for a in (base, at_y, at_x, own_first))
    embeddings, where = lax.optimization_barrier((embeddings, where))
    base, side, at_x, own_first = where
    line = exchange(pack(embeddings, labels, far), FAR).reshape(far * own, d + LANES)
    lines = [line] + [
        lax.ppermute(line, "x", [(i, (i - k) % wide) for i in range(wide)]) for k in range(1, wide)
    ]
    raw, chat = unit_centers(centers)
    first = merge(lines, d)
    second = lax.ppermute(first, "y", [(0, 1), (1, 0)])
    wa, sta, pay = first_scores(base, first, chat, wide)
    wb, stb, pay = second_scores((base, side, at_x), second, chat, pay, sta)
    received = exchange(middle(exchange(pay, NEAR), far, own), FAR)
    losses, emb_grad, center_grad = grads(
        (side, at_x, own_first), received, embeddings, (sta, stb), (first, second), (wa, wb), raw, wide
    )
    return (losses.reshape(own), emb_grad, center_grad)


def solution(mesh):
    dp = mesh.shape["dp"]
    fine = Mesh(mesh.devices.reshape(4, mesh.shape["cls"] // 8, 2, dp), ("x", FAR, "y", "dp"))
    rows = ("dp", "x", FAR, "y")
    in_specs = (P(rows, None), P(rows), P(rows, None))
    out_specs = (P(rows), P(rows, None), P(rows, None))
    return jax.shard_map(
        per_device, mesh=fine, in_specs=in_specs, out_specs=out_specs, check_vma=False
    )
```

```python
import functools
import math

import jax
import jax.numpy as jnp
from jax import lax
from jax.experimental import pallas as pl
from jax.experimental.pallas import tpu as pltpu
from jax.sharding import Mesh
from jax.sharding import PartitionSpec as P

logit_scale = 64.0
margin_cosine = math.cos(0.5)
margin_sine = math.sin(0.5)
sine_soften = 0.04
norm_eps = 1e-06

slope2 = logit_scale * math.log2(math.e)
shift2 = slope2 - math.log2(logit_scale)


LANES = 128
CAP = 16
MIB = 1024 * 1024
NEAR = ("x", "y")
FAR = "z"
f32, bf16, i32 = jnp.float32, jnp.bfloat16, jnp.int32
VMEM = pl.BlockSpec(memory_space=pltpu.VMEM)
SMEM = pl.BlockSpec(memory_space=pltpu.SMEM)
HBM = pl.BlockSpec(memory_space=pltpu.HBM)


def params(mib):
    return pltpu.CompilerParams(vmem_limit_bytes=mib * MIB)


def cost(gflops):
    return pl.CostEstimate(flops=int(gflops * 1e9), bytes_accessed=8 * MIB, transcendentals=0)


def in_hbm(x):
    return pltpu.with_memory_space_constraint(x, pltpu.HBM)


def dot(a, b, ca, cb):
    return lax.dot_general(a, b, (((ca,), (cb,)), ((), ())), preferred_element_type=f32)


def inverse_norm(x):
    return lax.rsqrt(jnp.sum(x * x, axis=1, keepdims=True) + norm_eps)


def margin(cosine):
    sine = jnp.sqrt(1.0 + sine_soften - cosine * cosine)
    shifted = cosine * margin_cosine - sine * margin_sine
    slope = margin_cosine + margin_sine * cosine / sine
    return jnp.exp2(slope2 * shifted - shift2), logit_scale * shifted, slope


def total_rows(total):
    row8 = lax.broadcasted_iota(i32, (8, total.shape[1]), 0)
    out = jnp.zeros(row8.shape, f32)
    rest = total
    for r in range(3):
        part = rest.astype(bf16).astype(f32)
        out = jnp.where(row8 == r, part, out)
        rest = rest - part
    return out.astype(bf16)


def pack_kernel(x_hbm, lab_hbm, o_ref, x_ref, lab_ref, sem):
    rows, d = x_ref.shape
    copies = (
        pltpu.make_async_copy(lab_hbm, lab_ref, sem.at[0]),
        pltpu.make_async_copy(x_hbm, x_ref, sem.at[1]),
    )
    for copy in copies:
        copy.start()
    for copy in copies:
        copy.wait()
    row = lax.broadcasted_iota(i32, (rows, LANES), 0)
    lane = lax.broadcasted_iota(i32, (rows, LANES), 1)
    lab = jnp.zeros((rows, LANES), i32)
    for j in range(rows):
        lab = jnp.where(row == j, lab_ref[j], lab)
    digit = jnp.where(lane == 0, lab >> 12, jnp.where(lane == 1, (lab >> 6) & 63, lab & 63))
    digit = jnp.where(lane < 3, digit, 0).astype(f32).astype(bf16)
    for p in range(o_ref.shape[0]):
        o_ref[p, :, :d] = x_ref[...]
        o_ref[p, :, d:] = digit


def pack(embeddings, labels, peers):
    rows, d = embeddings.shape
    return pl.pallas_call(
        pack_kernel,
        in_specs=[HBM, HBM],
        out_specs=VMEM,
        out_shape=jax.ShapeDtypeStruct((peers, rows, d + LANES), bf16),
        scratch_shapes=[
            pltpu.VMEM((rows, d), bf16),
            pltpu.SMEM((rows,), i32),
            pltpu.SemaphoreType.DMA((2,)),
        ],
        compiler_params=params(4),
        name="pack",
    )(in_hbm(embeddings), in_hbm(labels))


def digit_weights(shape):
    lane = lax.broadcasted_iota(i32, shape, 1)
    return jnp.where(lane == 0, 4096.0, jnp.where(lane == 1, 64.0, jnp.where(lane == 2, 1.0, 0.0)))


def merge_kernel(*refs):
    *line_refs, o_ref = refs
    rows, d = line_refs[0].shape[0], o_ref.shape[1]
    half = rows * len(line_refs)
    for p, line_ref in enumerate(line_refs):
        x = line_ref[:, :d].astype(f32)
        o_ref[p * rows : (p + 1) * rows, :] = (x * inverse_norm(x)).astype(bf16)
    tail = jnp.concatenate([line_ref[:, d:] for line_ref in line_refs], axis=0)
    same = lax.broadcasted_iota(i32, (8, LANES), 0) == lax.broadcasted_iota(i32, (8, LANES), 1)
    digits = dot(jnp.where(same, 1.0, 0.0).astype(bf16), tail, 1, 1).astype(bf16)
    o_ref[half:, :] = jnp.concatenate([digits] * (d // half), axis=1)


def merge(lines, d):
    rows = lines[0].shape[0] * len(lines)
    return pl.pallas_call(
        merge_kernel,
        in_specs=[VMEM] * len(lines),
        out_specs=VMEM,
        out_shape=jax.ShapeDtypeStruct((rows + 8, d), bf16),
        compiler_params=params(8),
        cost_estimate=cost(0.01),
        name="merge",
    )(*lines)


def unit_kernel(c_hbm, raw, chat, sem, *, tile):
    steps = c_hbm.shape[0] // tile

    def span(k):
        return pl.ds(pl.multiple_of(k * tile, tile), tile)

    def fetch(k):
        return pltpu.make_async_copy(c_hbm.at[span(k)], raw.at[span(k)], sem.at[k])

    for k in range(steps):
        fetch(k).start()

    def step(k, _):
        fetch(k).wait()
        w = raw[span(k), :].astype(f32)
        chat[span(k), :] = (w * inverse_norm(w)).astype(bf16)
        return 0

    lax.fori_loop(0, steps, step, 0)


def unit_centers(centers, tile=512):
    return pl.pallas_call(
        functools.partial(unit_kernel, tile=tile),
        in_specs=[HBM],
        out_specs=[VMEM] * 2,
        out_shape=[pltpu.VMEM(centers.shape, bf16)] * 2,
        scratch_shapes=[pltpu.SemaphoreType.DMA((centers.shape[0] // tile,))],
        compiler_params=params(12),
        cost_estimate=cost(3),
        name="unit_centers",
    )(in_hbm(centers))


def score_half(base_ref, g_ref, chat, w_ref, st_ref, acc, pck, rows, *, tile):
    n, d = chat.shape
    m = w_ref.shape[1]
    steps = n // tile
    digits = g_ref[m:, :m].astype(f32)
    lab1 = (digits[0:1] * 4096.0 + digits[1:2] * 64.0 + digits[2:3]).astype(i32) - base_ref[0]
    owned = (lab1 >= 0) & (lab1 < n)
    shift = rows.bit_length() - 1
    before, after = (lax.broadcasted_iota(i32, (m, m), a) for a in (0, 1))
    ahead = (before < after) & ((before >> shift) == (after >> shift))
    mine = jnp.broadcast_to(jnp.where(owned, 1.0, 0.0), (8, m)).astype(bf16)
    rank = dot(mine, jnp.where(ahead, 1.0, 0.0).astype(bf16), 1, 0)[0:1, :].astype(i32)
    block = lax.broadcasted_iota(i32, (1, m), 1) >> shift
    slots = (m // rows) * CAP
    place = jnp.where(owned & (rank < CAP), block * CAP + rank, -1)
    chosen = lax.broadcasted_iota(i32, (slots, m), 0) == place
    held = jnp.sum(jnp.where(chosen, lab1.astype(f32) + 1.0, 0.0), axis=1, keepdims=True).astype(i32) - 1

    def span(k):
        return pl.ds(pl.multiple_of(k * tile, tile), tile)

    def score(k, tot, tcs):
        cos = dot(chat[span(k), :], g_ref[:m, :], 1, 1)
        hit = lax.broadcasted_iota(i32, (tile, m), 0) == lab1 - k * tile
        e = jnp.where(hit, 0.0, jnp.exp2(cos * slope2 - shift2))
        w_ref[span(k), :] = e.astype(bf16)
        tot = tot + e.reshape(tile // 8, 8, m).sum(axis=0)
        tcs = tcs + jnp.where(hit, cos, 0.0).reshape(tile // 8, 8, m).sum(axis=0)
        return tot, tcs

    def gather(k):
        hot = lax.broadcasted_iota(i32, (slots, tile), 1) == held - k * tile
        c = chat[span(k), :]
        prod = dot(w_ref[span(k), :], c, 0, 0)
        pick = dot(jnp.where(hot, 1.0, 0.0).astype(bf16), c, 1, 0)
        return prod, pick

    zero = jnp.zeros((8, m), f32)
    tot, tcs = score(0, zero, zero)
    acc[...] = jnp.zeros(acc.shape, f32)

    def step(k, carry):
        tot, tcs, held_sum = carry
        prod, pick = gather(k - 1)
        tot, tcs = score(k, tot, tcs)
        acc[...] += prod
        return tot, tcs, held_sum + pick

    tot, tcs, held_sum = lax.fori_loop(1, steps, step, (tot, tcs, jnp.zeros((slots, d), f32)))
    prod, pick = gather(steps - 1)
    acc[...] += prod
    pck[...] = held_sum + pick
    texp, _, slope = margin(tcs.sum(axis=0, keepdims=True))
    texp = jnp.where(owned, texp, 0.0)
    slope = jnp.where(owned, slope, 0.0)
    total = (tot.sum(axis=0, keepdims=True) + texp) * (1.0 / logit_scale)
    row8 = lax.broadcasted_iota(i32, (8, m), 0)
    rest = jnp.where(row8 == 3, total, lab1.astype(f32))
    st_ref[...] = jnp.where(row8 == 0, slope, jnp.where(row8 == 1, texp, rest))


def first_kernel(base_ref, g_ref, chat, w_ref, st_ref, pay_ref, acc, pck, *, tile):
    blocks, rows = pay_ref.shape[0], pay_ref.shape[1] - CAP
    score_half(base_ref, g_ref, chat, w_ref, st_ref, acc, pck, rows, tile=tile)
    for p in range(blocks):
        pay_ref[p, :rows, :] = acc[p * rows : (p + 1) * rows].astype(bf16)
        pay_ref[p, rows:, :] = pck[p * CAP : (p + 1) * CAP].astype(bf16)


def most(local, base, n, shards, rows):
    m = local.shape[1]
    shift, wide = rows.bit_length() - 1, n.bit_length() - 1
    owner = (local.astype(i32) + base) >> wide
    hot = lax.broadcasted_iota(i32, (shards, m), 0) == owner
    block = (lax.broadcasted_iota(i32, (m, LANES), 0) >> shift) == lax.broadcasted_iota(i32, (m, LANES), 1)
    one = lambda a: jnp.where(a, 1.0, 0.0).astype(bf16)
    return jnp.max(dot(one(hot), one(block), 1, 0))


def second_kernel(
    base_ref, side_ref, x_ref, g_ref, chat, first_ref, firstst_ref, w_ref, st_ref, pay_ref, full_ref, acc, pck, *, tile, shards
):
    blocks, rows = first_ref.shape[0], first_ref.shape[1] - CAP
    score_half(base_ref, g_ref, chat, w_ref, st_ref, acc, pck, rows, tile=tile)
    count = functools.partial(most, base=base_ref[0], n=chat.shape[0], shards=shards, rows=rows)
    crowded = jnp.maximum(count(firstst_ref[2:3, :]), count(st_ref[2:3, :]))
    full_ref[0] = (crowded > CAP).astype(i32)
    side, at_x = side_ref[0], x_ref[0]
    mine = pltpu.roll(firstst_ref[...], at_x * rows, 1)[3:4, :]
    theirs = pltpu.roll(st_ref[...], at_x * rows, 1)[3:4, :]
    left = jnp.where(side == 0, mine, theirs)
    right = jnp.where(side == 0, theirs, mine)
    sums = total_rows(jnp.concatenate([left, right], axis=1))
    for p in range(2 * blocks):
        pay_ref[p, rows + CAP :, :] = sums
    for p in range(blocks):
        to = lax.rem(at_x + p, blocks)
        pay_ref[2 * to + side, : rows + CAP, :] = first_ref[p]
        other = 2 * to + 1 - side
        pay_ref[other, :rows, :] = acc[p * rows : (p + 1) * rows].astype(bf16)
        pay_ref[other, rows : rows + CAP, :] = pck[p * CAP : (p + 1) * CAP].astype(bf16)


def half_shapes(n, m):
    return [pltpu.VMEM((n, m), bf16), jax.ShapeDtypeStruct((8, m), f32)]


def first_scores(base, gathered, chat, blocks, tile=1024):
    n, d = chat.shape
    m = gathered.shape[0] - 8
    w, st = half_shapes(n, m)
    return pl.pallas_call(
        functools.partial(first_kernel, tile=tile),
        in_specs=[SMEM, VMEM, VMEM],
        out_specs=[VMEM] * 3,
        out_shape=[w, st, jax.ShapeDtypeStruct((blocks, m // blocks + CAP, d), bf16)],
        scratch_shapes=[pltpu.VMEM((m, d), f32), pltpu.VMEM((blocks * CAP, d), f32)],
        compiler_params=params(24),
        cost_estimate=cost(6),
        name="first_scores",
    )(base, gathered, chat)


def second_scores(where, gathered, chat, first, stats, shards, tile=1024):
    n, d = chat.shape
    m = gathered.shape[0] - 8
    blocks, rows = first.shape[0], first.shape[1]
    w, st = half_shapes(n, m)
    return pl.pallas_call(
        functools.partial(second_kernel, tile=tile, shards=shards),
        in_specs=[SMEM] * 3 + [VMEM] * 4,
        out_specs=[VMEM] * 3 + [SMEM],
        out_shape=[
            w,
            st,
            jax.ShapeDtypeStruct((2 * blocks, rows + 8, d), bf16),
            jax.ShapeDtypeStruct((1,), i32),
        ],
        scratch_shapes=[pltpu.VMEM((m, d), f32), pltpu.VMEM((blocks * CAP, d), f32)],
        compiler_params=params(24),
        cost_estimate=cost(6),
        name="second_scores",
    )(*where, gathered, chat, first, stats)


def middle_kernel(far_ref, line_ref, r_ref, o_ref, *, n):
    far, rows, d = o_ref.shape
    senders = r_ref.shape[0]
    own = rows // 3
    half = far * own
    low = r_ref[:, :half, :].astype(f32).sum(axis=0).astype(bf16)
    label = jnp.sum(line_ref[:, d:].astype(f32) * digit_weights((1, LANES)), axis=1, keepdims=True)
    lane = lax.broadcasted_iota(i32, (1, senders * CAP), 1)
    shift = CAP.bit_length() - 1
    sender, place = lane >> shift, lane & (CAP - 1)
    start = ((((sender >> 1) * far + far_ref[0]) * 2 + (sender & 1)) * n).astype(f32)
    owned = (label >= start) & (label < start + n)
    before = lax.broadcasted_iota(i32, (half, half), 1) < lax.broadcasted_iota(i32, (half, half), 0)
    one = lambda a: jnp.where(a, 1.0, 0.0).astype(bf16)
    rank = dot(one(before), one(owned), 1, 0)
    spread = one(owned & (rank == place.astype(f32)))
    held = jnp.concatenate([r_ref[q, half : half + CAP, :] for q in range(senders)], axis=0)
    pick = dot(spread, held, 1, 0).astype(bf16)
    totals = total_rows(r_ref[:, half + CAP :, :].astype(f32).sum(axis=0).sum(axis=0, keepdims=True))
    for q in range(far):
        o_ref[q, :own, :] = low[q * own : (q + 1) * own]
        o_ref[q, own : 2 * own, :] = pick[q * own : (q + 1) * own]
        o_ref[q, 2 * own :, :] = totals


def middle(at_far, line, received, far, own, n):
    d = received.shape[2]
    return pl.pallas_call(
        functools.partial(middle_kernel, n=n),
        in_specs=[SMEM, VMEM, VMEM],
        out_specs=VMEM,
        out_shape=jax.ShapeDtypeStruct((far, 3 * own, d), bf16),
        compiler_params=params(8),
        name="middle",
    )(at_far, line, received)


def grad_kernel(
    side_ref, at_ref, own_ref, full_ref, r_ref, x_ref, sta_ref, stb_ref, ea_ref, eb_ref, wa_ref, wb_ref, raw, l_hbm, xg_hbm, o_hbm, still_ref,
    out, xg_ref, l_ref, osem, sem, *, chunk, blocks
):
    n, d = raw.shape
    half = wa_ref.shape[1]
    m = 2 * half
    own = x_ref.shape[0]
    chunks = n // chunk

    def save(k):
        rows = pl.ds(pl.multiple_of(k * chunk, chunk), chunk)
        return pltpu.make_async_copy(out.at[rows], o_hbm.at[rows], osem.at[k])

    side, at_x, own_first = side_ref[0], at_ref[0], own_ref[0]
    still_ref[0] = full_ref[0]
    sums = r_ref[...].astype(f32).sum(axis=0)
    total = sums[2 * own :].sum(axis=0, keepdims=True)
    back = lax.rem(blocks - at_x, blocks) * (half // blocks)
    both = jnp.broadcast_to(total, (8, m))
    left = 1.0 / pltpu.roll(both[:, :half], back, 1)[0:1, :]
    right = 1.0 / pltpu.roll(both[:, half:], back, 1)[0:1, :]

    def factors(st_ref, scale):
        return st_ref[2:3, :].astype(i32), scale, st_ref[0:1, :] * (st_ref[1:2, :] * scale - logit_scale)

    halves = (
        (ea_ref, wa_ref, *factors(sta_ref, jnp.where(side == 0, left, right))),
        (eb_ref, wb_ref, *factors(stb_ref, jnp.where(side == 0, right, left))),
    )

    x = x_ref[...].astype(f32)
    inv = inverse_norm(x)
    units = x * inv
    unit16 = units.astype(bf16).astype(f32)
    pick = sums[own : 2 * own]
    texp, logit, slope = margin(jnp.sum(unit16 * pick, axis=1, keepdims=True))
    lane = lax.broadcasted_iota(i32, (own, m), 1)
    row = lax.broadcasted_iota(i32, (own, m), 0)
    own_total = jnp.sum(jnp.where(lane == row + own_first, total, 0.0), axis=1, keepdims=True)
    grad = sums[:own] / own_total + (slope * (texp / own_total - logit_scale)) * pick
    xg_ref[...] = inv * (grad - units * jnp.sum(units * grad, axis=1, keepdims=True))
    loss = jnp.log(own_total) + logit_scale - logit
    spread = jnp.where(lane[:, :LANES] == row[:, :LANES], loss, 0.0).sum(axis=0, keepdims=True)
    l_ref[...] = spread[:, :own]

    def step(k, _):
        rows = pl.ds(pl.multiple_of(k * chunk, chunk), chunk)
        row = lax.broadcasted_iota(i32, (chunk, half), 0)
        grad = 0.0
        for e_ref, w_ref, lab, scale, coef in halves:
            share = jnp.where(row == lab - k * chunk, coef, w_ref[rows, :].astype(f32) * scale)
            grad = grad + dot(share.astype(bf16), e_ref[:half, :], 1, 0)
        w = raw[rows, :].astype(f32)
        inv = inverse_norm(w)
        along = jnp.sum(w * grad, axis=1, keepdims=True) * (inv * inv)
        out[rows, :] = inv * (grad - w * along)
        save(k).start()
        return 0

    step(0, 0)
    small = (
        pltpu.make_async_copy(xg_ref, xg_hbm, sem.at[0]),
        pltpu.make_async_copy(l_ref, l_hbm, sem.at[1]),
    )
    for copy in small:
        copy.start()
    lax.fori_loop(1, chunks, step, 0)
    for copy in small:
        copy.wait()
    for k in range(chunks):
        save(k).wait()


def grads(where, received, embeddings, stats, ehats, weights, raw, blocks, chunk=512):
    n, d = raw.shape
    own = embeddings.shape[0]
    return pl.pallas_call(
        functools.partial(grad_kernel, chunk=chunk, blocks=blocks),
        in_specs=[SMEM] * 4 + [VMEM] * 9,
        out_specs=[HBM] * 3 + [SMEM],
        out_shape=[
            jax.ShapeDtypeStruct((1, own), f32),
            jax.ShapeDtypeStruct((own, d), f32),
            jax.ShapeDtypeStruct((n, d), f32),
            jax.ShapeDtypeStruct((1,), i32),
        ],
        scratch_shapes=[
            pltpu.VMEM((n, d), f32),
            pltpu.VMEM((own, d), f32),
            pltpu.VMEM((1, own), f32),
            pltpu.SemaphoreType.DMA((n // chunk,)),
            pltpu.SemaphoreType.DMA((2,)),
        ],
        compiler_params=params(24),
        name="grads",
    )(*where, received, embeddings, *stats, *ehats, *weights, raw)


def exchange(blocks, axis):
    return lax.all_to_all(blocks, axis, 0, 0, tiled=True)


def per_device(embeddings, labels, centers):
    own, d = embeddings.shape
    n = centers.shape[0]
    far, wide = lax.axis_size(FAR), lax.axis_size("x")
    at_x, at_y = lax.axis_index("x"), lax.axis_index("y")
    half = far * wide * own
    at_far = lax.axis_index(FAR)
    base = lax.axis_index(("x", FAR, "y")) * n
    own_first = at_y * half + (at_x * far + at_far) * own
    where = tuple(a.astype(i32)[None] for a in (base, at_y, at_x, own_first, at_far))
    embeddings, where = lax.optimization_barrier((embeddings, where))
    base, side, at_x, own_first, at_far = where
    line = exchange(pack(embeddings, labels, far), FAR).reshape(far * own, d + LANES)
    lines = [line] + [
        lax.ppermute(line, "x", [(i, (i - k) % wide) for i in range(wide)]) for k in range(1, wide)
    ]
    raw, chat = unit_centers(centers)
    first = merge(lines, d)
    second = lax.ppermute(first, "y", [(0, 1), (1, 0)])
    wa, sta, pay = first_scores(base, first, chat, wide)
    wb, stb, pay, crowded = second_scores((base, side, at_x), second, chat, pay, sta, far * wide * 2)
    received = exchange(middle(at_far, line, exchange(pay, NEAR), far, own, n), FAR)
    losses, emb_grad, center_grad, crowded = grads(
        (side, at_x, own_first, crowded), received, embeddings, (sta, stb), (first, second), (wa, wb), raw, wide
    )
    losses, emb_grad = lax.cond(
        crowded[0] > 0,
        lambda loss, grad, late, x, y, w: dense_examples(x, y + jnp.minimum(late, 0), w),
        lambda loss, grad, *_: (loss, grad),
        losses, emb_grad, crowded, embeddings, labels, centers,
    )
    return (losses.reshape(own), emb_grad, center_grad)


def dense_examples(embeddings, labels, centers):
    own, d = embeddings.shape
    n = centers.shape[0]
    cls = ("x", FAR, "y")
    peers = lax.axis_size(cls)

    def alone(blocks, *others):
        blocks, others = lax.optimization_barrier((blocks, others))
        return lax.optimization_barrier((exchange(blocks, cls), *others))

    def copies(a):
        return jnp.broadcast_to(a[None], (peers, *a.shape))

    index = lax.axis_index(cls)
    x, w = embeddings.astype(f32), centers.astype(f32)
    inv = inverse_norm(x)
    units = x * inv
    chat = (w * inverse_norm(w)).astype(bf16)
    label, units, inv, chat, index = alone(copies(labels), units, inv, chat, index)
    rows, label, units, inv, chat, index = alone(copies(units.astype(bf16)), label, units, inv, chat, index)
    rows = rows.reshape(-1, d)
    label = label.reshape(-1) - index * n
    hot = label[:, None] == jnp.arange(n)[None]
    cosine = dot(rows, chat, 1, 1)
    picked = jnp.sum(jnp.where(hot, cosine, 0.0), axis=1)
    texp, logit, slope = margin(picked)
    owned = (label >= 0) & (label < n)
    texp, logit, slope = (jnp.where(owned, a, 0.0) for a in (texp, logit, slope))
    weight = jnp.where(hot, 0.0, jnp.exp2(cosine * slope2 - shift2))
    total = (weight.sum(axis=1) + texp) / logit_scale
    prod = dot(weight.astype(bf16), chat, 1, 0)
    pick = dot(hot.astype(bf16), chat, 1, 0)
    sums, prod, pick, slope, texp, units, inv, index = alone(
        copies(jnp.stack([total, logit])), prod, pick, slope, texp, units, inv, index
    )
    sums = sums.sum(axis=0)
    total = sums[0]
    rows = prod / total[:, None] + (slope * (texp / total - logit_scale))[:, None] * pick
    grad, sums, units, inv, index = alone(
        rows.astype(bf16).reshape(peers, own, d), sums, units, inv, index
    )
    grad = grad.astype(f32).sum(axis=0)
    mine = lax.dynamic_slice_in_dim(sums, index * own, own, 1)
    loss = jnp.log(mine[0]) + logit_scale - mine[1]
    return loss[None], inv * (grad - units * jnp.sum(units * grad, axis=1, keepdims=True))


def solution(mesh):
    dp = mesh.shape["dp"]
    fine = Mesh(mesh.devices.reshape(4, mesh.shape["cls"] // 8, 2, dp), ("x", FAR, "y", "dp"))
    rows = ("dp", "x", FAR, "y")
    in_specs = (P(rows, None), P(rows), P(rows, None))
    out_specs = (P(rows), P(rows, None), P(rows, None))
    return jax.shard_map(
        per_device, mesh=fine, in_specs=in_specs, out_specs=out_specs, check_vma=False
    )
```

```python
import functools
import math

import jax
import jax.numpy as jnp
from jax import lax
from jax.experimental import pallas as pl
from jax.experimental.pallas import tpu as pltpu
from jax.sharding import Mesh
from jax.sharding import PartitionSpec as P

logit_scale = 64.0
margin_cosine = math.cos(0.5)
margin_sine = math.sin(0.5)
sine_soften = 0.04
norm_eps = 1e-06

slope2 = logit_scale * math.log2(math.e)
shift2 = slope2 - math.log2(logit_scale)


LANES = 128
CAP = 16
MIB = 1024 * 1024
NEAR = ("x", "y")
FAR = "z"
f32, bf16, i32 = jnp.float32, jnp.bfloat16, jnp.int32
VMEM = pl.BlockSpec(memory_space=pltpu.VMEM)
SMEM = pl.BlockSpec(memory_space=pltpu.SMEM)
HBM = pl.BlockSpec(memory_space=pltpu.HBM)


def params(mib):
    return pltpu.CompilerParams(vmem_limit_bytes=mib * MIB)


def cost(gflops):
    return pl.CostEstimate(flops=int(gflops * 1e9), bytes_accessed=8 * MIB, transcendentals=0)


def in_hbm(x):
    return pltpu.with_memory_space_constraint(x, pltpu.HBM)


def dot(a, b, ca, cb):
    return lax.dot_general(a, b, (((ca,), (cb,)), ((), ())), preferred_element_type=f32)


def inverse_norm(x):
    return lax.rsqrt(jnp.sum(x * x, axis=1, keepdims=True) + norm_eps)


def margin(cosine):
    sine = jnp.sqrt(1.0 + sine_soften - cosine * cosine)
    shifted = cosine * margin_cosine - sine * margin_sine
    slope = margin_cosine + margin_sine * cosine / sine
    return jnp.exp2(slope2 * shifted - shift2), logit_scale * shifted, slope


def total_rows(total):
    row8 = lax.broadcasted_iota(i32, (8, total.shape[1]), 0)
    out = jnp.zeros(row8.shape, f32)
    rest = total
    for r in range(3):
        part = rest.astype(bf16).astype(f32)
        out = jnp.where(row8 == r, part, out)
        rest = rest - part
    return out.astype(bf16)


def pack_kernel(x_hbm, lab_hbm, o_ref, x_ref, lab_ref, sem):
    rows, d = x_ref.shape
    copies = (
        pltpu.make_async_copy(lab_hbm, lab_ref, sem.at[0]),
        pltpu.make_async_copy(x_hbm, x_ref, sem.at[1]),
    )
    for copy in copies:
        copy.start()
    for copy in copies:
        copy.wait()
    row = lax.broadcasted_iota(i32, (rows, LANES), 0)
    lane = lax.broadcasted_iota(i32, (rows, LANES), 1)
    lab = jnp.zeros((rows, LANES), i32)
    for j in range(rows):
        lab = jnp.where(row == j, lab_ref[j], lab)
    digit = jnp.where(lane == 0, lab >> 12, jnp.where(lane == 1, (lab >> 6) & 63, lab & 63))
    digit = jnp.where(lane < 3, digit, 0).astype(f32).astype(bf16)
    for p in range(o_ref.shape[0]):
        o_ref[p, :, :d] = x_ref[...]
        o_ref[p, :, d:] = digit


def pack(embeddings, labels, peers):
    rows, d = embeddings.shape
    return pl.pallas_call(
        pack_kernel,
        in_specs=[HBM, HBM],
        out_specs=VMEM,
        out_shape=jax.ShapeDtypeStruct((peers, rows, d + LANES), bf16),
        scratch_shapes=[
            pltpu.VMEM((rows, d), bf16),
            pltpu.SMEM((rows,), i32),
            pltpu.SemaphoreType.DMA((2,)),
        ],
        compiler_params=params(4),
        name="pack",
    )(in_hbm(embeddings), in_hbm(labels))


def digit_weights(shape):
    lane = lax.broadcasted_iota(i32, shape, 1)
    return jnp.where(lane == 0, 4096.0, jnp.where(lane == 1, 64.0, jnp.where(lane == 2, 1.0, 0.0)))


def merge_kernel(*refs):
    *line_refs, o_ref = refs
    rows, d = line_refs[0].shape[0], o_ref.shape[1]
    half = rows * len(line_refs)
    for p, line_ref in enumerate(line_refs):
        x = line_ref[:, :d].astype(f32)
        o_ref[p * rows : (p + 1) * rows, :] = (x * inverse_norm(x)).astype(bf16)
    tail = jnp.concatenate([line_ref[:, d:] for line_ref in line_refs], axis=0)
    same = lax.broadcasted_iota(i32, (8, LANES), 0) == lax.broadcasted_iota(i32, (8, LANES), 1)
    digits = dot(jnp.where(same, 1.0, 0.0).astype(bf16), tail, 1, 1).astype(bf16)
    o_ref[half:, :] = jnp.concatenate([digits] * (d // half), axis=1)


def merge(lines, d):
    rows = lines[0].shape[0] * len(lines)
    return pl.pallas_call(
        merge_kernel,
        in_specs=[VMEM] * len(lines),
        out_specs=VMEM,
        out_shape=jax.ShapeDtypeStruct((rows + 8, d), bf16),
        compiler_params=params(8),
        cost_estimate=cost(0.01),
        name="merge",
    )(*lines)


def unit_kernel(c_hbm, raw, chat, sem, *, tile):
    steps = c_hbm.shape[0] // tile

    def span(k):
        return pl.ds(pl.multiple_of(k * tile, tile), tile)

    def fetch(k):
        return pltpu.make_async_copy(c_hbm.at[span(k)], raw.at[span(k)], sem.at[k])

    for k in range(steps):
        fetch(k).start()

    def step(k, _):
        fetch(k).wait()
        w = raw[span(k), :].astype(f32)
        chat[span(k), :] = (w * inverse_norm(w)).astype(bf16)
        return 0

    lax.fori_loop(0, steps, step, 0)


def unit_centers(centers, tile=512):
    return pl.pallas_call(
        functools.partial(unit_kernel, tile=tile),
        in_specs=[HBM],
        out_specs=[VMEM] * 2,
        out_shape=[pltpu.VMEM(centers.shape, bf16)] * 2,
        scratch_shapes=[pltpu.SemaphoreType.DMA((centers.shape[0] // tile,))],
        compiler_params=params(12),
        cost_estimate=cost(3),
        name="unit_centers",
    )(in_hbm(centers))


def score_half(base_ref, g_ref, chat, w_ref, st_ref, acc, pck, rows, *, tile):
    n, d = chat.shape
    m = w_ref.shape[1]
    steps = n // tile
    digits = g_ref[m:, :m].astype(f32)
    lab1 = (digits[0:1] * 4096.0 + digits[1:2] * 64.0 + digits[2:3]).astype(i32) - base_ref[0]
    owned = (lab1 >= 0) & (lab1 < n)
    shift = rows.bit_length() - 1
    before, after = (lax.broadcasted_iota(i32, (m, m), a) for a in (0, 1))
    ahead = (before < after) & ((before >> shift) == (after >> shift))
    mine = jnp.broadcast_to(jnp.where(owned, 1.0, 0.0), (8, m)).astype(bf16)
    rank = dot(mine, jnp.where(ahead, 1.0, 0.0).astype(bf16), 1, 0)[0:1, :].astype(i32)
    block = lax.broadcasted_iota(i32, (1, m), 1) >> shift
    slots = (m // rows) * CAP
    place = jnp.where(owned & (rank < CAP), block * CAP + rank, -1)
    chosen = lax.broadcasted_iota(i32, (slots, m), 0) == place
    held = jnp.sum(jnp.where(chosen, lab1.astype(f32) + 1.0, 0.0), axis=1, keepdims=True).astype(i32) - 1

    def span(k):
        return pl.ds(pl.multiple_of(k * tile, tile), tile)

    def score(k, tot, tcs):
        cos = dot(chat[span(k), :], g_ref[:m, :], 1, 1)
        hit = lax.broadcasted_iota(i32, (tile, m), 0) == lab1 - k * tile
        e = jnp.where(hit, 0.0, jnp.exp2(cos * slope2 - shift2))
        w_ref[span(k), :] = e.astype(bf16)
        tot = tot + e.reshape(tile // 8, 8, m).sum(axis=0)
        tcs = tcs + jnp.where(hit, cos, 0.0).reshape(tile // 8, 8, m).sum(axis=0)
        return tot, tcs

    def gather(k):
        hot = lax.broadcasted_iota(i32, (slots, tile), 1) == held - k * tile
        c = chat[span(k), :]
        prod = dot(w_ref[span(k), :], c, 0, 0)
        pick = dot(jnp.where(hot, 1.0, 0.0).astype(bf16), c, 1, 0)
        return prod, pick

    zero = jnp.zeros((8, m), f32)
    tot, tcs = score(0, zero, zero)
    acc[...] = jnp.zeros(acc.shape, f32)

    def step(k, carry):
        tot, tcs, held_sum = carry
        prod, pick = gather(k - 1)
        tot, tcs = score(k, tot, tcs)
        acc[...] += prod
        return tot, tcs, held_sum + pick

    tot, tcs, held_sum = lax.fori_loop(1, steps, step, (tot, tcs, jnp.zeros((slots, d), f32)))
    prod, pick = gather(steps - 1)
    acc[...] += prod
    pck[...] = held_sum + pick
    texp, _, slope = margin(tcs.sum(axis=0, keepdims=True))
    texp = jnp.where(owned, texp, 0.0)
    slope = jnp.where(owned, slope, 0.0)
    total = (tot.sum(axis=0, keepdims=True) + texp) * (1.0 / logit_scale)
    row8 = lax.broadcasted_iota(i32, (8, m), 0)
    rest = jnp.where(row8 == 3, total, lab1.astype(f32))
    st_ref[...] = jnp.where(row8 == 0, slope, jnp.where(row8 == 1, texp, rest))


def first_kernel(base_ref, g_ref, chat, w_ref, st_ref, pay_ref, acc, pck, *, tile):
    blocks, rows = pay_ref.shape[0], pay_ref.shape[1] - CAP
    score_half(base_ref, g_ref, chat, w_ref, st_ref, acc, pck, rows, tile=tile)
    for p in range(blocks):
        pay_ref[p, :rows, :] = acc[p * rows : (p + 1) * rows].astype(bf16)
        pay_ref[p, rows:, :] = pck[p * CAP : (p + 1) * CAP].astype(bf16)


def most(label, n, shards, rows):
    m = label.shape[1]
    shift, wide = rows.bit_length() - 1, n.bit_length() - 1
    owner = label >> wide
    hot = lax.broadcasted_iota(i32, (shards, m), 0) == owner
    block = (lax.broadcasted_iota(i32, (m, LANES), 0) >> shift) == lax.broadcasted_iota(i32, (m, LANES), 1)
    one = lambda a: jnp.where(a, 1.0, 0.0).astype(bf16)
    return jnp.max(dot(one(hot), one(block), 1, 0))


def second_kernel(
    base_ref, side_ref, x_ref, g_ref, chat, first_ref, firstst_ref, w_ref, st_ref, pay_ref, full_hbm, acc, pck, full_ref, sem, *, tile, shards
):
    blocks, rows = first_ref.shape[0], first_ref.shape[1] - CAP
    count = functools.partial(most, n=chat.shape[0], shards=shards, rows=rows)
    digits = g_ref[w_ref.shape[1] :, : w_ref.shape[1]].astype(f32)
    label = digits[0:1] * 4096.0 + digits[1:2] * 64.0 + digits[2:3]
    crowded = jnp.maximum(count(firstst_ref[2:3, :].astype(i32) + base_ref[0]), count(label.astype(i32)))
    full_ref[0] = (crowded > CAP).astype(i32)
    copy = pltpu.make_async_copy(full_ref, full_hbm, sem)
    copy.start()
    score_half(base_ref, g_ref, chat, w_ref, st_ref, acc, pck, rows, tile=tile)
    side, at_x = side_ref[0], x_ref[0]
    mine = pltpu.roll(firstst_ref[...], at_x * rows, 1)[3:4, :]
    theirs = pltpu.roll(st_ref[...], at_x * rows, 1)[3:4, :]
    left = jnp.where(side == 0, mine, theirs)
    right = jnp.where(side == 0, theirs, mine)
    sums = total_rows(jnp.concatenate([left, right], axis=1))
    for p in range(2 * blocks):
        pay_ref[p, rows + CAP :, :] = sums
    for p in range(blocks):
        to = lax.rem(at_x + p, blocks)
        pay_ref[2 * to + side, : rows + CAP, :] = first_ref[p]
        other = 2 * to + 1 - side
        pay_ref[other, :rows, :] = acc[p * rows : (p + 1) * rows].astype(bf16)
        pay_ref[other, rows : rows + CAP, :] = pck[p * CAP : (p + 1) * CAP].astype(bf16)
    copy.wait()


def half_shapes(n, m):
    return [pltpu.VMEM((n, m), bf16), jax.ShapeDtypeStruct((8, m), f32)]


def first_scores(base, gathered, chat, blocks, tile=1024):
    n, d = chat.shape
    m = gathered.shape[0] - 8
    w, st = half_shapes(n, m)
    return pl.pallas_call(
        functools.partial(first_kernel, tile=tile),
        in_specs=[SMEM, VMEM, VMEM],
        out_specs=[VMEM] * 3,
        out_shape=[w, st, jax.ShapeDtypeStruct((blocks, m // blocks + CAP, d), bf16)],
        scratch_shapes=[pltpu.VMEM((m, d), f32), pltpu.VMEM((blocks * CAP, d), f32)],
        compiler_params=params(24),
        cost_estimate=cost(6),
        name="first_scores",
    )(base, gathered, chat)


def second_scores(where, gathered, chat, first, stats, shards, tile=1024):
    n, d = chat.shape
    m = gathered.shape[0] - 8
    blocks, rows = first.shape[0], first.shape[1]
    w, st = half_shapes(n, m)
    return pl.pallas_call(
        functools.partial(second_kernel, tile=tile, shards=shards),
        in_specs=[SMEM] * 3 + [VMEM] * 4,
        out_specs=[VMEM] * 3 + [HBM],
        out_shape=[
            w,
            st,
            jax.ShapeDtypeStruct((2 * blocks, rows + 8, d), bf16),
            pltpu.HBM((1,), i32),
        ],
        scratch_shapes=[
            pltpu.VMEM((m, d), f32),
            pltpu.VMEM((blocks * CAP, d), f32),
            pltpu.SMEM((1,), i32),
            pltpu.SemaphoreType.DMA(()),
        ],
        compiler_params=params(24),
        cost_estimate=cost(6),
        name="second_scores",
    )(*where, gathered, chat, first, stats)


def middle_kernel(far_ref, line_ref, r_ref, o_ref, *, n):
    far, rows, d = o_ref.shape
    senders = r_ref.shape[0]
    own = rows // 3
    half = far * own
    low = r_ref[:, :half, :].astype(f32).sum(axis=0).astype(bf16)
    label = jnp.sum(line_ref[:, d:].astype(f32) * digit_weights((1, LANES)), axis=1, keepdims=True)
    lane = lax.broadcasted_iota(i32, (1, senders * CAP), 1)
    shift = CAP.bit_length() - 1
    sender, place = lane >> shift, lane & (CAP - 1)
    start = ((((sender >> 1) * far + far_ref[0]) * 2 + (sender & 1)) * n).astype(f32)
    owned = (label >= start) & (label < start + n)
    before = lax.broadcasted_iota(i32, (half, half), 1) < lax.broadcasted_iota(i32, (half, half), 0)
    one = lambda a: jnp.where(a, 1.0, 0.0).astype(bf16)
    rank = dot(one(before), one(owned), 1, 0)
    spread = one(owned & (rank == place.astype(f32)))
    held = jnp.concatenate([r_ref[q, half : half + CAP, :] for q in range(senders)], axis=0)
    pick = dot(spread, held, 1, 0).astype(bf16)
    totals = total_rows(r_ref[:, half + CAP :, :].astype(f32).sum(axis=0).sum(axis=0, keepdims=True))
    for q in range(far):
        o_ref[q, :own, :] = low[q * own : (q + 1) * own]
        o_ref[q, own : 2 * own, :] = pick[q * own : (q + 1) * own]
        o_ref[q, 2 * own :, :] = totals


def middle(at_far, line, received, far, own, n):
    d = received.shape[2]
    return pl.pallas_call(
        functools.partial(middle_kernel, n=n),
        in_specs=[SMEM, VMEM, VMEM],
        out_specs=VMEM,
        out_shape=jax.ShapeDtypeStruct((far, 3 * own, d), bf16),
        compiler_params=params(8),
        name="middle",
    )(at_far, line, received)


def grad_kernel(
    side_ref, at_ref, own_ref, full_ref, r_ref, x_ref, sta_ref, stb_ref, ea_ref, eb_ref, wa_ref, wb_ref, raw, l_hbm, xg_hbm, o_hbm, still_hbm,
    out, xg_ref, l_ref, osem, sem, *, chunk, blocks
):
    n, d = raw.shape
    half = wa_ref.shape[1]
    m = 2 * half
    own = x_ref.shape[0]
    chunks = n // chunk

    def save(k):
        rows = pl.ds(pl.multiple_of(k * chunk, chunk), chunk)
        return pltpu.make_async_copy(out.at[rows], o_hbm.at[rows], osem.at[k])

    side, at_x, own_first = side_ref[0], at_ref[0], own_ref[0]
    still = pltpu.make_async_copy(full_ref, still_hbm, sem.at[2])
    still.start()
    sums = r_ref[...].astype(f32).sum(axis=0)
    total = sums[2 * own :].sum(axis=0, keepdims=True)
    back = lax.rem(blocks - at_x, blocks) * (half // blocks)
    both = jnp.broadcast_to(total, (8, m))
    left = 1.0 / pltpu.roll(both[:, :half], back, 1)[0:1, :]
    right = 1.0 / pltpu.roll(both[:, half:], back, 1)[0:1, :]

    def factors(st_ref, scale):
        return st_ref[2:3, :].astype(i32), scale, st_ref[0:1, :] * (st_ref[1:2, :] * scale - logit_scale)

    halves = (
        (ea_ref, wa_ref, *factors(sta_ref, jnp.where(side == 0, left, right))),
        (eb_ref, wb_ref, *factors(stb_ref, jnp.where(side == 0, right, left))),
    )

    x = x_ref[...].astype(f32)
    inv = inverse_norm(x)
    units = x * inv
    unit16 = units.astype(bf16).astype(f32)
    pick = sums[own : 2 * own]
    texp, logit, slope = margin(jnp.sum(unit16 * pick, axis=1, keepdims=True))
    lane = lax.broadcasted_iota(i32, (own, m), 1)
    row = lax.broadcasted_iota(i32, (own, m), 0)
    own_total = jnp.sum(jnp.where(lane == row + own_first, total, 0.0), axis=1, keepdims=True)
    grad = sums[:own] / own_total + (slope * (texp / own_total - logit_scale)) * pick
    xg_ref[...] = inv * (grad - units * jnp.sum(units * grad, axis=1, keepdims=True))
    loss = jnp.log(own_total) + logit_scale - logit
    spread = jnp.where(lane[:, :LANES] == row[:, :LANES], loss, 0.0).sum(axis=0, keepdims=True)
    l_ref[...] = spread[:, :own]

    def step(k, _):
        rows = pl.ds(pl.multiple_of(k * chunk, chunk), chunk)
        row = lax.broadcasted_iota(i32, (chunk, half), 0)
        grad = 0.0
        for e_ref, w_ref, lab, scale, coef in halves:
            share = jnp.where(row == lab - k * chunk, coef, w_ref[rows, :].astype(f32) * scale)
            grad = grad + dot(share.astype(bf16), e_ref[:half, :], 1, 0)
        w = raw[rows, :].astype(f32)
        inv = inverse_norm(w)
        along = jnp.sum(w * grad, axis=1, keepdims=True) * (inv * inv)
        out[rows, :] = inv * (grad - w * along)
        save(k).start()
        return 0

    step(0, 0)
    small = (
        pltpu.make_async_copy(xg_ref, xg_hbm, sem.at[0]),
        pltpu.make_async_copy(l_ref, l_hbm, sem.at[1]),
    )
    for copy in small:
        copy.start()
    lax.fori_loop(1, chunks, step, 0)
    for copy in (*small, still):
        copy.wait()
    for k in range(chunks):
        save(k).wait()


def grads(where, received, embeddings, stats, ehats, weights, raw, blocks, chunk=512):
    n, d = raw.shape
    own = embeddings.shape[0]
    return pl.pallas_call(
        functools.partial(grad_kernel, chunk=chunk, blocks=blocks),
        in_specs=[SMEM] * 4 + [VMEM] * 9,
        out_specs=[HBM] * 4,
        out_shape=[
            pltpu.HBM((1, own), f32),
            pltpu.HBM((own, d), f32),
            jax.ShapeDtypeStruct((n, d), f32),
            pltpu.HBM((1,), i32),
        ],
        scratch_shapes=[
            pltpu.VMEM((n, d), f32),
            pltpu.VMEM((own, d), f32),
            pltpu.VMEM((1, own), f32),
            pltpu.SemaphoreType.DMA((n // chunk,)),
            pltpu.SemaphoreType.DMA((3,)),
        ],
        compiler_params=params(24),
        name="grads",
    )(*where, received, embeddings, *stats, *ehats, *weights, raw)


def exchange(blocks, axis):
    return lax.all_to_all(blocks, axis, 0, 0, tiled=True)


def per_device(embeddings, labels, centers):
    own, d = embeddings.shape
    n = centers.shape[0]
    far, wide = lax.axis_size(FAR), lax.axis_size("x")
    at_x, at_y = lax.axis_index("x"), lax.axis_index("y")
    half = far * wide * own
    at_far = lax.axis_index(FAR)
    base = lax.axis_index(("x", FAR, "y")) * n
    own_first = at_y * half + (at_x * far + at_far) * own
    where = tuple(a.astype(i32)[None] for a in (base, at_y, at_x, own_first, at_far))
    embeddings, where = lax.optimization_barrier((embeddings, where))
    base, side, at_x, own_first, at_far = where
    line = exchange(pack(embeddings, labels, far), FAR).reshape(far * own, d + LANES)
    lines = [line] + [
        lax.ppermute(line, "x", [(i, (i - k) % wide) for i in range(wide)]) for k in range(1, wide)
    ]
    raw, chat = unit_centers(centers)
    first = merge(lines, d)
    second = lax.ppermute(first, "y", [(0, 1), (1, 0)])
    wa, sta, pay = first_scores(base, first, chat, wide)
    wb, stb, pay, crowded = second_scores((base, side, at_x), second, chat, pay, sta, far * wide * 2)
    received = exchange(middle(at_far, line, exchange(pay, NEAR), far, own, n), FAR)
    losses, emb_grad, center_grad, crowded = grads(
        (side, at_x, own_first, crowded), received, embeddings, (sta, stb), (first, second), (wa, wb), raw, wide
    )
    losses, emb_grad = lax.cond(
        crowded[0] > 0,
        lambda loss, grad, late, x, y, w: dense_examples(x, y + jnp.minimum(late, 0), w),
        lambda loss, grad, *_: (loss, grad),
        losses, emb_grad, crowded, embeddings, labels, centers,
    )
    return (losses.reshape(own), emb_grad, center_grad)


def dense_examples(embeddings, labels, centers):
    own, d = embeddings.shape
    n = centers.shape[0]
    cls = ("x", FAR, "y")
    peers = lax.axis_size(cls)

    def alone(blocks, *others):
        blocks, others = lax.optimization_barrier((blocks, others))
        return lax.optimization_barrier((exchange(blocks, cls), *others))

    def copies(a):
        return jnp.broadcast_to(a[None], (peers, *a.shape))

    index = lax.axis_index(cls)
    x, w = embeddings.astype(f32), centers.astype(f32)
    inv = inverse_norm(x)
    units = x * inv
    chat = (w * inverse_norm(w)).astype(bf16)
    label, units, inv, chat, index = alone(copies(labels), units, inv, chat, index)
    rows, label, units, inv, chat, index = alone(copies(units.astype(bf16)), label, units, inv, chat, index)
    rows = rows.reshape(-1, d)
    label = label.reshape(-1) - index * n
    hot = label[:, None] == jnp.arange(n)[None]
    cosine = dot(rows, chat, 1, 1)
    picked = jnp.sum(jnp.where(hot, cosine, 0.0), axis=1)
    texp, logit, slope = margin(picked)
    owned = (label >= 0) & (label < n)
    texp, logit, slope = (jnp.where(owned, a, 0.0) for a in (texp, logit, slope))
    weight = jnp.where(hot, 0.0, jnp.exp2(cosine * slope2 - shift2))
    total = (weight.sum(axis=1) + texp) / logit_scale
    prod = dot(weight.astype(bf16), chat, 1, 0)
    pick = dot(hot.astype(bf16), chat, 1, 0)
    sums, prod, pick, slope, texp, units, inv, index = alone(
        copies(jnp.stack([total, logit])), prod, pick, slope, texp, units, inv, index
    )
    sums = sums.sum(axis=0)
    total = sums[0]
    rows = prod / total[:, None] + (slope * (texp / total - logit_scale))[:, None] * pick
    grad, sums, units, inv, index = alone(
        rows.astype(bf16).reshape(peers, own, d), sums, units, inv, index
    )
    grad = grad.astype(f32).sum(axis=0)
    mine = lax.dynamic_slice_in_dim(sums, index * own, own, 1)
    loss = jnp.log(mine[0]) + logit_scale - mine[1]
    return loss[None], inv * (grad - units * jnp.sum(units * grad, axis=1, keepdims=True))


def solution(mesh):
    dp = mesh.shape["dp"]
    fine = Mesh(mesh.devices.reshape(4, mesh.shape["cls"] // 8, 2, dp), ("x", FAR, "y", "dp"))
    rows = ("dp", "x", FAR, "y")
    in_specs = (P(rows, None), P(rows), P(rows, None))
    out_specs = (P(rows), P(rows, None), P(rows, None))
    return jax.shard_map(
        per_device, mesh=fine, in_specs=in_specs, out_specs=out_specs, check_vma=False
    )
```

```python
import functools
import math

import jax
import jax.numpy as jnp
from jax import lax
from jax.experimental import pallas as pl
from jax.experimental.pallas import tpu as pltpu
from jax.sharding import Mesh
from jax.sharding import PartitionSpec as P

logit_scale = 64.0
margin_cosine = math.cos(0.5)
margin_sine = math.sin(0.5)
sine_soften = 0.04
norm_eps = 1e-06

slope2 = logit_scale * math.log2(math.e)
shift2 = slope2 - math.log2(logit_scale)


LANES = 128
CAP = 16
MIB = 1024 * 1024
NEAR = ("x", "y")
FAR = "z"
f32, bf16, i32 = jnp.float32, jnp.bfloat16, jnp.int32
VMEM = pl.BlockSpec(memory_space=pltpu.VMEM)
SMEM = pl.BlockSpec(memory_space=pltpu.SMEM)
HBM = pl.BlockSpec(memory_space=pltpu.HBM)


def params(mib):
    return pltpu.CompilerParams(vmem_limit_bytes=mib * MIB)


def cost(gflops):
    return pl.CostEstimate(flops=int(gflops * 1e9), bytes_accessed=8 * MIB, transcendentals=0)


def at(axis):
    return lax.axis_index(axis)


def class_base(n):
    return ((at("x") * lax.axis_size(FAR) + at(FAR)) * lax.axis_size("y") + at("y")) * n


def in_hbm(x):
    return pltpu.with_memory_space_constraint(x, pltpu.HBM)


def dot(a, b, ca, cb):
    return lax.dot_general(a, b, (((ca,), (cb,)), ((), ())), preferred_element_type=f32)


def inverse_norm(x):
    return lax.rsqrt(jnp.sum(x * x, axis=1, keepdims=True) + norm_eps)


def margin(cosine):
    sine = jnp.sqrt(1.0 + sine_soften - cosine * cosine)
    shifted = cosine * margin_cosine - sine * margin_sine
    slope = margin_cosine + margin_sine * cosine / sine
    return jnp.exp2(slope2 * shifted - shift2), logit_scale * shifted, slope


def total_rows(total):
    row8 = lax.broadcasted_iota(i32, (8, total.shape[1]), 0)
    out = jnp.zeros(row8.shape, f32)
    rest = total
    for r in range(3):
        part = rest.astype(bf16).astype(f32)
        out = jnp.where(row8 == r, part, out)
        rest = rest - part
    return out.astype(bf16)


def pack_kernel(x_hbm, lab_hbm, o_ref, x_ref, lab_ref, sem):
    rows, d = x_ref.shape
    copies = (
        pltpu.make_async_copy(lab_hbm, lab_ref, sem.at[0]),
        pltpu.make_async_copy(x_hbm, x_ref, sem.at[1]),
    )
    for copy in copies:
        copy.start()
    for copy in copies:
        copy.wait()
    row = lax.broadcasted_iota(i32, (rows, LANES), 0)
    lane = lax.broadcasted_iota(i32, (rows, LANES), 1)
    lab = jnp.zeros((rows, LANES), i32)
    for j in range(rows):
        lab = jnp.where(row == j, lab_ref[j], lab)
    digit = jnp.where(lane == 0, lab >> 12, jnp.where(lane == 1, (lab >> 6) & 63, lab & 63))
    digit = jnp.where(lane < 3, digit, 0).astype(f32).astype(bf16)
    for p in range(o_ref.shape[0]):
        o_ref[p, :, :d] = x_ref[...]
        o_ref[p, :, d:] = digit


def pack(embeddings, labels, peers):
    rows, d = embeddings.shape
    return pl.pallas_call(
        pack_kernel,
        in_specs=[HBM, HBM],
        out_specs=VMEM,
        out_shape=jax.ShapeDtypeStruct((peers, rows, d + LANES), bf16),
        scratch_shapes=[
            pltpu.VMEM((rows, d), bf16),
            pltpu.SMEM((rows,), i32),
            pltpu.SemaphoreType.DMA((2,)),
        ],
        compiler_params=params(4),
        name="pack",
    )(in_hbm(embeddings), in_hbm(labels))


def digit_weights(shape):
    lane = lax.broadcasted_iota(i32, shape, 1)
    return jnp.where(lane == 0, 4096.0, jnp.where(lane == 1, 64.0, jnp.where(lane == 2, 1.0, 0.0)))


def merge_kernel(*refs):
    *line_refs, o_ref = refs
    rows, d = line_refs[0].shape[0], o_ref.shape[1]
    half = rows * len(line_refs)
    for p, line_ref in enumerate(line_refs):
        x = line_ref[:, :d].astype(f32)
        o_ref[p * rows : (p + 1) * rows, :] = (x * inverse_norm(x)).astype(bf16)
    tail = jnp.concatenate([line_ref[:, d:] for line_ref in line_refs], axis=0)
    same = lax.broadcasted_iota(i32, (8, LANES), 0) == lax.broadcasted_iota(i32, (8, LANES), 1)
    digits = dot(jnp.where(same, 1.0, 0.0).astype(bf16), tail, 1, 1).astype(bf16)
    o_ref[half:, :] = jnp.concatenate([digits] * (d // half), axis=1)


def merge(lines, d):
    rows = lines[0].shape[0] * len(lines)
    return pl.pallas_call(
        merge_kernel,
        in_specs=[VMEM] * len(lines),
        out_specs=VMEM,
        out_shape=jax.ShapeDtypeStruct((rows + 8, d), bf16),
        compiler_params=params(8),
        cost_estimate=cost(0.01),
        name="merge",
    )(*lines)


def unit_kernel(c_hbm, raw, chat, sem, *, tile):
    steps = c_hbm.shape[0] // tile

    def span(k):
        return pl.ds(pl.multiple_of(k * tile, tile), tile)

    def fetch(k):
        return pltpu.make_async_copy(c_hbm.at[span(k)], raw.at[span(k)], sem.at[k])

    for k in range(steps):
        fetch(k).start()

    def step(k, _):
        fetch(k).wait()
        w = raw[span(k), :].astype(f32)
        chat[span(k), :] = (w * inverse_norm(w)).astype(bf16)
        return 0

    lax.fori_loop(0, steps, step, 0)


def unit_centers(centers, tile=512):
    return pl.pallas_call(
        functools.partial(unit_kernel, tile=tile),
        in_specs=[HBM],
        out_specs=[VMEM] * 2,
        out_shape=[pltpu.VMEM(centers.shape, bf16)] * 2,
        scratch_shapes=[pltpu.SemaphoreType.DMA((centers.shape[0] // tile,))],
        compiler_params=params(12),
        cost_estimate=cost(3),
        name="unit_centers",
    )(in_hbm(centers))


def score_half(base, g_ref, chat, w_ref, st_ref, acc, pck, rows, *, tile):
    n, d = chat.shape
    m = w_ref.shape[1]
    steps = n // tile
    digits = g_ref[m:, :m].astype(f32)
    lab1 = (digits[0:1] * 4096.0 + digits[1:2] * 64.0 + digits[2:3]).astype(i32) - base
    owned = (lab1 >= 0) & (lab1 < n)
    shift = rows.bit_length() - 1
    before, after = (lax.broadcasted_iota(i32, (m, m), a) for a in (0, 1))
    ahead = (before < after) & ((before >> shift) == (after >> shift))
    mine = jnp.broadcast_to(jnp.where(owned, 1.0, 0.0), (8, m)).astype(bf16)
    rank = dot(mine, jnp.where(ahead, 1.0, 0.0).astype(bf16), 1, 0)[0:1, :].astype(i32)
    block = lax.broadcasted_iota(i32, (1, m), 1) >> shift
    slots = (m // rows) * CAP
    place = jnp.where(owned & (rank < CAP), block * CAP + rank, -1)
    chosen = lax.broadcasted_iota(i32, (slots, m), 0) == place
    held = jnp.sum(jnp.where(chosen, lab1.astype(f32) + 1.0, 0.0), axis=1, keepdims=True).astype(i32) - 1

    def span(k):
        return pl.ds(pl.multiple_of(k * tile, tile), tile)

    def score(k, tot, tcs):
        cos = dot(chat[span(k), :], g_ref[:m, :], 1, 1)
        hit = lax.broadcasted_iota(i32, (tile, m), 0) == lab1 - k * tile
        e = jnp.where(hit, 0.0, jnp.exp2(cos * slope2 - shift2))
        w_ref[span(k), :] = e.astype(bf16)
        tot = tot + e.reshape(tile // 8, 8, m).sum(axis=0)
        tcs = tcs + jnp.where(hit, cos, 0.0).reshape(tile // 8, 8, m).sum(axis=0)
        return tot, tcs

    def gather(k):
        hot = lax.broadcasted_iota(i32, (slots, tile), 1) == held - k * tile
        c = chat[span(k), :]
        prod = dot(w_ref[span(k), :], c, 0, 0)
        pick = dot(jnp.where(hot, 1.0, 0.0).astype(bf16), c, 1, 0)
        return prod, pick

    zero = jnp.zeros((8, m), f32)
    tot, tcs = score(0, zero, zero)
    acc[...] = jnp.zeros(acc.shape, f32)

    def step(k, carry):
        tot, tcs, held_sum = carry
        prod, pick = gather(k - 1)
        tot, tcs = score(k, tot, tcs)
        acc[...] += prod
        return tot, tcs, held_sum + pick

    tot, tcs, held_sum = lax.fori_loop(1, steps, step, (tot, tcs, jnp.zeros((slots, d), f32)))
    prod, pick = gather(steps - 1)
    acc[...] += prod
    pck[...] = held_sum + pick
    texp, _, slope = margin(tcs.sum(axis=0, keepdims=True))
    texp = jnp.where(owned, texp, 0.0)
    slope = jnp.where(owned, slope, 0.0)
    total = (tot.sum(axis=0, keepdims=True) + texp) * (1.0 / logit_scale)
    row8 = lax.broadcasted_iota(i32, (8, m), 0)
    rest = jnp.where(row8 == 3, total, lab1.astype(f32))
    st_ref[...] = jnp.where(row8 == 0, slope, jnp.where(row8 == 1, texp, rest))


def first_kernel(g_ref, chat, w_ref, st_ref, pay_ref, acc, pck, *, tile):
    blocks, rows = pay_ref.shape[0], pay_ref.shape[1] - CAP
    score_half(class_base(chat.shape[0]), g_ref, chat, w_ref, st_ref, acc, pck, rows, tile=tile)
    for p in range(blocks):
        pay_ref[p, :rows, :] = acc[p * rows : (p + 1) * rows].astype(bf16)
        pay_ref[p, rows:, :] = pck[p * CAP : (p + 1) * CAP].astype(bf16)


def most(label, n, shards, rows):
    m = label.shape[1]
    shift, wide = rows.bit_length() - 1, n.bit_length() - 1
    owner = label >> wide
    hot = lax.broadcasted_iota(i32, (shards, m), 0) == owner
    block = (lax.broadcasted_iota(i32, (m, LANES), 0) >> shift) == lax.broadcasted_iota(i32, (m, LANES), 1)
    one = lambda a: jnp.where(a, 1.0, 0.0).astype(bf16)
    return jnp.max(dot(one(hot), one(block), 1, 0))


def second_kernel(
    g_ref, chat, first_ref, firstst_ref, w_ref, st_ref, pay_ref, full_hbm, acc, pck, full_ref, sem, *, tile, shards
):
    blocks, rows = first_ref.shape[0], first_ref.shape[1] - CAP
    count = functools.partial(most, n=chat.shape[0], shards=shards, rows=rows)
    digits = g_ref[w_ref.shape[1] :, : w_ref.shape[1]].astype(f32)
    label = digits[0:1] * 4096.0 + digits[1:2] * 64.0 + digits[2:3]
    crowded = jnp.maximum(count(firstst_ref[2:3, :].astype(i32) + class_base(chat.shape[0])), count(label.astype(i32)))
    full_ref[0] = (crowded > CAP).astype(i32)
    copy = pltpu.make_async_copy(full_ref, full_hbm, sem)
    copy.start()
    score_half(class_base(chat.shape[0]), g_ref, chat, w_ref, st_ref, acc, pck, rows, tile=tile)
    side, at_x = at("y"), at("x")
    mine = pltpu.roll(firstst_ref[...], at_x * rows, 1)[3:4, :]
    theirs = pltpu.roll(st_ref[...], at_x * rows, 1)[3:4, :]
    left = jnp.where(side == 0, mine, theirs)
    right = jnp.where(side == 0, theirs, mine)
    sums = total_rows(jnp.concatenate([left, right], axis=1))
    for p in range(2 * blocks):
        pay_ref[p, rows + CAP :, :] = sums
    for p in range(blocks):
        to = lax.rem(at_x + p, blocks)
        pay_ref[2 * to + side, : rows + CAP, :] = first_ref[p]
        other = 2 * to + 1 - side
        pay_ref[other, :rows, :] = acc[p * rows : (p + 1) * rows].astype(bf16)
        pay_ref[other, rows : rows + CAP, :] = pck[p * CAP : (p + 1) * CAP].astype(bf16)
    copy.wait()


def half_shapes(n, m):
    return [pltpu.VMEM((n, m), bf16), jax.ShapeDtypeStruct((8, m), f32)]


def first_scores(gathered, chat, blocks, tile=1024):
    n, d = chat.shape
    m = gathered.shape[0] - 8
    w, st = half_shapes(n, m)
    return pl.pallas_call(
        functools.partial(first_kernel, tile=tile),
        in_specs=[VMEM, VMEM],
        out_specs=[VMEM] * 3,
        out_shape=[w, st, jax.ShapeDtypeStruct((blocks, m // blocks + CAP, d), bf16)],
        scratch_shapes=[pltpu.VMEM((m, d), f32), pltpu.VMEM((blocks * CAP, d), f32)],
        compiler_params=params(24),
        cost_estimate=cost(6),
        name="first_scores",
    )(gathered, chat)


def second_scores(gathered, chat, first, stats, shards, tile=1024):
    n, d = chat.shape
    m = gathered.shape[0] - 8
    blocks, rows = first.shape[0], first.shape[1]
    w, st = half_shapes(n, m)
    return pl.pallas_call(
        functools.partial(second_kernel, tile=tile, shards=shards),
        in_specs=[VMEM] * 4,
        out_specs=[VMEM] * 3 + [HBM],
        out_shape=[
            w,
            st,
            jax.ShapeDtypeStruct((2 * blocks, rows + 8, d), bf16),
            pltpu.HBM((1,), i32),
        ],
        scratch_shapes=[
            pltpu.VMEM((m, d), f32),
            pltpu.VMEM((blocks * CAP, d), f32),
            pltpu.SMEM((1,), i32),
            pltpu.SemaphoreType.DMA(()),
        ],
        compiler_params=params(24),
        cost_estimate=cost(6),
        name="second_scores",
    )(gathered, chat, first, stats)


def middle_kernel(line_ref, r_ref, o_ref, *, n):
    far, rows, d = o_ref.shape
    senders = r_ref.shape[0]
    own = rows // 3
    half = far * own
    low = r_ref[:, :half, :].astype(f32).sum(axis=0).astype(bf16)
    label = jnp.sum(line_ref[:, d:].astype(f32) * digit_weights((1, LANES)), axis=1, keepdims=True)
    lane = lax.broadcasted_iota(i32, (1, senders * CAP), 1)
    shift = CAP.bit_length() - 1
    sender, place = lane >> shift, lane & (CAP - 1)
    start = ((((sender >> 1) * far + at(FAR)) * 2 + (sender & 1)) * n).astype(f32)
    owned = (label >= start) & (label < start + n)
    before = lax.broadcasted_iota(i32, (half, half), 1) < lax.broadcasted_iota(i32, (half, half), 0)
    one = lambda a: jnp.where(a, 1.0, 0.0).astype(bf16)
    rank = dot(one(before), one(owned), 1, 0)
    spread = one(owned & (rank == place.astype(f32)))
    held = jnp.concatenate([r_ref[q, half : half + CAP, :] for q in range(senders)], axis=0)
    pick = dot(spread, held, 1, 0).astype(bf16)
    totals = total_rows(r_ref[:, half + CAP :, :].astype(f32).sum(axis=0).sum(axis=0, keepdims=True))
    for q in range(far):
        o_ref[q, :own, :] = low[q * own : (q + 1) * own]
        o_ref[q, own : 2 * own, :] = pick[q * own : (q + 1) * own]
        o_ref[q, 2 * own :, :] = totals


def middle(line, received, far, own, n):
    d = received.shape[2]
    return pl.pallas_call(
        functools.partial(middle_kernel, n=n),
        in_specs=[VMEM, VMEM],
        out_specs=VMEM,
        out_shape=jax.ShapeDtypeStruct((far, 3 * own, d), bf16),
        compiler_params=params(8),
        name="middle",
    )(line, received)


def grad_kernel(
    full_hbm, r_ref, x_ref, sta_ref, stb_ref, ea_ref, eb_ref, wa_ref, wb_ref, raw, l_hbm, xg_hbm, o_hbm, still_hbm,
    out, xg_ref, l_ref, osem, sem, *, chunk, blocks
):
    n, d = raw.shape
    half = wa_ref.shape[1]
    m = 2 * half
    own = x_ref.shape[0]
    chunks = n // chunk

    def save(k):
        rows = pl.ds(pl.multiple_of(k * chunk, chunk), chunk)
        return pltpu.make_async_copy(out.at[rows], o_hbm.at[rows], osem.at[k])

    side, at_x = at("y"), at("x")
    own_first = side * half + (at_x * lax.axis_size(FAR) + at(FAR)) * own
    still = pltpu.make_async_copy(full_hbm, still_hbm, sem.at[2])
    still.start()
    sums = r_ref[...].astype(f32).sum(axis=0)
    total = sums[2 * own :].sum(axis=0, keepdims=True)
    back = lax.rem(blocks - at_x, blocks) * (half // blocks)
    both = jnp.broadcast_to(total, (8, m))
    left = 1.0 / pltpu.roll(both[:, :half], back, 1)[0:1, :]
    right = 1.0 / pltpu.roll(both[:, half:], back, 1)[0:1, :]

    def factors(st_ref, scale):
        return st_ref[2:3, :].astype(i32), scale, st_ref[0:1, :] * (st_ref[1:2, :] * scale - logit_scale)

    halves = (
        (ea_ref, wa_ref, *factors(sta_ref, jnp.where(side == 0, left, right))),
        (eb_ref, wb_ref, *factors(stb_ref, jnp.where(side == 0, right, left))),
    )

    x = x_ref[...].astype(f32)
    inv = inverse_norm(x)
    units = x * inv
    unit16 = units.astype(bf16).astype(f32)
    pick = sums[own : 2 * own]
    texp, logit, slope = margin(jnp.sum(unit16 * pick, axis=1, keepdims=True))
    lane = lax.broadcasted_iota(i32, (own, m), 1)
    row = lax.broadcasted_iota(i32, (own, m), 0)
    own_total = jnp.sum(jnp.where(lane == row + own_first, total, 0.0), axis=1, keepdims=True)
    grad = sums[:own] / own_total + (slope * (texp / own_total - logit_scale)) * pick
    xg_ref[...] = inv * (grad - units * jnp.sum(units * grad, axis=1, keepdims=True))
    loss = jnp.log(own_total) + logit_scale - logit
    spread = jnp.where(lane[:, :LANES] == row[:, :LANES], loss, 0.0).sum(axis=0, keepdims=True)
    l_ref[...] = spread[:, :own]

    def step(k, _):
        rows = pl.ds(pl.multiple_of(k * chunk, chunk), chunk)
        row = lax.broadcasted_iota(i32, (chunk, half), 0)
        grad = 0.0
        for e_ref, w_ref, lab, scale, coef in halves:
            share = jnp.where(row == lab - k * chunk, coef, w_ref[rows, :].astype(f32) * scale)
            grad = grad + dot(share.astype(bf16), e_ref[:half, :], 1, 0)
        w = raw[rows, :].astype(f32)
        inv = inverse_norm(w)
        along = jnp.sum(w * grad, axis=1, keepdims=True) * (inv * inv)
        out[rows, :] = inv * (grad - w * along)
        save(k).start()
        return 0

    step(0, 0)
    small = (
        pltpu.make_async_copy(xg_ref, xg_hbm, sem.at[0]),
        pltpu.make_async_copy(l_ref, l_hbm, sem.at[1]),
    )
    for copy in small:
        copy.start()
    lax.fori_loop(1, chunks, step, 0)
    for copy in (*small, still):
        copy.wait()
    for k in range(chunks):
        save(k).wait()


def grads(crowded, received, embeddings, stats, ehats, weights, raw, blocks, chunk=512):
    n, d = raw.shape
    own = embeddings.shape[0]
    return pl.pallas_call(
        functools.partial(grad_kernel, chunk=chunk, blocks=blocks),
        in_specs=[HBM] + [VMEM] * 9,
        out_specs=[HBM] * 4,
        out_shape=[
            pltpu.HBM((1, own), f32),
            pltpu.HBM((own, d), f32),
            jax.ShapeDtypeStruct((n, d), f32),
            pltpu.HBM((1,), i32),
        ],
        scratch_shapes=[
            pltpu.VMEM((n, d), f32),
            pltpu.VMEM((own, d), f32),
            pltpu.VMEM((1, own), f32),
            pltpu.SemaphoreType.DMA((n // chunk,)),
            pltpu.SemaphoreType.DMA((3,)),
        ],
        compiler_params=params(24),
        name="grads",
    )(in_hbm(crowded), received, embeddings, *stats, *ehats, *weights, raw)


def exchange(blocks, axis):
    return lax.all_to_all(blocks, axis, 0, 0, tiled=True)


def per_device(embeddings, labels, centers):
    own, d = embeddings.shape
    n = centers.shape[0]
    far, wide = lax.axis_size(FAR), lax.axis_size("x")
    line = exchange(pack(embeddings, labels, far), FAR).reshape(far * own, d + LANES)
    lines = [line] + [
        lax.ppermute(line, "x", [(i, (i - k) % wide) for i in range(wide)]) for k in range(1, wide)
    ]
    raw, chat = unit_centers(centers)
    first = merge(lines, d)
    second = lax.ppermute(first, "y", [(0, 1), (1, 0)])
    wa, sta, pay = first_scores(first, chat, wide)
    wb, stb, pay, crowded = second_scores(second, chat, pay, sta, far * wide * 2)
    received = exchange(middle(line, exchange(pay, NEAR), far, own, n), FAR)
    losses, emb_grad, center_grad, crowded = grads(
        crowded, received, embeddings, (sta, stb), (first, second), (wa, wb), raw, wide
    )
    losses, emb_grad = lax.cond(
        crowded[0] > 0,
        lambda loss, grad, late, x, y, w: dense_examples(x, y + jnp.minimum(late, 0), w),
        lambda loss, grad, *_: (loss, grad),
        losses, emb_grad, crowded, embeddings, labels, centers,
    )
    return (losses.reshape(own), emb_grad, center_grad)


def dense_examples(embeddings, labels, centers):
    own, d = embeddings.shape
    n = centers.shape[0]
    cls = ("x", FAR, "y")
    peers = lax.axis_size(cls)

    def alone(blocks, *others):
        blocks, others = lax.optimization_barrier((blocks, others))
        return lax.optimization_barrier((exchange(blocks, cls), *others))

    def copies(a):
        return jnp.broadcast_to(a[None], (peers, *a.shape))

    index = lax.axis_index(cls)
    x, w = embeddings.astype(f32), centers.astype(f32)
    inv = inverse_norm(x)
    units = x * inv
    chat = (w * inverse_norm(w)).astype(bf16)
    label, units, inv, chat, index = alone(copies(labels), units, inv, chat, index)
    rows, label, units, inv, chat, index = alone(copies(units.astype(bf16)), label, units, inv, chat, index)
    rows = rows.reshape(-1, d)
    label = label.reshape(-1) - index * n
    hot = label[:, None] == jnp.arange(n)[None]
    cosine = dot(rows, chat, 1, 1)
    picked = jnp.sum(jnp.where(hot, cosine, 0.0), axis=1)
    texp, logit, slope = margin(picked)
    owned = (label >= 0) & (label < n)
    texp, logit, slope = (jnp.where(owned, a, 0.0) for a in (texp, logit, slope))
    weight = jnp.where(hot, 0.0, jnp.exp2(cosine * slope2 - shift2))
    total = (weight.sum(axis=1) + texp) / logit_scale
    prod = dot(weight.astype(bf16), chat, 1, 0)
    pick = dot(hot.astype(bf16), chat, 1, 0)
    sums, prod, pick, slope, texp, units, inv, index = alone(
        copies(jnp.stack([total, logit])), prod, pick, slope, texp, units, inv, index
    )
    sums = sums.sum(axis=0)
    total = sums[0]
    rows = prod / total[:, None] + (slope * (texp / total - logit_scale))[:, None] * pick
    grad, sums, units, inv, index = alone(
        rows.astype(bf16).reshape(peers, own, d), sums, units, inv, index
    )
    grad = grad.astype(f32).sum(axis=0)
    mine = lax.dynamic_slice_in_dim(sums, index * own, own, 1)
    loss = jnp.log(mine[0]) + logit_scale - mine[1]
    return loss[None], inv * (grad - units * jnp.sum(units * grad, axis=1, keepdims=True))


def solution(mesh):
    dp = mesh.shape["dp"]
    fine = Mesh(mesh.devices.reshape(4, mesh.shape["cls"] // 8, 2, dp), ("x", FAR, "y", "dp"))
    rows = ("dp", "x", FAR, "y")
    in_specs = (P(rows, None), P(rows), P(rows, None))
    out_specs = (P(rows), P(rows, None), P(rows, None))
    return jax.shard_map(
        per_device, mesh=fine, in_specs=in_specs, out_specs=out_specs, check_vma=False
    )
```

```python
import functools
import math

import jax
import jax.numpy as jnp
from jax import lax
from jax.experimental import pallas as pl
from jax.experimental.pallas import tpu as pltpu
from jax.sharding import Mesh
from jax.sharding import PartitionSpec as P

logit_scale = 64.0
margin_cosine = math.cos(0.5)
margin_sine = math.sin(0.5)
sine_soften = 0.04
norm_eps = 1e-06

slope2 = logit_scale * math.log2(math.e)
shift2 = slope2 - math.log2(logit_scale)


LANES = 128
CAP = 8
MIB = 1024 * 1024
NEAR = ("x", "y")
FAR = "z"
f32, bf16, i32 = jnp.float32, jnp.bfloat16, jnp.int32
VMEM = pl.BlockSpec(memory_space=pltpu.VMEM)
SMEM = pl.BlockSpec(memory_space=pltpu.SMEM)
HBM = pl.BlockSpec(memory_space=pltpu.HBM)


def params(mib):
    return pltpu.CompilerParams(vmem_limit_bytes=mib * MIB)


def cost(gflops):
    return pl.CostEstimate(flops=int(gflops * 1e9), bytes_accessed=8 * MIB, transcendentals=0)


def in_hbm(x):
    return pltpu.with_memory_space_constraint(x, pltpu.HBM)


def dot(a, b, ca, cb):
    return lax.dot_general(a, b, (((ca,), (cb,)), ((), ())), preferred_element_type=f32)


def inverse_norm(x):
    return lax.rsqrt(jnp.sum(x * x, axis=1, keepdims=True) + norm_eps)


def margin(cosine):
    sine = jnp.sqrt(1.0 + sine_soften - cosine * cosine)
    shifted = cosine * margin_cosine - sine * margin_sine
    slope = margin_cosine + margin_sine * cosine / sine
    return jnp.exp2(slope2 * shifted - shift2), logit_scale * shifted, slope


def total_rows(total):
    row8 = lax.broadcasted_iota(i32, (8, total.shape[1]), 0)
    out = jnp.zeros(row8.shape, f32)
    rest = total
    for r in range(3):
        part = rest.astype(bf16).astype(f32)
        out = jnp.where(row8 == r, part, out)
        rest = rest - part
    return out.astype(bf16)


def pack_kernel(x_hbm, lab_hbm, o_ref, x_ref, lab_ref, sem):
    rows, d = x_ref.shape
    copies = (
        pltpu.make_async_copy(lab_hbm, lab_ref, sem.at[0]),
        pltpu.make_async_copy(x_hbm, x_ref, sem.at[1]),
    )
    for copy in copies:
        copy.start()
    for copy in copies:
        copy.wait()
    row = lax.broadcasted_iota(i32, (rows, LANES), 0)
    lane = lax.broadcasted_iota(i32, (rows, LANES), 1)
    lab = jnp.zeros((rows, LANES), i32)
    for j in range(rows):
        lab = jnp.where(row == j, lab_ref[j], lab)
    digit = jnp.where(lane == 0, lab >> 12, jnp.where(lane == 1, (lab >> 6) & 63, lab & 63))
    digit = jnp.where(lane < 3, digit, 0).astype(f32).astype(bf16)
    for p in range(o_ref.shape[0]):
        o_ref[p, :, :d] = x_ref[...]
        o_ref[p, :, d:] = digit


def pack(embeddings, labels, peers):
    rows, d = embeddings.shape
    return pl.pallas_call(
        pack_kernel,
        in_specs=[HBM, HBM],
        out_specs=VMEM,
        out_shape=jax.ShapeDtypeStruct((peers, rows, d + LANES), bf16),
        scratch_shapes=[
            pltpu.VMEM((rows, d), bf16),
            pltpu.SMEM((rows,), i32),
            pltpu.SemaphoreType.DMA((2,)),
        ],
        compiler_params=params(4),
        name="pack",
    )(in_hbm(embeddings), in_hbm(labels))


def digit_weights(shape):
    lane = lax.broadcasted_iota(i32, shape, 1)
    return jnp.where(lane == 0, 4096.0, jnp.where(lane == 1, 64.0, jnp.where(lane == 2, 1.0, 0.0)))


def merge_kernel(*refs):
    *line_refs, o_ref = refs
    rows, d = line_refs[0].shape[0], o_ref.shape[1]
    half = rows * len(line_refs)
    for p, line_ref in enumerate(line_refs):
        x = line_ref[:, :d].astype(f32)
        o_ref[p * rows : (p + 1) * rows, :] = (x * inverse_norm(x)).astype(bf16)
    tail = jnp.concatenate([line_ref[:, d:] for line_ref in line_refs], axis=0)
    same = lax.broadcasted_iota(i32, (8, LANES), 0) == lax.broadcasted_iota(i32, (8, LANES), 1)
    digits = dot(jnp.where(same, 1.0, 0.0).astype(bf16), tail, 1, 1).astype(bf16)
    o_ref[half:, :] = jnp.concatenate([digits] * (d // half), axis=1)


def merge(lines, d):
    rows = lines[0].shape[0] * len(lines)
    return pl.pallas_call(
        merge_kernel,
        in_specs=[VMEM] * len(lines),
        out_specs=VMEM,
        out_shape=jax.ShapeDtypeStruct((rows + 8, d), bf16),
        compiler_params=params(8),
        cost_estimate=cost(0.01),
        name="merge",
    )(*lines)


def unit_kernel(c_hbm, raw, chat, sem, *, tile):
    steps = c_hbm.shape[0] // tile

    def span(k):
        return pl.ds(pl.multiple_of(k * tile, tile), tile)

    def fetch(k):
        return pltpu.make_async_copy(c_hbm.at[span(k)], raw.at[span(k)], sem.at[k])

    for k in range(steps):
        fetch(k).start()

    def step(k, _):
        fetch(k).wait()
        w = raw[span(k), :].astype(f32)
        chat[span(k), :] = (w * inverse_norm(w)).astype(bf16)
        return 0

    lax.fori_loop(0, steps, step, 0)


def unit_centers(centers, tile=512):
    return pl.pallas_call(
        functools.partial(unit_kernel, tile=tile),
        in_specs=[HBM],
        out_specs=[VMEM] * 2,
        out_shape=[pltpu.VMEM(centers.shape, bf16)] * 2,
        scratch_shapes=[pltpu.SemaphoreType.DMA((centers.shape[0] // tile,))],
        compiler_params=params(12),
        cost_estimate=cost(3),
        name="unit_centers",
    )(in_hbm(centers))


def score_half(base_ref, g_ref, chat, w_ref, st_ref, acc, pck, rows, *, tile):
    n, d = chat.shape
    m = w_ref.shape[1]
    steps = n // tile
    digits = g_ref[m:, :m].astype(f32)
    lab1 = (digits[0:1] * 4096.0 + digits[1:2] * 64.0 + digits[2:3]).astype(i32) - base_ref[0]
    owned = (lab1 >= 0) & (lab1 < n)
    shift = rows.bit_length() - 1
    before, after = (lax.broadcasted_iota(i32, (m, m), a) for a in (0, 1))
    ahead = (before < after) & ((before >> shift) == (after >> shift))
    mine = jnp.broadcast_to(jnp.where(owned, 1.0, 0.0), (8, m)).astype(bf16)
    rank = dot(mine, jnp.where(ahead, 1.0, 0.0).astype(bf16), 1, 0)[0:1, :].astype(i32)
    block = lax.broadcasted_iota(i32, (1, m), 1) >> shift
    slots = (m // rows) * CAP
    place = jnp.where(owned & (rank < CAP), block * CAP + rank, -1)
    chosen = lax.broadcasted_iota(i32, (slots, m), 0) == place
    held = jnp.sum(jnp.where(chosen, lab1.astype(f32) + 1.0, 0.0), axis=1, keepdims=True).astype(i32) - 1

    def span(k):
        return pl.ds(pl.multiple_of(k * tile, tile), tile)

    def score(k, tot, tcs):
        cos = dot(chat[span(k), :], g_ref[:m, :], 1, 1)
        hit = lax.broadcasted_iota(i32, (tile, m), 0) == lab1 - k * tile
        e = jnp.where(hit, 0.0, jnp.exp2(cos * slope2 - shift2))
        w_ref[span(k), :] = e.astype(bf16)
        tot = tot + e.reshape(tile // 8, 8, m).sum(axis=0)
        tcs = tcs + jnp.where(hit, cos, 0.0).reshape(tile // 8, 8, m).sum(axis=0)
        return tot, tcs

    def gather(k):
        hot = lax.broadcasted_iota(i32, (slots, tile), 1) == held - k * tile
        c = chat[span(k), :]
        prod = dot(w_ref[span(k), :], c, 0, 0)
        pick = dot(jnp.where(hot, 1.0, 0.0).astype(bf16), c, 1, 0)
        return prod, pick

    zero = jnp.zeros((8, m), f32)
    tot, tcs = score(0, zero, zero)
    acc[...] = jnp.zeros(acc.shape, f32)

    def step(k, carry):
        tot, tcs, held_sum = carry
        prod, pick = gather(k - 1)
        tot, tcs = score(k, tot, tcs)
        acc[...] += prod
        return tot, tcs, held_sum + pick

    tot, tcs, held_sum = lax.fori_loop(1, steps, step, (tot, tcs, jnp.zeros((slots, d), f32)))
    prod, pick = gather(steps - 1)
    acc[...] += prod
    pck[...] = held_sum + pick
    texp, _, slope = margin(tcs.sum(axis=0, keepdims=True))
    texp = jnp.where(owned, texp, 0.0)
    slope = jnp.where(owned, slope, 0.0)
    total = (tot.sum(axis=0, keepdims=True) + texp) * (1.0 / logit_scale)
    row8 = lax.broadcasted_iota(i32, (8, m), 0)
    rest = jnp.where(row8 == 3, total, lab1.astype(f32))
    st_ref[...] = jnp.where(row8 == 0, slope, jnp.where(row8 == 1, texp, rest))


def first_kernel(base_ref, g_ref, chat, w_ref, st_ref, pay_ref, acc, pck, *, tile):
    blocks, rows = pay_ref.shape[0], pay_ref.shape[1] - CAP
    score_half(base_ref, g_ref, chat, w_ref, st_ref, acc, pck, rows, tile=tile)
    for p in range(blocks):
        pay_ref[p, :rows, :] = acc[p * rows : (p + 1) * rows].astype(bf16)
        pay_ref[p, rows:, :] = pck[p * CAP : (p + 1) * CAP].astype(bf16)


def most(label, n, shards, rows):
    m = label.shape[1]
    shift, wide = rows.bit_length() - 1, n.bit_length() - 1
    owner = label >> wide
    hot = lax.broadcasted_iota(i32, (shards, m), 0) == owner
    block = (lax.broadcasted_iota(i32, (m, LANES), 0) >> shift) == lax.broadcasted_iota(i32, (m, LANES), 1)
    one = lambda a: jnp.where(a, 1.0, 0.0).astype(bf16)
    return jnp.max(dot(one(hot), one(block), 1, 0))


def second_kernel(
    base_ref, side_ref, x_ref, g_ref, chat, first_ref, firstst_ref, w_ref, st_ref, pay_ref, full_hbm, acc, pck, full_ref, sem, *, tile, shards
):
    blocks, rows = first_ref.shape[0], first_ref.shape[1] - CAP
    count = functools.partial(most, n=chat.shape[0], shards=shards, rows=rows)
    digits = g_ref[w_ref.shape[1] :, : w_ref.shape[1]].astype(f32)
    label = digits[0:1] * 4096.0 + digits[1:2] * 64.0 + digits[2:3]
    crowded = jnp.maximum(count(firstst_ref[2:3, :].astype(i32) + base_ref[0]), count(label.astype(i32)))
    full_ref[0] = (crowded > CAP).astype(i32)
    copy = pltpu.make_async_copy(full_ref, full_hbm, sem)
    copy.start()
    score_half(base_ref, g_ref, chat, w_ref, st_ref, acc, pck, rows, tile=tile)
    side, at_x = side_ref[0], x_ref[0]
    mine = pltpu.roll(firstst_ref[...], at_x * rows, 1)[3:4, :]
    theirs = pltpu.roll(st_ref[...], at_x * rows, 1)[3:4, :]
    left = jnp.where(side == 0, mine, theirs)
    right = jnp.where(side == 0, theirs, mine)
    sums = total_rows(jnp.concatenate([left, right], axis=1))
    for p in range(2 * blocks):
        pay_ref[p, rows + CAP :, :] = sums
    for p in range(blocks):
        to = lax.rem(at_x + p, blocks)
        pay_ref[2 * to + side, : rows + CAP, :] = first_ref[p]
        other = 2 * to + 1 - side
        pay_ref[other, :rows, :] = acc[p * rows : (p + 1) * rows].astype(bf16)
        pay_ref[other, rows : rows + CAP, :] = pck[p * CAP : (p + 1) * CAP].astype(bf16)
    copy.wait()


def half_shapes(n, m):
    return [pltpu.VMEM((n, m), bf16), jax.ShapeDtypeStruct((8, m), f32)]


def first_scores(base, gathered, chat, blocks, tile=1024):
    n, d = chat.shape
    m = gathered.shape[0] - 8
    w, st = half_shapes(n, m)
    return pl.pallas_call(
        functools.partial(first_kernel, tile=tile),
        in_specs=[SMEM, VMEM, VMEM],
        out_specs=[VMEM] * 3,
        out_shape=[w, st, jax.ShapeDtypeStruct((blocks, m // blocks + CAP, d), bf16)],
        scratch_shapes=[pltpu.VMEM((m, d), f32), pltpu.VMEM((blocks * CAP, d), f32)],
        compiler_params=params(24),
        cost_estimate=cost(6),
        name="first_scores",
    )(base, gathered, chat)


def second_scores(where, gathered, chat, first, stats, shards, tile=1024):
    n, d = chat.shape
    m = gathered.shape[0] - 8
    blocks, rows = first.shape[0], first.shape[1]
    w, st = half_shapes(n, m)
    return pl.pallas_call(
        functools.partial(second_kernel, tile=tile, shards=shards),
        in_specs=[SMEM] * 3 + [VMEM] * 4,
        out_specs=[VMEM] * 3 + [HBM],
        out_shape=[
            w,
            st,
            jax.ShapeDtypeStruct((2 * blocks, rows + 8, d), bf16),
            pltpu.HBM((1,), i32),
        ],
        scratch_shapes=[
            pltpu.VMEM((m, d), f32),
            pltpu.VMEM((blocks * CAP, d), f32),
            pltpu.SMEM((1,), i32),
            pltpu.SemaphoreType.DMA(()),
        ],
        compiler_params=params(24),
        cost_estimate=cost(6),
        name="second_scores",
    )(*where, gathered, chat, first, stats)


def middle_kernel(far_ref, line_ref, r_ref, o_ref, *, n):
    far, rows, d = o_ref.shape
    senders = r_ref.shape[0]
    own = rows // 3
    half = far * own
    low = r_ref[:, :half, :].astype(f32).sum(axis=0).astype(bf16)
    label = jnp.sum(line_ref[:, d:].astype(f32) * digit_weights((1, LANES)), axis=1, keepdims=True)
    lane = lax.broadcasted_iota(i32, (1, senders * CAP), 1)
    shift = CAP.bit_length() - 1
    sender, place = lane >> shift, lane & (CAP - 1)
    start = ((((sender >> 1) * far + far_ref[0]) * 2 + (sender & 1)) * n).astype(f32)
    owned = (label >= start) & (label < start + n)
    before = lax.broadcasted_iota(i32, (half, half), 1) < lax.broadcasted_iota(i32, (half, half), 0)
    one = lambda a: jnp.where(a, 1.0, 0.0).astype(bf16)
    rank = dot(one(before), one(owned), 1, 0)
    spread = one(owned & (rank == place.astype(f32)))
    held = jnp.concatenate([r_ref[q, half : half + CAP, :] for q in range(senders)], axis=0)
    pick = dot(spread, held, 1, 0).astype(bf16)
    totals = total_rows(r_ref[:, half + CAP :, :].astype(f32).sum(axis=0).sum(axis=0, keepdims=True))
    for q in range(far):
        o_ref[q, :own, :] = low[q * own : (q + 1) * own]
        o_ref[q, own : 2 * own, :] = pick[q * own : (q + 1) * own]
        o_ref[q, 2 * own :, :] = totals


def middle(at_far, line, received, far, own, n):
    d = received.shape[2]
    return pl.pallas_call(
        functools.partial(middle_kernel, n=n),
        in_specs=[SMEM, VMEM, VMEM],
        out_specs=VMEM,
        out_shape=jax.ShapeDtypeStruct((far, 3 * own, d), bf16),
        compiler_params=params(8),
        name="middle",
    )(at_far, line, received)


def grad_kernel(
    side_ref, at_ref, own_ref, full_ref, r_ref, x_ref, sta_ref, stb_ref, ea_ref, eb_ref, wa_ref, wb_ref, raw, l_hbm, xg_hbm, o_hbm, still_hbm,
    out, xg_ref, l_ref, osem, sem, *, chunk, blocks
):
    n, d = raw.shape
    half = wa_ref.shape[1]
    m = 2 * half
    own = x_ref.shape[0]
    chunks = n // chunk

    def save(k):
        rows = pl.ds(pl.multiple_of(k * chunk, chunk), chunk)
        return pltpu.make_async_copy(out.at[rows], o_hbm.at[rows], osem.at[k])

    side, at_x, own_first = side_ref[0], at_ref[0], own_ref[0]
    still = pltpu.make_async_copy(full_ref, still_hbm, sem.at[2])
    still.start()
    sums = r_ref[...].astype(f32).sum(axis=0)
    total = sums[2 * own :].sum(axis=0, keepdims=True)
    back = lax.rem(blocks - at_x, blocks) * (half // blocks)
    both = jnp.broadcast_to(total, (8, m))
    left = 1.0 / pltpu.roll(both[:, :half], back, 1)[0:1, :]
    right = 1.0 / pltpu.roll(both[:, half:], back, 1)[0:1, :]

    def factors(st_ref, scale):
        return st_ref[2:3, :].astype(i32), scale, st_ref[0:1, :] * (st_ref[1:2, :] * scale - logit_scale)

    halves = (
        (ea_ref, wa_ref, *factors(sta_ref, jnp.where(side == 0, left, right))),
        (eb_ref, wb_ref, *factors(stb_ref, jnp.where(side == 0, right, left))),
    )

    x = x_ref[...].astype(f32)
    inv = inverse_norm(x)
    units = x * inv
    unit16 = units.astype(bf16).astype(f32)
    pick = sums[own : 2 * own]
    texp, logit, slope = margin(jnp.sum(unit16 * pick, axis=1, keepdims=True))
    lane = lax.broadcasted_iota(i32, (own, m), 1)
    row = lax.broadcasted_iota(i32, (own, m), 0)
    own_total = jnp.sum(jnp.where(lane == row + own_first, total, 0.0), axis=1, keepdims=True)
    grad = sums[:own] / own_total + (slope * (texp / own_total - logit_scale)) * pick
    xg_ref[...] = inv * (grad - units * jnp.sum(units * grad, axis=1, keepdims=True))
    loss = jnp.log(own_total) + logit_scale - logit
    spread = jnp.where(lane[:, :LANES] == row[:, :LANES], loss, 0.0).sum(axis=0, keepdims=True)
    l_ref[...] = spread[:, :own]

    def step(k, _):
        rows = pl.ds(pl.multiple_of(k * chunk, chunk), chunk)
        row = lax.broadcasted_iota(i32, (chunk, half), 0)
        grad = 0.0
        for e_ref, w_ref, lab, scale, coef in halves:
            share = jnp.where(row == lab - k * chunk, coef, w_ref[rows, :].astype(f32) * scale)
            grad = grad + dot(share.astype(bf16), e_ref[:half, :], 1, 0)
        w = raw[rows, :].astype(f32)
        inv = inverse_norm(w)
        along = jnp.sum(w * grad, axis=1, keepdims=True) * (inv * inv)
        out[rows, :] = inv * (grad - w * along)
        save(k).start()
        return 0

    step(0, 0)
    small = (
        pltpu.make_async_copy(xg_ref, xg_hbm, sem.at[0]),
        pltpu.make_async_copy(l_ref, l_hbm, sem.at[1]),
    )
    for copy in small:
        copy.start()
    lax.fori_loop(1, chunks, step, 0)
    for copy in (*small, still):
        copy.wait()
    for k in range(chunks):
        save(k).wait()


def grads(where, received, embeddings, stats, ehats, weights, raw, blocks, chunk=512):
    n, d = raw.shape
    own = embeddings.shape[0]
    return pl.pallas_call(
        functools.partial(grad_kernel, chunk=chunk, blocks=blocks),
        in_specs=[SMEM] * 4 + [VMEM] * 9,
        out_specs=[HBM] * 4,
        out_shape=[
            pltpu.HBM((1, own), f32),
            pltpu.HBM((own, d), f32),
            jax.ShapeDtypeStruct((n, d), f32),
            pltpu.HBM((1,), i32),
        ],
        scratch_shapes=[
            pltpu.VMEM((n, d), f32),
            pltpu.VMEM((own, d), f32),
            pltpu.VMEM((1, own), f32),
            pltpu.SemaphoreType.DMA((n // chunk,)),
            pltpu.SemaphoreType.DMA((3,)),
        ],
        compiler_params=params(24),
        name="grads",
    )(*where, received, embeddings, *stats, *ehats, *weights, raw)


def exchange(blocks, axis):
    return lax.all_to_all(blocks, axis, 0, 0, tiled=True)


def per_device(embeddings, labels, centers):
    own, d = embeddings.shape
    n = centers.shape[0]
    far, wide = lax.axis_size(FAR), lax.axis_size("x")
    at_x, at_y = lax.axis_index("x"), lax.axis_index("y")
    half = far * wide * own
    at_far = lax.axis_index(FAR)
    base = lax.axis_index(("x", FAR, "y")) * n
    own_first = at_y * half + (at_x * far + at_far) * own
    where = tuple(a.astype(i32)[None] for a in (base, at_y, at_x, own_first, at_far))
    embeddings, where = lax.optimization_barrier((embeddings, where))
    base, side, at_x, own_first, at_far = where
    line = exchange(pack(embeddings, labels, far), FAR).reshape(far * own, d + LANES)
    lines = [line] + [
        lax.ppermute(line, "x", [(i, (i - k) % wide) for i in range(wide)]) for k in range(1, wide)
    ]
    raw, chat = unit_centers(centers)
    first = merge(lines, d)
    second = lax.ppermute(first, "y", [(0, 1), (1, 0)])
    wa, sta, pay = first_scores(base, first, chat, wide)
    wb, stb, pay, crowded = second_scores((base, side, at_x), second, chat, pay, sta, far * wide * 2)
    received = exchange(middle(at_far, line, exchange(pay, NEAR), far, own, n), FAR)
    losses, emb_grad, center_grad, crowded = grads(
        (side, at_x, own_first, crowded), received, embeddings, (sta, stb), (first, second), (wa, wb), raw, wide
    )
    losses, emb_grad = lax.cond(
        crowded[0] > 0,
        lambda loss, grad, late, x, y, w: dense_examples(x, y + jnp.minimum(late, 0), w),
        lambda loss, grad, *_: (loss, grad),
        losses, emb_grad, crowded, embeddings, labels, centers,
    )
    return (losses.reshape(own), emb_grad, center_grad)


def dense_examples(embeddings, labels, centers):
    own, d = embeddings.shape
    n = centers.shape[0]
    cls = ("x", FAR, "y")
    peers = lax.axis_size(cls)

    def alone(blocks, *others):
        blocks, others = lax.optimization_barrier((blocks, others))
        return lax.optimization_barrier((exchange(blocks, cls), *others))

    def copies(a):
        return jnp.broadcast_to(a[None], (peers, *a.shape))

    index = lax.axis_index(cls)
    x, w = embeddings.astype(f32), centers.astype(f32)
    inv = inverse_norm(x)
    units = x * inv
    chat = (w * inverse_norm(w)).astype(bf16)
    label, units, inv, chat, index = alone(copies(labels), units, inv, chat, index)
    rows, label, units, inv, chat, index = alone(copies(units.astype(bf16)), label, units, inv, chat, index)
    rows = rows.reshape(-1, d)
    label = label.reshape(-1) - index * n
    hot = label[:, None] == jnp.arange(n)[None]
    cosine = dot(rows, chat, 1, 1)
    picked = jnp.sum(jnp.where(hot, cosine, 0.0), axis=1)
    texp, logit, slope = margin(picked)
    owned = (label >= 0) & (label < n)
    texp, logit, slope = (jnp.where(owned, a, 0.0) for a in (texp, logit, slope))
    weight = jnp.where(hot, 0.0, jnp.exp2(cosine * slope2 - shift2))
    total = (weight.sum(axis=1) + texp) / logit_scale
    prod = dot(weight.astype(bf16), chat, 1, 0)
    pick = dot(hot.astype(bf16), chat, 1, 0)
    sums, prod, pick, slope, texp, units, inv, index = alone(
        copies(jnp.stack([total, logit])), prod, pick, slope, texp, units, inv, index
    )
    sums = sums.sum(axis=0)
    total = sums[0]
    rows = prod / total[:, None] + (slope * (texp / total - logit_scale))[:, None] * pick
    grad, sums, units, inv, index = alone(
        rows.astype(bf16).reshape(peers, own, d), sums, units, inv, index
    )
    grad = grad.astype(f32).sum(axis=0)
    mine = lax.dynamic_slice_in_dim(sums, index * own, own, 1)
    loss = jnp.log(mine[0]) + logit_scale - mine[1]
    return loss[None], inv * (grad - units * jnp.sum(units * grad, axis=1, keepdims=True))


def solution(mesh):
    dp = mesh.shape["dp"]
    fine = Mesh(mesh.devices.reshape(4, mesh.shape["cls"] // 8, 2, dp), ("x", FAR, "y", "dp"))
    rows = ("dp", "x", FAR, "y")
    in_specs = (P(rows, None), P(rows), P(rows, None))
    out_specs = (P(rows), P(rows, None), P(rows, None))
    return jax.shard_map(
        per_device, mesh=fine, in_specs=in_specs, out_specs=out_specs, check_vma=False
    )
```

```python
import functools
import math

import jax
import jax.numpy as jnp
from jax import lax
from jax.experimental import pallas as pl
from jax.experimental.pallas import tpu as pltpu
from jax.sharding import Mesh
from jax.sharding import PartitionSpec as P

logit_scale = 64.0
margin_cosine = math.cos(0.5)
margin_sine = math.sin(0.5)
sine_soften = 0.04
norm_eps = 1e-06

slope2 = logit_scale * math.log2(math.e)
shift2 = slope2 - math.log2(logit_scale)


LANES = 128
CAP = 16
MIB = 1024 * 1024
NEAR = ("x", "y")
FAR = "z"
f32, bf16, i32 = jnp.float32, jnp.bfloat16, jnp.int32
VMEM = pl.BlockSpec(memory_space=pltpu.VMEM)
SMEM = pl.BlockSpec(memory_space=pltpu.SMEM)
HBM = pl.BlockSpec(memory_space=pltpu.HBM)


def params(mib):
    return pltpu.CompilerParams(vmem_limit_bytes=mib * MIB)


def cost(gflops):
    return pl.CostEstimate(flops=int(gflops * 1e9), bytes_accessed=8 * MIB, transcendentals=0)


def at(axis):
    return lax.axis_index(axis)


def class_base(n):
    return ((at("x") * lax.axis_size(FAR) + at(FAR)) * lax.axis_size("y") + at("y")) * n


def in_hbm(x):
    return pltpu.with_memory_space_constraint(x, pltpu.HBM)


def dot(a, b, ca, cb):
    return lax.dot_general(a, b, (((ca,), (cb,)), ((), ())), preferred_element_type=f32)


def inverse_norm(x):
    return lax.rsqrt(jnp.sum(x * x, axis=1, keepdims=True) + norm_eps)


def margin(cosine):
    sine = jnp.sqrt(1.0 + sine_soften - cosine * cosine)
    shifted = cosine * margin_cosine - sine * margin_sine
    slope = margin_cosine + margin_sine * cosine / sine
    return jnp.exp2(slope2 * shifted - shift2), logit_scale * shifted, slope


def total_rows(total):
    row8 = lax.broadcasted_iota(i32, (8, total.shape[1]), 0)
    out = jnp.zeros(row8.shape, f32)
    rest = total
    for r in range(3):
        part = rest.astype(bf16).astype(f32)
        out = jnp.where(row8 == r, part, out)
        rest = rest - part
    return out.astype(bf16)


def pack_kernel(x_hbm, lab_hbm, o_ref, x_ref, lab_ref, sem):
    rows, d = x_ref.shape
    copies = (
        pltpu.make_async_copy(lab_hbm, lab_ref, sem.at[0]),
        pltpu.make_async_copy(x_hbm, x_ref, sem.at[1]),
    )
    for copy in copies:
        copy.start()
    for copy in copies:
        copy.wait()
    row = lax.broadcasted_iota(i32, (rows, LANES), 0)
    lane = lax.broadcasted_iota(i32, (rows, LANES), 1)
    lab = jnp.zeros((rows, LANES), i32)
    for j in range(rows):
        lab = jnp.where(row == j, lab_ref[j], lab)
    digit = jnp.where(lane == 0, lab >> 12, jnp.where(lane == 1, (lab >> 6) & 63, lab & 63))
    digit = jnp.where(lane < 3, digit, 0).astype(f32).astype(bf16)
    for p in range(o_ref.shape[0]):
        o_ref[p, :, :d] = x_ref[...]
        o_ref[p, :, d:] = digit


def pack(embeddings, labels, peers):
    rows, d = embeddings.shape
    return pl.pallas_call(
        pack_kernel,
        in_specs=[HBM, HBM],
        out_specs=VMEM,
        out_shape=jax.ShapeDtypeStruct((peers, rows, d + LANES), bf16),
        scratch_shapes=[
            pltpu.VMEM((rows, d), bf16),
            pltpu.SMEM((rows,), i32),
            pltpu.SemaphoreType.DMA((2,)),
        ],
        compiler_params=params(4),
        name="pack",
    )(in_hbm(embeddings), in_hbm(labels))


def digit_weights(shape):
    lane = lax.broadcasted_iota(i32, shape, 1)
    return jnp.where(lane == 0, 4096.0, jnp.where(lane == 1, 64.0, jnp.where(lane == 2, 1.0, 0.0)))


def merge_kernel(*refs):
    *line_refs, o_ref = refs
    rows, d = line_refs[0].shape[0], o_ref.shape[1]
    half = rows * len(line_refs)
    for p, line_ref in enumerate(line_refs):
        x = line_ref[:, :d].astype(f32)
        o_ref[p * rows : (p + 1) * rows, :] = (x * inverse_norm(x)).astype(bf16)
    tail = jnp.concatenate([line_ref[:, d:] for line_ref in line_refs], axis=0)
    same = lax.broadcasted_iota(i32, (8, LANES), 0) == lax.broadcasted_iota(i32, (8, LANES), 1)
    digits = dot(jnp.where(same, 1.0, 0.0).astype(bf16), tail, 1, 1).astype(bf16)
    o_ref[half:, :] = jnp.concatenate([digits] * (d // half), axis=1)


def merge(lines, d):
    rows = lines[0].shape[0] * len(lines)
    return pl.pallas_call(
        merge_kernel,
        in_specs=[VMEM] * len(lines),
        out_specs=VMEM,
        out_shape=jax.ShapeDtypeStruct((rows + 8, d), bf16),
        compiler_params=params(8),
        cost_estimate=cost(0.01),
        name="merge",
    )(*lines)


def unit_kernel(c_hbm, raw, chat, sem, *, tile):
    steps = c_hbm.shape[0] // tile

    def span(k):
        return pl.ds(pl.multiple_of(k * tile, tile), tile)

    def fetch(k):
        return pltpu.make_async_copy(c_hbm.at[span(k)], raw.at[span(k)], sem.at[k])

    for k in range(steps):
        fetch(k).start()

    def step(k, _):
        fetch(k).wait()
        w = raw[span(k), :].astype(f32)
        chat[span(k), :] = (w * inverse_norm(w)).astype(bf16)
        return 0

    lax.fori_loop(0, steps, step, 0)


def unit_centers(centers, tile=512):
    return pl.pallas_call(
        functools.partial(unit_kernel, tile=tile),
        in_specs=[HBM],
        out_specs=[VMEM] * 2,
        out_shape=[pltpu.VMEM(centers.shape, bf16)] * 2,
        scratch_shapes=[pltpu.SemaphoreType.DMA((centers.shape[0] // tile,))],
        compiler_params=params(12),
        cost_estimate=cost(3),
        name="unit_centers",
    )(in_hbm(centers))


def score_half(base, g_ref, chat, w_ref, st_ref, acc, pck, rows, *, tile):
    n, d = chat.shape
    m = w_ref.shape[1]
    steps = n // tile
    digits = g_ref[m:, :m].astype(f32)
    lab1 = (digits[0:1] * 4096.0 + digits[1:2] * 64.0 + digits[2:3]).astype(i32) - base
    owned = (lab1 >= 0) & (lab1 < n)
    shift = rows.bit_length() - 1
    before, after = (lax.broadcasted_iota(i32, (m, m), a) for a in (0, 1))
    ahead = (before < after) & ((before >> shift) == (after >> shift))
    mine = jnp.broadcast_to(jnp.where(owned, 1.0, 0.0), (8, m)).astype(bf16)
    rank = dot(mine, jnp.where(ahead, 1.0, 0.0).astype(bf16), 1, 0)[0:1, :].astype(i32)
    block = lax.broadcasted_iota(i32, (1, m), 1) >> shift
    slots = (m // rows) * CAP
    place = jnp.where(owned & (rank < CAP), block * CAP + rank, -1)
    chosen = lax.broadcasted_iota(i32, (slots, m), 0) == place
    held = jnp.sum(jnp.where(chosen, lab1.astype(f32) + 1.0, 0.0), axis=1, keepdims=True).astype(i32) - 1

    def span(k):
        return pl.ds(pl.multiple_of(k * tile, tile), tile)

    def score(k, tot, tcs):
        cos = dot(chat[span(k), :], g_ref[:m, :], 1, 1)
        hit = lax.broadcasted_iota(i32, (tile, m), 0) == lab1 - k * tile
        e = jnp.where(hit, 0.0, jnp.exp2(cos * slope2 - shift2))
        w_ref[span(k), :] = e.astype(bf16)
        tot = tot + e.reshape(tile // 8, 8, m).sum(axis=0)
        tcs = tcs + jnp.where(hit, cos, 0.0).reshape(tile // 8, 8, m).sum(axis=0)
        return tot, tcs

    def gather(k):
        hot = lax.broadcasted_iota(i32, (slots, tile), 1) == held - k * tile
        c = chat[span(k), :]
        prod = dot(w_ref[span(k), :], c, 0, 0)
        pick = dot(jnp.where(hot, 1.0, 0.0).astype(bf16), c, 1, 0)
        return prod, pick

    zero = jnp.zeros((8, m), f32)
    tot, tcs = score(0, zero, zero)
    acc[...] = jnp.zeros(acc.shape, f32)

    def step(k, carry):
        tot, tcs, held_sum = carry
        prod, pick = gather(k - 1)
        tot, tcs = score(k, tot, tcs)
        acc[...] += prod
        return tot, tcs, held_sum + pick

    tot, tcs, held_sum = lax.fori_loop(1, steps, step, (tot, tcs, jnp.zeros((slots, d), f32)))
    prod, pick = gather(steps - 1)
    acc[...] += prod
    pck[...] = held_sum + pick
    texp, _, slope = margin(tcs.sum(axis=0, keepdims=True))
    texp = jnp.where(owned, texp, 0.0)
    slope = jnp.where(owned, slope, 0.0)
    total = (tot.sum(axis=0, keepdims=True) + texp) * (1.0 / logit_scale)
    row8 = lax.broadcasted_iota(i32, (8, m), 0)
    rest = jnp.where(row8 == 3, total, lab1.astype(f32))
    st_ref[...] = jnp.where(row8 == 0, slope, jnp.where(row8 == 1, texp, rest))


def first_kernel(g_ref, chat, w_ref, st_ref, pay_ref, acc, pck, *, tile):
    blocks, rows = pay_ref.shape[0], pay_ref.shape[1] - CAP
    score_half(class_base(chat.shape[0]), g_ref, chat, w_ref, st_ref, acc, pck, rows, tile=tile)
    for p in range(blocks):
        pay_ref[p, :rows, :] = acc[p * rows : (p + 1) * rows].astype(bf16)
        pay_ref[p, rows:, :] = pck[p * CAP : (p + 1) * CAP].astype(bf16)


def most(label, n, shards, rows):
    m = label.shape[1]
    shift, wide = rows.bit_length() - 1, n.bit_length() - 1
    owner = label >> wide
    hot = lax.broadcasted_iota(i32, (shards, m), 0) == owner
    block = (lax.broadcasted_iota(i32, (m, LANES), 0) >> shift) == lax.broadcasted_iota(i32, (m, LANES), 1)
    one = lambda a: jnp.where(a, 1.0, 0.0).astype(bf16)
    return jnp.max(dot(one(hot), one(block), 1, 0))


def second_kernel(
    g_ref, chat, first_ref, firstst_ref, w_ref, st_ref, pay_ref, full_hbm, acc, pck, full_ref, sem, *, tile, shards
):
    blocks, rows = first_ref.shape[0], first_ref.shape[1] - CAP
    count = functools.partial(most, n=chat.shape[0], shards=shards, rows=rows)
    digits = g_ref[w_ref.shape[1] :, : w_ref.shape[1]].astype(f32)
    label = digits[0:1] * 4096.0 + digits[1:2] * 64.0 + digits[2:3]
    crowded = jnp.maximum(count(firstst_ref[2:3, :].astype(i32) + class_base(chat.shape[0])), count(label.astype(i32)))
    full_ref[0] = (crowded > CAP).astype(i32)
    copy = pltpu.make_async_copy(full_ref, full_hbm, sem)
    copy.start()
    score_half(class_base(chat.shape[0]), g_ref, chat, w_ref, st_ref, acc, pck, rows, tile=tile)
    side, at_x = at("y"), at("x")
    mine = pltpu.roll(firstst_ref[...], at_x * rows, 1)[3:4, :]
    theirs = pltpu.roll(st_ref[...], at_x * rows, 1)[3:4, :]
    left = jnp.where(side == 0, mine, theirs)
    right = jnp.where(side == 0, theirs, mine)
    sums = total_rows(jnp.concatenate([left, right], axis=1))
    for p in range(2 * blocks):
        pay_ref[p, rows + CAP :, :] = sums
    for p in range(blocks):
        to = lax.rem(at_x + p, blocks)
        pay_ref[2 * to + side, : rows + CAP, :] = first_ref[p]
        other = 2 * to + 1 - side
        pay_ref[other, :rows, :] = acc[p * rows : (p + 1) * rows].astype(bf16)
        pay_ref[other, rows : rows + CAP, :] = pck[p * CAP : (p + 1) * CAP].astype(bf16)
    copy.wait()


def half_shapes(n, m):
    return [pltpu.VMEM((n, m), bf16), jax.ShapeDtypeStruct((8, m), f32)]


def first_scores(gathered, chat, blocks, tile=1024):
    n, d = chat.shape
    m = gathered.shape[0] - 8
    w, st = half_shapes(n, m)
    return pl.pallas_call(
        functools.partial(first_kernel, tile=tile),
        in_specs=[VMEM, VMEM],
        out_specs=[VMEM] * 3,
        out_shape=[w, st, jax.ShapeDtypeStruct((blocks, m // blocks + CAP, d), bf16)],
        scratch_shapes=[pltpu.VMEM((m, d), f32), pltpu.VMEM((blocks * CAP, d), f32)],
        compiler_params=params(24),
        cost_estimate=cost(6),
        name="first_scores",
    )(gathered, chat)


def second_scores(gathered, chat, first, stats, shards, tile=1024):
    n, d = chat.shape
    m = gathered.shape[0] - 8
    blocks, rows = first.shape[0], first.shape[1]
    w, st = half_shapes(n, m)
    return pl.pallas_call(
        functools.partial(second_kernel, tile=tile, shards=shards),
        in_specs=[VMEM] * 4,
        out_specs=[VMEM] * 3 + [HBM],
        out_shape=[
            w,
            st,
            jax.ShapeDtypeStruct((2 * blocks, rows + 8, d), bf16),
            pltpu.HBM((1,), i32),
        ],
        scratch_shapes=[
            pltpu.VMEM((m, d), f32),
            pltpu.VMEM((blocks * CAP, d), f32),
            pltpu.SMEM((1,), i32),
            pltpu.SemaphoreType.DMA(()),
        ],
        compiler_params=params(24),
        cost_estimate=cost(6),
        name="second_scores",
    )(gathered, chat, first, stats)


def middle_kernel(line_ref, r_ref, o_ref, *, n):
    far, rows, d = o_ref.shape
    senders = r_ref.shape[0]
    own = rows // 3
    half = far * own
    low = r_ref[:, :half, :].astype(f32).sum(axis=0).astype(bf16)
    label = jnp.sum(line_ref[:, d:].astype(f32) * digit_weights((1, LANES)), axis=1, keepdims=True)
    lane = lax.broadcasted_iota(i32, (1, senders * CAP), 1)
    shift = CAP.bit_length() - 1
    sender, place = lane >> shift, lane & (CAP - 1)
    start = ((((sender >> 1) * far + at(FAR)) * 2 + (sender & 1)) * n).astype(f32)
    owned = (label >= start) & (label < start + n)
    before = lax.broadcasted_iota(i32, (half, half), 1) < lax.broadcasted_iota(i32, (half, half), 0)
    one = lambda a: jnp.where(a, 1.0, 0.0).astype(bf16)
    rank = dot(one(before), one(owned), 1, 0)
    spread = one(owned & (rank == place.astype(f32)))
    held = jnp.concatenate([r_ref[q, half : half + CAP, :] for q in range(senders)], axis=0)
    pick = dot(spread, held, 1, 0).astype(bf16)
    totals = total_rows(r_ref[:, half + CAP :, :].astype(f32).sum(axis=0).sum(axis=0, keepdims=True))
    for q in range(far):
        o_ref[q, :own, :] = low[q * own : (q + 1) * own]
        o_ref[q, own : 2 * own, :] = pick[q * own : (q + 1) * own]
        o_ref[q, 2 * own :, :] = totals


def middle(line, received, far, own, n):
    d = received.shape[2]
    return pl.pallas_call(
        functools.partial(middle_kernel, n=n),
        in_specs=[VMEM, VMEM],
        out_specs=VMEM,
        out_shape=jax.ShapeDtypeStruct((far, 3 * own, d), bf16),
        compiler_params=params(8),
        name="middle",
    )(line, received)


def grad_kernel(
    full_hbm, r_ref, x_ref, sta_ref, stb_ref, ea_ref, eb_ref, wa_ref, wb_ref, raw, l_hbm, xg_hbm, o_hbm, still_hbm,
    out, xg_ref, l_ref, flag_ref, osem, sem, *, chunk, blocks
):
    n, d = raw.shape
    half = wa_ref.shape[1]
    m = 2 * half
    own = x_ref.shape[0]
    chunks = n // chunk

    def save(k):
        rows = pl.ds(pl.multiple_of(k * chunk, chunk), chunk)
        return pltpu.make_async_copy(out.at[rows], o_hbm.at[rows], osem.at[k])

    side, at_x = at("y"), at("x")
    own_first = side * half + (at_x * lax.axis_size(FAR) + at(FAR)) * own
    flag = pltpu.make_async_copy(full_hbm, flag_ref, sem.at[2])
    flag.start()
    sums = r_ref[...].astype(f32).sum(axis=0)
    total = sums[2 * own :].sum(axis=0, keepdims=True)
    back = lax.rem(blocks - at_x, blocks) * (half // blocks)
    both = jnp.broadcast_to(total, (8, m))
    left = 1.0 / pltpu.roll(both[:, :half], back, 1)[0:1, :]
    right = 1.0 / pltpu.roll(both[:, half:], back, 1)[0:1, :]

    def factors(st_ref, scale):
        return st_ref[2:3, :].astype(i32), scale, st_ref[0:1, :] * (st_ref[1:2, :] * scale - logit_scale)

    halves = (
        (ea_ref, wa_ref, *factors(sta_ref, jnp.where(side == 0, left, right))),
        (eb_ref, wb_ref, *factors(stb_ref, jnp.where(side == 0, right, left))),
    )

    x = x_ref[...].astype(f32)
    inv = inverse_norm(x)
    units = x * inv
    unit16 = units.astype(bf16).astype(f32)
    pick = sums[own : 2 * own]
    texp, logit, slope = margin(jnp.sum(unit16 * pick, axis=1, keepdims=True))
    lane = lax.broadcasted_iota(i32, (own, m), 1)
    row = lax.broadcasted_iota(i32, (own, m), 0)
    own_total = jnp.sum(jnp.where(lane == row + own_first, total, 0.0), axis=1, keepdims=True)
    grad = sums[:own] / own_total + (slope * (texp / own_total - logit_scale)) * pick
    xg_ref[...] = inv * (grad - units * jnp.sum(units * grad, axis=1, keepdims=True))
    loss = jnp.log(own_total) + logit_scale - logit
    spread = jnp.where(lane[:, :LANES] == row[:, :LANES], loss, 0.0).sum(axis=0, keepdims=True)
    l_ref[...] = spread[:, :own]

    def step(k, _):
        rows = pl.ds(pl.multiple_of(k * chunk, chunk), chunk)
        row = lax.broadcasted_iota(i32, (chunk, half), 0)
        grad = 0.0
        for e_ref, w_ref, lab, scale, coef in halves:
            share = jnp.where(row == lab - k * chunk, coef, w_ref[rows, :].astype(f32) * scale)
            grad = grad + dot(share.astype(bf16), e_ref[:half, :], 1, 0)
        w = raw[rows, :].astype(f32)
        inv = inverse_norm(w)
        along = jnp.sum(w * grad, axis=1, keepdims=True) * (inv * inv)
        out[rows, :] = inv * (grad - w * along)
        save(k).start()
        return 0

    step(0, 0)
    small = (
        pltpu.make_async_copy(xg_ref, xg_hbm, sem.at[0]),
        pltpu.make_async_copy(l_ref, l_hbm, sem.at[1]),
    )
    for copy in small:
        copy.start()
    flag.wait()
    still = pltpu.make_async_copy(flag_ref, still_hbm, sem.at[3])
    still.start()
    lax.fori_loop(1, chunks, step, 0)
    for copy in (*small, still):
        copy.wait()
    for k in range(chunks):
        save(k).wait()


def grads(crowded, received, embeddings, stats, ehats, weights, raw, blocks, chunk=512):
    n, d = raw.shape
    own = embeddings.shape[0]
    return pl.pallas_call(
        functools.partial(grad_kernel, chunk=chunk, blocks=blocks),
        in_specs=[HBM] + [VMEM] * 9,
        out_specs=[HBM] * 4,
        out_shape=[
            pltpu.HBM((1, own), f32),
            pltpu.HBM((own, d), f32),
            jax.ShapeDtypeStruct((n, d), f32),
            pltpu.HBM((1,), i32),
        ],
        scratch_shapes=[
            pltpu.VMEM((n, d), f32),
            pltpu.VMEM((own, d), f32),
            pltpu.VMEM((1, own), f32),
            pltpu.SMEM((1,), i32),
            pltpu.SemaphoreType.DMA((n // chunk,)),
            pltpu.SemaphoreType.DMA((4,)),
        ],
        compiler_params=params(24),
        name="grads",
    )(in_hbm(crowded), received, embeddings, *stats, *ehats, *weights, raw)


def exchange(blocks, axis):
    return lax.all_to_all(blocks, axis, 0, 0, tiled=True)


def per_device(embeddings, labels, centers):
    own, d = embeddings.shape
    n = centers.shape[0]
    far, wide = lax.axis_size(FAR), lax.axis_size("x")
    line = exchange(pack(embeddings, labels, far), FAR).reshape(far * own, d + LANES)
    lines = [line] + [
        lax.ppermute(line, "x", [(i, (i - k) % wide) for i in range(wide)]) for k in range(1, wide)
    ]
    raw, chat = unit_centers(centers)
    first = merge(lines, d)
    second = lax.ppermute(first, "y", [(0, 1), (1, 0)])
    wa, sta, pay = first_scores(first, chat, wide)
    wb, stb, pay, crowded = second_scores(second, chat, pay, sta, far * wide * 2)
    received = exchange(middle(line, exchange(pay, NEAR), far, own, n), FAR)
    losses, emb_grad, center_grad, crowded = grads(
        crowded, received, embeddings, (sta, stb), (first, second), (wa, wb), raw, wide
    )
    losses, emb_grad = lax.cond(
        crowded[0] > 0,
        lambda loss, grad, late, x, y, w: dense_examples(x, y + jnp.minimum(late, 0), w),
        lambda loss, grad, *_: (loss, grad),
        losses, emb_grad, crowded, embeddings, labels, centers,
    )
    return (losses.reshape(own), emb_grad, center_grad)


def dense_examples(embeddings, labels, centers):
    own, d = embeddings.shape
    n = centers.shape[0]
    cls = ("x", FAR, "y")
    peers = lax.axis_size(cls)

    def alone(blocks, *others):
        blocks, others = lax.optimization_barrier((blocks, others))
        return lax.optimization_barrier((exchange(blocks, cls), *others))

    def copies(a):
        return jnp.broadcast_to(a[None], (peers, *a.shape))

    index = lax.axis_index(cls)
    x, w = embeddings.astype(f32), centers.astype(f32)
    inv = inverse_norm(x)
    units = x * inv
    chat = (w * inverse_norm(w)).astype(bf16)
    label, units, inv, chat, index = alone(copies(labels), units, inv, chat, index)
    rows, label, units, inv, chat, index = alone(copies(units.astype(bf16)), label, units, inv, chat, index)
    rows = rows.reshape(-1, d)
    label = label.reshape(-1) - index * n
    hot = label[:, None] == jnp.arange(n)[None]
    cosine = dot(rows, chat, 1, 1)
    picked = jnp.sum(jnp.where(hot, cosine, 0.0), axis=1)
    texp, logit, slope = margin(picked)
    owned = (label >= 0) & (label < n)
    texp, logit, slope = (jnp.where(owned, a, 0.0) for a in (texp, logit, slope))
    weight = jnp.where(hot, 0.0, jnp.exp2(cosine * slope2 - shift2))
    total = (weight.sum(axis=1) + texp) / logit_scale
    prod = dot(weight.astype(bf16), chat, 1, 0)
    pick = dot(hot.astype(bf16), chat, 1, 0)
    sums, prod, pick, slope, texp, units, inv, index = alone(
        copies(jnp.stack([total, logit])), prod, pick, slope, texp, units, inv, index
    )
    sums = sums.sum(axis=0)
    total = sums[0]
    rows = prod / total[:, None] + (slope * (texp / total - logit_scale))[:, None] * pick
    grad, sums, units, inv, index = alone(
        rows.astype(bf16).reshape(peers, own, d), sums, units, inv, index
    )
    grad = grad.astype(f32).sum(axis=0)
    mine = lax.dynamic_slice_in_dim(sums, index * own, own, 1)
    loss = jnp.log(mine[0]) + logit_scale - mine[1]
    return loss[None], inv * (grad - units * jnp.sum(units * grad, axis=1, keepdims=True))


def solution(mesh):
    dp = mesh.shape["dp"]
    fine = Mesh(mesh.devices.reshape(4, mesh.shape["cls"] // 8, 2, dp), ("x", FAR, "y", "dp"))
    rows = ("dp", "x", FAR, "y")
    in_specs = (P(rows, None), P(rows), P(rows, None))
    out_specs = (P(rows), P(rows, None), P(rows, None))
    return jax.shard_map(
        per_device, mesh=fine, in_specs=in_specs, out_specs=out_specs, check_vma=False
    )
```

```python
import functools
import math

import jax
import jax.numpy as jnp
from jax import lax
from jax.experimental import pallas as pl
from jax.experimental.pallas import tpu as pltpu
from jax.sharding import Mesh
from jax.sharding import PartitionSpec as P

logit_scale = 64.0
margin_cosine = math.cos(0.5)
margin_sine = math.sin(0.5)
sine_soften = 0.04
norm_eps = 1e-06

slope2 = logit_scale * math.log2(math.e)
shift2 = slope2 - math.log2(logit_scale)


LANES = 128
CAP = 16
MIB = 1024 * 1024
NEAR = ("x", "y")
FAR = "z"
f32, bf16, i32 = jnp.float32, jnp.bfloat16, jnp.int32
VMEM = pl.BlockSpec(memory_space=pltpu.VMEM)
SMEM = pl.BlockSpec(memory_space=pltpu.SMEM)
HBM = pl.BlockSpec(memory_space=pltpu.HBM)


def params(mib):
    return pltpu.CompilerParams(vmem_limit_bytes=mib * MIB)


def cost(gflops):
    return pl.CostEstimate(flops=int(gflops * 1e9), bytes_accessed=8 * MIB, transcendentals=0)


def in_hbm(x):
    return pltpu.with_memory_space_constraint(x, pltpu.HBM)


def dot(a, b, ca, cb):
    return lax.dot_general(a, b, (((ca,), (cb,)), ((), ())), preferred_element_type=f32)


def inverse_norm(x):
    return lax.rsqrt(jnp.sum(x * x, axis=1, keepdims=True) + norm_eps)


def margin(cosine):
    sine = jnp.sqrt(1.0 + sine_soften - cosine * cosine)
    shifted = cosine * margin_cosine - sine * margin_sine
    slope = margin_cosine + margin_sine * cosine / sine
    return jnp.exp2(slope2 * shifted - shift2), logit_scale * shifted, slope


def total_rows(total):
    row8 = lax.broadcasted_iota(i32, (8, total.shape[1]), 0)
    out = jnp.zeros(row8.shape, f32)
    rest = total
    for r in range(3):
        part = rest.astype(bf16).astype(f32)
        out = jnp.where(row8 == r, part, out)
        rest = rest - part
    return out.astype(bf16)


def pack_kernel(x_hbm, lab_hbm, o_ref, x_ref, lab_ref, sem):
    rows, d = x_ref.shape
    copies = (
        pltpu.make_async_copy(lab_hbm, lab_ref, sem.at[0]),
        pltpu.make_async_copy(x_hbm, x_ref, sem.at[1]),
    )
    for copy in copies:
        copy.start()
    for copy in copies:
        copy.wait()
    row = lax.broadcasted_iota(i32, (rows, LANES), 0)
    lane = lax.broadcasted_iota(i32, (rows, LANES), 1)
    lab = jnp.zeros((rows, LANES), i32)
    for j in range(rows):
        lab = jnp.where(row == j, lab_ref[j], lab)
    digit = jnp.where(lane == 0, lab >> 12, jnp.where(lane == 1, (lab >> 6) & 63, lab & 63))
    digit = jnp.where(lane < 3, digit, 0).astype(f32).astype(bf16)
    for p in range(o_ref.shape[0]):
        o_ref[p, :, :d] = x_ref[...]
        o_ref[p, :, d:] = digit


def pack(embeddings, labels, peers):
    rows, d = embeddings.shape
    return pl.pallas_call(
        pack_kernel,
        in_specs=[HBM, HBM],
        out_specs=VMEM,
        out_shape=jax.ShapeDtypeStruct((peers, rows, d + LANES), bf16),
        scratch_shapes=[
            pltpu.VMEM((rows, d), bf16),
            pltpu.SMEM((rows,), i32),
            pltpu.SemaphoreType.DMA((2,)),
        ],
        compiler_params=params(4),
        name="pack",
    )(in_hbm(embeddings), in_hbm(labels))


def digit_weights(shape):
    lane = lax.broadcasted_iota(i32, shape, 1)
    return jnp.where(lane == 0, 4096.0, jnp.where(lane == 1, 64.0, jnp.where(lane == 2, 1.0, 0.0)))


def merge_kernel(*refs):
    *line_refs, o_ref = refs
    rows, d = line_refs[0].shape[0], o_ref.shape[1]
    half = rows * len(line_refs)
    for p, line_ref in enumerate(line_refs):
        x = line_ref[:, :d].astype(f32)
        o_ref[p * rows : (p + 1) * rows, :] = (x * inverse_norm(x)).astype(bf16)
    tail = jnp.concatenate([line_ref[:, d:] for line_ref in line_refs], axis=0)
    same = lax.broadcasted_iota(i32, (8, LANES), 0) == lax.broadcasted_iota(i32, (8, LANES), 1)
    digits = dot(jnp.where(same, 1.0, 0.0).astype(bf16), tail, 1, 1).astype(bf16)
    o_ref[half:, :] = jnp.concatenate([digits] * (d // half), axis=1)


def merge(lines, d):
    rows = lines[0].shape[0] * len(lines)
    return pl.pallas_call(
        merge_kernel,
        in_specs=[VMEM] * len(lines),
        out_specs=VMEM,
        out_shape=jax.ShapeDtypeStruct((rows + 8, d), bf16),
        compiler_params=params(8),
        cost_estimate=cost(0.01),
        name="merge",
    )(*lines)


def unit_kernel(c_hbm, raw, chat, sem, *, tile):
    steps = c_hbm.shape[0] // tile

    def span(k):
        return pl.ds(pl.multiple_of(k * tile, tile), tile)

    def fetch(k):
        return pltpu.make_async_copy(c_hbm.at[span(k)], raw.at[span(k)], sem.at[k])

    for k in range(steps):
        fetch(k).start()

    def step(k, _):
        fetch(k).wait()
        w = raw[span(k), :].astype(f32)
        chat[span(k), :] = (w * inverse_norm(w)).astype(bf16)
        return 0

    lax.fori_loop(0, steps, step, 0)


def unit_centers(centers, tile=512):
    return pl.pallas_call(
        functools.partial(unit_kernel, tile=tile),
        in_specs=[HBM],
        out_specs=[VMEM] * 2,
        out_shape=[pltpu.VMEM(centers.shape, bf16)] * 2,
        scratch_shapes=[pltpu.SemaphoreType.DMA((centers.shape[0] // tile,))],
        compiler_params=params(12),
        cost_estimate=cost(3),
        name="unit_centers",
    )(in_hbm(centers))


def score_half(base_ref, g_ref, chat, w_ref, st_ref, acc, pck, rows, *, tile):
    n, d = chat.shape
    m = w_ref.shape[1]
    steps = n // tile
    digits = g_ref[m:, :m].astype(f32)
    lab1 = (digits[0:1] * 4096.0 + digits[1:2] * 64.0 + digits[2:3]).astype(i32) - base_ref[0]
    owned = (lab1 >= 0) & (lab1 < n)
    shift = rows.bit_length() - 1
    before, after = (lax.broadcasted_iota(i32, (m, m), a) for a in (0, 1))
    ahead = (before < after) & ((before >> shift) == (after >> shift))
    mine = jnp.broadcast_to(jnp.where(owned, 1.0, 0.0), (8, m)).astype(bf16)
    rank = dot(mine, jnp.where(ahead, 1.0, 0.0).astype(bf16), 1, 0)[0:1, :].astype(i32)
    block = lax.broadcasted_iota(i32, (1, m), 1) >> shift
    slots = (m // rows) * CAP
    place = jnp.where(owned & (rank < CAP), block * CAP + rank, -1)
    chosen = lax.broadcasted_iota(i32, (slots, m), 0) == place
    held = jnp.sum(jnp.where(chosen, lab1.astype(f32) + 1.0, 0.0), axis=1, keepdims=True).astype(i32) - 1

    def span(k):
        return pl.ds(pl.multiple_of(k * tile, tile), tile)

    def score(k, tot, tcs):
        cos = dot(chat[span(k), :], g_ref[:m, :], 1, 1)
        hit = lax.broadcasted_iota(i32, (tile, m), 0) == lab1 - k * tile
        e = jnp.where(hit, 0.0, jnp.exp2(cos * slope2 - shift2))
        w_ref[span(k), :] = e.astype(bf16)
        tot = tot + e.reshape(tile // 8, 8, m).sum(axis=0)
        tcs = tcs + jnp.where(hit, cos, 0.0).reshape(tile // 8, 8, m).sum(axis=0)
        return tot, tcs

    def gather(k):
        hot = lax.broadcasted_iota(i32, (slots, tile), 1) == held - k * tile
        c = chat[span(k), :]
        prod = dot(w_ref[span(k), :], c, 0, 0)
        pick = dot(jnp.where(hot, 1.0, 0.0).astype(bf16), c, 1, 0)
        return prod, pick

    zero = jnp.zeros((8, m), f32)
    tot, tcs = score(0, zero, zero)
    acc[...] = jnp.zeros(acc.shape, f32)

    def step(k, carry):
        tot, tcs, held_sum = carry
        prod, pick = gather(k - 1)
        tot, tcs = score(k, tot, tcs)
        acc[...] += prod
        return tot, tcs, held_sum + pick

    tot, tcs, held_sum = lax.fori_loop(1, steps, step, (tot, tcs, jnp.zeros((slots, d), f32)))
    prod, pick = gather(steps - 1)
    acc[...] += prod
    pck[...] = held_sum + pick
    texp, _, slope = margin(tcs.sum(axis=0, keepdims=True))
    texp = jnp.where(owned, texp, 0.0)
    slope = jnp.where(owned, slope, 0.0)
    total = (tot.sum(axis=0, keepdims=True) + texp) * (1.0 / logit_scale)
    row8 = lax.broadcasted_iota(i32, (8, m), 0)
    rest = jnp.where(row8 == 3, total, lab1.astype(f32))
    st_ref[...] = jnp.where(row8 == 0, slope, jnp.where(row8 == 1, texp, rest))


def first_kernel(base_ref, g_ref, chat, w_ref, st_ref, pay_ref, acc, pck, *, tile):
    blocks, rows = pay_ref.shape[0], pay_ref.shape[1] - CAP
    score_half(base_ref, g_ref, chat, w_ref, st_ref, acc, pck, rows, tile=tile)
    for p in range(blocks):
        pay_ref[p, :rows, :] = acc[p * rows : (p + 1) * rows].astype(bf16)
        pay_ref[p, rows:, :] = pck[p * CAP : (p + 1) * CAP].astype(bf16)


def most(label, n, shards, rows):
    m = label.shape[1]
    shift, wide = rows.bit_length() - 1, n.bit_length() - 1
    owner = label >> wide
    hot = lax.broadcasted_iota(i32, (shards, m), 0) == owner
    block = (lax.broadcasted_iota(i32, (m, LANES), 0) >> shift) == lax.broadcasted_iota(i32, (m, LANES), 1)
    one = lambda a: jnp.where(a, 1.0, 0.0).astype(bf16)
    return jnp.max(dot(one(hot), one(block), 1, 0))


def second_kernel(
    base_ref, side_ref, x_ref, g_ref, chat, first_ref, firstst_ref, w_ref, st_ref, pay_ref, full_hbm, acc, pck, full_ref, sem, *, tile, shards
):
    blocks, rows = first_ref.shape[0], first_ref.shape[1] - CAP
    count = functools.partial(most, n=chat.shape[0], shards=shards, rows=rows)
    digits = g_ref[w_ref.shape[1] :, : w_ref.shape[1]].astype(f32)
    label = digits[0:1] * 4096.0 + digits[1:2] * 64.0 + digits[2:3]
    crowded = jnp.maximum(count(firstst_ref[2:3, :].astype(i32) + base_ref[0]), count(label.astype(i32)))
    full_ref[0] = (crowded > CAP).astype(i32)
    copy = pltpu.make_async_copy(full_ref, full_hbm, sem)
    copy.start()
    score_half(base_ref, g_ref, chat, w_ref, st_ref, acc, pck, rows, tile=tile)
    side, at_x = side_ref[0], x_ref[0]
    mine = pltpu.roll(firstst_ref[...], at_x * rows, 1)[3:4, :]
    theirs = pltpu.roll(st_ref[...], at_x * rows, 1)[3:4, :]
    left = jnp.where(side == 0, mine, theirs)
    right = jnp.where(side == 0, theirs, mine)
    sums = total_rows(jnp.concatenate([left, right], axis=1))
    for p in range(2 * blocks):
        pay_ref[p, rows + CAP :, :] = sums
    for p in range(blocks):
        to = lax.rem(at_x + p, blocks)
        pay_ref[2 * to + side, : rows + CAP, :] = first_ref[p]
        other = 2 * to + 1 - side
        pay_ref[other, :rows, :] = acc[p * rows : (p + 1) * rows].astype(bf16)
        pay_ref[other, rows : rows + CAP, :] = pck[p * CAP : (p + 1) * CAP].astype(bf16)
    copy.wait()


def half_shapes(n, m):
    return [pltpu.VMEM((n, m), bf16), jax.ShapeDtypeStruct((8, m), f32)]


def first_scores(base, gathered, chat, blocks, tile=1024):
    n, d = chat.shape
    m = gathered.shape[0] - 8
    w, st = half_shapes(n, m)
    return pl.pallas_call(
        functools.partial(first_kernel, tile=tile),
        in_specs=[SMEM, VMEM, VMEM],
        out_specs=[VMEM] * 3,
        out_shape=[w, st, jax.ShapeDtypeStruct((blocks, m // blocks + CAP, d), bf16)],
        scratch_shapes=[pltpu.VMEM((m, d), f32), pltpu.VMEM((blocks * CAP, d), f32)],
        compiler_params=params(24),
        cost_estimate=cost(6),
        name="first_scores",
    )(base, gathered, chat)


def second_scores(where, gathered, chat, first, stats, shards, tile=1024):
    n, d = chat.shape
    m = gathered.shape[0] - 8
    blocks, rows = first.shape[0], first.shape[1]
    w, st = half_shapes(n, m)
    return pl.pallas_call(
        functools.partial(second_kernel, tile=tile, shards=shards),
        in_specs=[SMEM] * 3 + [VMEM] * 4,
        out_specs=[VMEM] * 3 + [HBM],
        out_shape=[
            w,
            st,
            jax.ShapeDtypeStruct((2 * blocks, rows + 8, d), bf16),
            pltpu.HBM((1,), i32),
        ],
        scratch_shapes=[
            pltpu.VMEM((m, d), f32),
            pltpu.VMEM((blocks * CAP, d), f32),
            pltpu.SMEM((1,), i32),
            pltpu.SemaphoreType.DMA(()),
        ],
        compiler_params=params(24),
        cost_estimate=cost(6),
        name="second_scores",
    )(*where, gathered, chat, first, stats)


def middle_kernel(far_ref, line_ref, r_ref, o_ref, *, n):
    far, rows, d = o_ref.shape
    senders = r_ref.shape[0]
    own = rows // 3
    half = far * own
    low = r_ref[:, :half, :].astype(f32).sum(axis=0).astype(bf16)
    label = jnp.sum(line_ref[:, d:].astype(f32) * digit_weights((1, LANES)), axis=1, keepdims=True)
    lane = lax.broadcasted_iota(i32, (1, senders * CAP), 1)
    shift = CAP.bit_length() - 1
    sender, place = lane >> shift, lane & (CAP - 1)
    start = ((((sender >> 1) * far + far_ref[0]) * 2 + (sender & 1)) * n).astype(f32)
    owned = (label >= start) & (label < start + n)
    before = lax.broadcasted_iota(i32, (half, half), 1) < lax.broadcasted_iota(i32, (half, half), 0)
    one = lambda a: jnp.where(a, 1.0, 0.0).astype(bf16)
    rank = dot(one(before), one(owned), 1, 0)
    spread = one(owned & (rank == place.astype(f32)))
    held = jnp.concatenate([r_ref[q, half : half + CAP, :] for q in range(senders)], axis=0)
    pick = dot(spread, held, 1, 0).astype(bf16)
    totals = total_rows(r_ref[:, half + CAP :, :].astype(f32).sum(axis=0).sum(axis=0, keepdims=True))
    for q in range(far):
        o_ref[q, :own, :] = low[q * own : (q + 1) * own]
        o_ref[q, own : 2 * own, :] = pick[q * own : (q + 1) * own]
        o_ref[q, 2 * own :, :] = totals


def middle(at_far, line, received, far, own, n):
    d = received.shape[2]
    return pl.pallas_call(
        functools.partial(middle_kernel, n=n),
        in_specs=[SMEM, VMEM, VMEM],
        out_specs=VMEM,
        out_shape=jax.ShapeDtypeStruct((far, 3 * own, d), bf16),
        compiler_params=params(8),
        name="middle",
    )(at_far, line, received)


def grad_kernel(
    side_ref, at_ref, own_ref, full_ref, r_ref, x_ref, sta_ref, stb_ref, ea_ref, eb_ref, wa_ref, wb_ref, raw, l_hbm, xg_hbm, o_hbm, still_hbm,
    out, xg_ref, l_ref, osem, sem, *, chunk, blocks
):
    n, d = raw.shape
    half = wa_ref.shape[1]
    m = 2 * half
    own = x_ref.shape[0]
    chunks = n // chunk

    def save(k):
        rows = pl.ds(pl.multiple_of(k * chunk, chunk), chunk)
        return pltpu.make_async_copy(out.at[rows], o_hbm.at[rows], osem.at[k])

    side, at_x, own_first = side_ref[0], at_ref[0], own_ref[0]
    still = pltpu.make_async_copy(full_ref, still_hbm, sem.at[2])
    still.start()
    sums = r_ref[...].astype(f32).sum(axis=0)
    total = sums[2 * own :].sum(axis=0, keepdims=True)
    back = lax.rem(blocks - at_x, blocks) * (half // blocks)
    both = jnp.broadcast_to(total, (8, m))
    left = 1.0 / pltpu.roll(both[:, :half], back, 1)[0:1, :]
    right = 1.0 / pltpu.roll(both[:, half:], back, 1)[0:1, :]

    def factors(st_ref, scale):
        return st_ref[2:3, :].astype(i32), scale, st_ref[0:1, :] * (st_ref[1:2, :] * scale - logit_scale)

    halves = (
        (ea_ref, wa_ref, *factors(sta_ref, jnp.where(side == 0, left, right))),
        (eb_ref, wb_ref, *factors(stb_ref, jnp.where(side == 0, right, left))),
    )

    def step(k, _):
        rows = pl.ds(pl.multiple_of(k * chunk, chunk), chunk)
        row = lax.broadcasted_iota(i32, (chunk, half), 0)
        grad = 0.0
        for e_ref, w_ref, lab, scale, coef in halves:
            share = jnp.where(row == lab - k * chunk, coef, w_ref[rows, :].astype(f32) * scale)
            grad = grad + dot(share.astype(bf16), e_ref[:half, :], 1, 0)
        w = raw[rows, :].astype(f32)
        inv = inverse_norm(w)
        along = jnp.sum(w * grad, axis=1, keepdims=True) * (inv * inv)
        out[rows, :] = inv * (grad - w * along)
        save(k).start()
        return 0

    lax.fori_loop(0, chunks, step, 0)

    x = x_ref[...].astype(f32)
    inv = inverse_norm(x)
    units = x * inv
    unit16 = units.astype(bf16).astype(f32)
    pick = sums[own : 2 * own]
    texp, logit, slope = margin(jnp.sum(unit16 * pick, axis=1, keepdims=True))
    lane = lax.broadcasted_iota(i32, (own, m), 1)
    row = lax.broadcasted_iota(i32, (own, m), 0)
    own_total = jnp.sum(jnp.where(lane == row + own_first, total, 0.0), axis=1, keepdims=True)
    grad = sums[:own] / own_total + (slope * (texp / own_total - logit_scale)) * pick
    xg_ref[...] = inv * (grad - units * jnp.sum(units * grad, axis=1, keepdims=True))
    loss = jnp.log(own_total) + logit_scale - logit
    spread = jnp.where(lane[:, :LANES] == row[:, :LANES], loss, 0.0).sum(axis=0, keepdims=True)
    l_ref[...] = spread[:, :own]

    small = (
        pltpu.make_async_copy(xg_ref, xg_hbm, sem.at[0]),
        pltpu.make_async_copy(l_ref, l_hbm, sem.at[1]),
    )
    for copy in small:
        copy.start()
    for copy in (*small, still):
        copy.wait()
    for k in range(chunks):
        save(k).wait()


def grads(where, received, embeddings, stats, ehats, weights, raw, blocks, chunk=512):
    n, d = raw.shape
    own = embeddings.shape[0]
    return pl.pallas_call(
        functools.partial(grad_kernel, chunk=chunk, blocks=blocks),
        in_specs=[SMEM] * 4 + [VMEM] * 9,
        out_specs=[HBM] * 4,
        out_shape=[
            pltpu.HBM((1, own), f32),
            pltpu.HBM((own, d), f32),
            jax.ShapeDtypeStruct((n, d), f32),
            pltpu.HBM((1,), i32),
        ],
        scratch_shapes=[
            pltpu.VMEM((n, d), f32),
            pltpu.VMEM((own, d), f32),
            pltpu.VMEM((1, own), f32),
            pltpu.SemaphoreType.DMA((n // chunk,)),
            pltpu.SemaphoreType.DMA((3,)),
        ],
        compiler_params=params(24),
        name="grads",
    )(*where, received, embeddings, *stats, *ehats, *weights, raw)


def exchange(blocks, axis):
    return lax.all_to_all(blocks, axis, 0, 0, tiled=True)


def per_device(embeddings, labels, centers):
    own, d = embeddings.shape
    n = centers.shape[0]
    far, wide = lax.axis_size(FAR), lax.axis_size("x")
    at_x, at_y = lax.axis_index("x"), lax.axis_index("y")
    half = far * wide * own
    at_far = lax.axis_index(FAR)
    base = lax.axis_index(("x", FAR, "y")) * n
    own_first = at_y * half + (at_x * far + at_far) * own
    where = tuple(a.astype(i32)[None] for a in (base, at_y, at_x, own_first, at_far))
    embeddings, where = lax.optimization_barrier((embeddings, where))
    base, side, at_x, own_first, at_far = where
    line = exchange(pack(embeddings, labels, far), FAR).reshape(far * own, d + LANES)
    lines = [line] + [
        lax.ppermute(line, "x", [(i, (i - k) % wide) for i in range(wide)]) for k in range(1, wide)
    ]
    raw, chat = unit_centers(centers)
    first = merge(lines, d)
    second = lax.ppermute(first, "y", [(0, 1), (1, 0)])
    wa, sta, pay = first_scores(base, first, chat, wide)
    wb, stb, pay, crowded = second_scores((base, side, at_x), second, chat, pay, sta, far * wide * 2)
    received = exchange(middle(at_far, line, exchange(pay, NEAR), far, own, n), FAR)
    losses, emb_grad, center_grad, crowded = grads(
        (side, at_x, own_first, crowded), received, embeddings, (sta, stb), (first, second), (wa, wb), raw, wide
    )
    losses, emb_grad = lax.cond(
        crowded[0] > 0,
        lambda loss, grad, late, x, y, w: dense_examples(x, y + jnp.minimum(late, 0), w),
        lambda loss, grad, *_: (loss, grad),
        losses, emb_grad, crowded, embeddings, labels, centers,
    )
    return (losses.reshape(own), emb_grad, center_grad)


def dense_examples(embeddings, labels, centers):
    own, d = embeddings.shape
    n = centers.shape[0]
    cls = ("x", FAR, "y")
    peers = lax.axis_size(cls)

    def alone(blocks, *others):
        blocks, others = lax.optimization_barrier((blocks, others))
        return lax.optimization_barrier((exchange(blocks, cls), *others))

    def copies(a):
        return jnp.broadcast_to(a[None], (peers, *a.shape))

    index = lax.axis_index(cls)
    x, w = embeddings.astype(f32), centers.astype(f32)
    inv = inverse_norm(x)
    units = x * inv
    chat = (w * inverse_norm(w)).astype(bf16)
    label, units, inv, chat, index = alone(copies(labels), units, inv, chat, index)
    rows, label, units, inv, chat, index = alone(copies(units.astype(bf16)), label, units, inv, chat, index)
    rows = rows.reshape(-1, d)
    label = label.reshape(-1) - index * n
    hot = label[:, None] == jnp.arange(n)[None]
    cosine = dot(rows, chat, 1, 1)
    picked = jnp.sum(jnp.where(hot, cosine, 0.0), axis=1)
    texp, logit, slope = margin(picked)
    owned = (label >= 0) & (label < n)
    texp, logit, slope = (jnp.where(owned, a, 0.0) for a in (texp, logit, slope))
    weight = jnp.where(hot, 0.0, jnp.exp2(cosine * slope2 - shift2))
    total = (weight.sum(axis=1) + texp) / logit_scale
    prod = dot(weight.astype(bf16), chat, 1, 0)
    pick = dot(hot.astype(bf16), chat, 1, 0)
    sums, prod, pick, slope, texp, units, inv, index = alone(
        copies(jnp.stack([total, logit])), prod, pick, slope, texp, units, inv, index
    )
    sums = sums.sum(axis=0)
    total = sums[0]
    rows = prod / total[:, None] + (slope * (texp / total - logit_scale))[:, None] * pick
    grad, sums, units, inv, index = alone(
        rows.astype(bf16).reshape(peers, own, d), sums, units, inv, index
    )
    grad = grad.astype(f32).sum(axis=0)
    mine = lax.dynamic_slice_in_dim(sums, index * own, own, 1)
    loss = jnp.log(mine[0]) + logit_scale - mine[1]
    return loss[None], inv * (grad - units * jnp.sum(units * grad, axis=1, keepdims=True))


def solution(mesh):
    dp = mesh.shape["dp"]
    fine = Mesh(mesh.devices.reshape(4, mesh.shape["cls"] // 8, 2, dp), ("x", FAR, "y", "dp"))
    rows = ("dp", "x", FAR, "y")
    in_specs = (P(rows, None), P(rows), P(rows, None))
    out_specs = (P(rows), P(rows, None), P(rows, None))
    return jax.shard_map(
        per_device, mesh=fine, in_specs=in_specs, out_specs=out_specs, check_vma=False
    )
```
